32 devices in a mesh: dp: 2 (over x), tp2: 4 (over z), tp: 4 (over y, core).
Axes of the slice: x: 2, y: 2, z: 4, core: 2. Of those that a mesh axis runs over, the one named last changes fastest.
Arguments:
- attn_out: bfloat16 [16384, 8192], P('dp', 'tp'), parts along dimension 0
- w_out: bfloat16 [8192, 8192], P('tp', 'tp2')
- residual: bfloat16 [16384, 8192], P(('dp', 'tp'), 'tp2'), parts along dimension 0
- norm_gain: float32 [8192], P('tp2')
Outputs:
- output 1: bfloat16 [16384, 8192], P(('dp', 'tp'), 'tp2'), parts along dimension 0
- output 2: bfloat16 [16384, 8192], P(('dp', 'tp'), 'tp2'), parts along dimension 0
There are 2 independent parts. The reference program is written for one: setup_inputs(seed, part) draws one part's arguments, and reference() takes and returns one part's arrays. A program takes and returns all parts, laid end to end along the dimension named above; an argument that names none is the same for every part.
All inputs are finite; a program needn't handle non-finite values.
Results may differ from the reference program's by a relative error of at most 0.00720324.
Values are sent between devices in bfloat16 or wider.
A program may use at most 1 GiB of HBM per device.

```python
import jax
import jax.numpy as jnp
from jax import lax

TOKENS = 8192
D = 8192
HEADS = 64
HEAD = 128
TP = 4
EPS_NORM = 1e-6


def setup_inputs(seed: int = 0, part: int = 0) -> dict:
    attn_width = HEADS * HEAD
    root_key = jax.random.key(seed)
    key_attn, key_w, key_res, key_gain = jax.random.split(root_key, 4)
    attn_vals = jax.random.normal(jax.random.fold_in(key_attn, part), (TOKENS, attn_width), jnp.float32)
    w_vals = jax.random.normal(key_w, (attn_width, D), jnp.float32) * (attn_width ** -0.5)
    res_vals = jax.random.normal(jax.random.fold_in(key_res, part), (TOKENS, D), jnp.float32)
    gain_vals = 1.0 + 0.3 * jax.random.normal(key_gain, (D,), jnp.float32)
    return {"attn_out": attn_vals.astype(jnp.bfloat16), "w_out": w_vals.astype(jnp.bfloat16), "residual": res_vals.astype(jnp.bfloat16), "norm_gain": gain_vals}


def reference(attn_out, w_out, residual, norm_gain):
    attn_width = attn_out.shape[1]
    shard_cols = attn_width // TP
    attn_shards = attn_out.reshape(TOKENS, TP, shard_cols).transpose(1, 0, 2)
    w_shards = w_out.reshape(TP, shard_cols, D)

    def add_shard(running, shard_pair):
        attn_blk, w_blk = shard_pair
        block_prod = jnp.dot(attn_blk, w_blk, preferred_element_type=jnp.float32).astype(jnp.bfloat16)
        return running + block_prod.astype(jnp.float32), None

    y_sum, _ = lax.scan(add_shard, jnp.zeros((TOKENS, D), jnp.float32), (attn_shards, w_shards))
    hidden = residual.astype(jnp.float32) + y_sum
    mean_sq = jnp.mean(hidden * hidden, axis=-1, keepdims=True)
    normed = hidden * lax.rsqrt(mean_sq + EPS_NORM) * norm_gain
    return hidden.astype(jnp.bfloat16), normed.astype(jnp.bfloat16)
```

```python
import functools

import jax
import jax.numpy as jnp
from jax import lax
from jax.experimental import pallas as pl
from jax.experimental.pallas import tpu as pltpu
from jax.sharding import PartitionSpec as P

EPS_NORM = 1e-6
MESH = pl.DeviceIdType.MESH
NCH = 32
NWC = 8
GRP = 4
NUNIT = NCH // GRP
AHEAD = 3
NSLOT = 21
LOCAL0 = 2


def step_count(i, slots):
    n = jnp.int32(0)
    for s in slots:
        n = n + jnp.where(i >= s, 1, 0)
    return n


END_UNITS = (10, 10, 12, 13, 16, 17, 19, 20)
MID_UNITS = (17, 18, 19, 19, 19, 20, 20, 20)


def kernel(a, w, r, g, h_out, n_out, ax, ap, wl, wr, acc, abuf, rbuf, obuf, ss_loc, ss_all,
           recv_a, send_ya, send_yw, send_zi, send_zo, recv_wy, recv_wx, recv_wd, send_wx, send_wd,
           recv_da, recv_dw, send_da, send_dw, load_sem, load_w, out_sem, send_ss, recv_ss):
    x = lax.axis_index("dp")
    z = lax.axis_index("tp2")
    t = lax.axis_index("tp")
    y = t // 2
    c = t % 2
    rows, cols = acc.shape
    kb = w.shape[0]
    ch = rows // NCH
    wch = kb // 2 // NWC
    unit = ch * GRP
    side = z // 2
    end = (z == 0) | (z == 3)
    mid = (z == 1) | (z == 2)
    base = side * (NCH // 2)
    other = (1 - side) * (NCH // 2)
    z_in = jnp.where(side == 0, z + 1, z - 1)
    z_out = jnp.where(side == 0, z - 1, z + 1)

    partner = (x, z, y * 2 + 1 - c)
    x_peer = (1 - x, z, t)
    y_same = (x, z, (1 - y) * 2 + c)
    y_cross = (x, z, (1 - y) * 2 + 1 - c)

    def remote(src, dst, send, recv, dev):
        return pltpu.make_async_remote_copy(
            src_ref=src, dst_ref=dst, send_sem=send, recv_sem=recv, device_id=dev, device_id_type=MESH)

    def wait_bytes(ref, sem):
        pltpu.make_async_copy(ref, ref, sem).wait()

    barrier = pltpu.get_barrier_semaphore()
    for dev in (partner, x_peer, y_same, y_cross):
        pl.semaphore_signal(barrier, inc=1, device_id=dev, device_id_type=MESH)
    for k in range(1, 4):
        pl.semaphore_signal(barrier, inc=1, device_id=(x, lax.rem(z + k, 4), t), device_id_type=MESH)
    pl.semaphore_wait(barrier, 7)

    def mp(start, j):
        return start + NCH // 4 + lax.rem(j + NCH // 8, NCH // 4)

    def send_y_a(q):
        for cc in range(2):
            row = ((1 - y) * 2 + cc) * rows + q * ch
            remote(a.at[pl.ds(pl.multiple_of(row, ch), ch)], ax.at[q, c], send_ya, recv_a.at[q],
                   (x, z, (1 - y) * 2 + cc)).start()

    def w_rows(half, i):
        return pl.ds(pl.multiple_of(half * (kb // 2) + i * wch, wch), wch)

    def send_y_w(i):
        remote(w.at[w_rows(x, i)], wr.at[c, w_rows(x, i)], send_yw, recv_wy.at[i], y_same).start()

    def y_sends(i):
        @pl.when(end & (i < NWC))
        def _():
            send_y_w(i)

        @pl.when(end & (i >= NWC) & (i < NWC + 12))
        def _():
            send_y_a(base + i - NWC)

        @pl.when(mid & (i < 8))
        def _():
            send_y_a(mp(base, i))

        @pl.when(mid & (i >= 8) & (i < 8 + NWC))
        def _():
            send_y_w(i - 8)

    lax.fori_loop(0, AHEAD, lambda i, _: (y_sends(i), None)[1], None)

    remote(w, wl.at[1], send_dw, recv_dw, partner).start()
    prow = pl.ds(pl.multiple_of((y * 2 + 1 - c) * rows, rows), rows)
    remote(a.at[prow], ap, send_da, recv_da, partner).start()
    own_w = pltpu.make_async_copy(w, wl.at[0], load_w)
    own_w.start()

    def arrive(q):
        wait_bytes(ax.at[q], recv_a.at[q])

    def pass_in(q):
        remote(ax.at[q], ax.at[q], send_zi, recv_a.at[q], (x, z_in, t)).start()

    def pass_out(q):
        remote(ax.at[q], ax.at[q], send_zo, recv_a.at[q], (x, z_out, t)).start()

    def w_from_y(i):
        part = wr.at[c, w_rows(x, i)]
        wait_bytes(part, recv_wy.at[i])
        remote(part, part, send_wx, recv_wx.at[i], x_peer).start()
        remote(part, part, send_wd, recv_wd, partner).start()

    def w_from_x(i):
        part = wr.at[c, w_rows(1 - x, i)]
        wait_bytes(part, recv_wx.at[i])
        remote(part, part, send_wd, recv_wd, partner).start()

    def comm(i):
        y_sends(i + AHEAD)

        @pl.when(end)
        def _():
            @pl.when(i < NWC)
            def _():
                w_from_y(i)

            @pl.when((i >= NWC) & (i < NWC + 12))
            def _():
                q = base + i - NWC
                arrive(q)

                @pl.when(i < NWC + 8)
                def _():
                    pass_in(q)

            @pl.when((i >= 1) & (i < 1 + NWC))
            def _():
                w_from_x(i - 1)

            j = i - 1

            @pl.when((j >= 0) & (j < 4))
            def _():
                arrive(mp(base, j))

            @pl.when((j >= 4) & (j < 12))
            def _():
                arrive(mp(other, j - 4))

            @pl.when((j >= 12) & (j < 20))
            def _():
                arrive(other + j - 12)

        @pl.when(mid)
        def _():
            @pl.when(i < 8)
            def _():
                q = mp(base, i)
                arrive(q)

                @pl.when(i < 4)
                def _():
                    pass_out(q)

                pass_in(q)

            @pl.when((i >= 1) & (i < 9))
            def _():
                q = mp(other, i - 1)
                arrive(q)
                pass_out(q)

            @pl.when((i >= 9) & (i < 17))
            def _():
                q = base + i - 9
                arrive(q)
                pass_in(q)

            @pl.when((i >= 10) & (i < 18))
            def _():
                q = other + i - 10
                arrive(q)
                pass_out(q)

            @pl.when((i >= 8) & (i < 8 + NWC))
            def _():
                w_from_y(i - 8)

            @pl.when((i >= 9) & (i < 9 + NWC))
            def _():
                w_from_x(i - 9)

    tn = min(512, cols)
    ntile = cols // tn

    def local_loads(u):
        slot = lax.rem(u, 2)
        here = pl.ds(pl.multiple_of(u * unit, unit), unit)
        mine = pl.ds(pl.multiple_of(t * rows + u * unit, unit), unit)
        return (pltpu.make_async_copy(a.at[mine], abuf.at[slot, 0], load_sem.at[slot, 0]),
                pltpu.make_async_copy(ap.at[here], abuf.at[slot, 1], load_sem.at[slot, 1]),
                pltpu.make_async_copy(r.at[here], rbuf.at[slot], load_sem.at[slot, 2]))

    def local_unit(u):
        slot = lax.rem(u, 2)
        here = pl.ds(pl.multiple_of(u * unit, unit), unit)
        for cp in local_loads(u):
            cp.wait()

        @pl.when(u + 1 < NUNIT)
        def _():
            for cp in local_loads(u + 1):
                cp.start()

        def tile(n, _):
            cs = pl.ds(pl.multiple_of(n * tn, tn), tn)
            p0 = jnp.dot(abuf[slot, 0], wl[0, :, cs], preferred_element_type=jnp.float32)
            p1 = jnp.dot(abuf[slot, 1], wl[1, :, cs], preferred_element_type=jnp.float32)
            acc[here, cs] = (rbuf[slot, :, cs].astype(jnp.float32) + p0.astype(jnp.bfloat16).astype(jnp.float32)
                             + p1.astype(jnp.bfloat16).astype(jnp.float32))
            return None

        lax.fori_loop(0, ntile, tile, None)

    def out_copy(u, q, dst, k):
        here = pl.ds(pl.multiple_of(q * unit, unit), unit)
        return pltpu.make_async_copy(obuf.at[lax.rem(u, 2)], dst.at[here], out_sem.at[lax.rem(u, 2)])

    def unit_of(u):
        gs = NUNIT // 2
        b = side * gs
        o = (1 - side) * gs
        end_order = (b + 3, o + 3, b, o + 2, b + 1, o, b + 2, o + 1)
        mid_order = (b + 3, b + 2, o + 3, o + 2, b, o, b + 1, o + 1)
        q = jnp.int32(0)
        for k in range(NUNIT):
            q = q + jnp.where(u == k, jnp.where(end, end_order[k], mid_order[k]), 0)
        return q

    def remote_unit(u, _):
        q = unit_of(u)
        here = pl.ds(pl.multiple_of(q * unit, unit), unit)
        slot = lax.rem(u, 2)
        loads = [pltpu.make_async_copy(ax.at[pl.ds(q * GRP, GRP), b], abuf.at[slot, b].reshape(GRP, ch, kb),
                                       load_sem.at[slot, b]) for b in range(2)]
        for cp in loads:
            cp.start()

        @pl.when(u >= 2)
        def _():
            out_copy(u, q, h_out, 0).wait()

        for cp in loads:
            cp.wait()

        def tile(n, part):
            cs = pl.ds(pl.multiple_of(n * tn, tn), tn)
            p0 = jnp.dot(abuf[slot, 0], wr[0, :, cs], preferred_element_type=jnp.float32)
            p1 = jnp.dot(abuf[slot, 1], wr[1, :, cs], preferred_element_type=jnp.float32)
            v = acc[here, cs] + (p0.astype(jnp.bfloat16).astype(jnp.float32) + p1.astype(jnp.bfloat16).astype(jnp.float32))
            acc[here, cs] = v
            obuf[slot, :, cs] = v.astype(jnp.bfloat16)
            sq = v * v
            for k in range(tn // 128):
                part = part + sq[:, k * 128:(k + 1) * 128]
            return part

        part = lax.fori_loop(0, ntile, tile, jnp.zeros((unit, 128), jnp.float32))
        out_copy(u, q, h_out, 0).start()
        for k in range(unit // 128):
            ss_loc[q, k:k + 1, :] = jnp.sum(part[k * 128:(k + 1) * 128, :].T, axis=0, keepdims=True)
        return None

    def slot_body(i, _):
        comm(i)

        @pl.when(i == LOCAL0 - 1)
        def _():
            own_w.wait()
            wait_bytes(wl.at[1], recv_dw)
            wait_bytes(ap, recv_da)
            for cp in local_loads(0):
                cp.start()

        @pl.when((i >= LOCAL0) & (i < LOCAL0 + NUNIT))
        def _():
            local_unit(i - LOCAL0)

        @pl.when(i == jnp.where(end, END_UNITS[0], MID_UNITS[0]))
        def _():
            wait_bytes(wr.at[1 - c], recv_wd)

        lo = jnp.where(end, step_count(i - 1, END_UNITS), step_count(i - 1, MID_UNITS))
        hi = jnp.where(end, step_count(i, END_UNITS), step_count(i, MID_UNITS))
        lax.fori_loop(lo, hi, remote_unit, None)
        return None

    lax.fori_loop(0, NSLOT, slot_body, None)

    for k in range(1, 4):
        remote(ss_loc, ss_all.at[z], send_ss.at[k - 1], recv_ss.at[z], (x, lax.rem(z + k, 4), t)).start()
    for u in range(NUNIT - 2, NUNIT):
        out_copy(jnp.int32(u), jnp.int32(0), h_out, 0).wait()
    wait_bytes(wl.at[1], send_dw)
    wait_bytes(ap, send_da)
    wait_bytes(wr.at[0], send_wd)
    wait_bytes(wr.at[0, pl.ds(0, kb // 2)], send_wx)
    wait_bytes(wr.at[0, pl.ds(0, kb // 2)], send_yw)

    @pl.when(end)
    def _():
        wait_bytes(ax.at[pl.ds(0, 12)], send_ya)
        wait_bytes(ax.at[pl.ds(0, 8)], send_zi)

    @pl.when(mid)
    def _():
        wait_bytes(ax.at[pl.ds(0, 8)], send_ya)
        wait_bytes(ax.at[pl.ds(0, 16)], send_zi)
        wait_bytes(ax.at[pl.ds(0, 20)], send_zo)

    for k in range(1, 4):
        src = lax.rem(z + k, 4)
        remote(ss_loc, ss_all.at[src], send_ss.at[k - 1], recv_ss.at[src], (x, src, t)).wait_recv()
        remote(ss_loc, ss_all.at[src], send_ss.at[k - 1], recv_ss.at[src], (x, src, t)).wait_send()
    ss_all[z] = ss_loc[...]

    def finish(q, _):
        here = pl.ds(pl.multiple_of(q * unit, unit), unit)
        slot = lax.rem(q, 2)

        @pl.when(q >= 2)
        def _():
            out_copy(q, q, n_out, 1).wait()

        total = ss_all[0, q] + ss_all[1, q] + ss_all[2, q] + ss_all[3, q]
        inv = lax.rsqrt(total / (cols * 4) + EPS_NORM)
        for k in range(unit // 128):
            col = jnp.broadcast_to(inv[k:k + 1, :], (128, 128)).T
            rs = pl.ds(pl.multiple_of(q * unit + k * 128, 128), 128)
            for m in range(cols // 128):
                cs = slice(m * 128, (m + 1) * 128)
                obuf[slot, k * 128:(k + 1) * 128, cs] = (acc[rs, cs] * col * g[:, cs]).astype(jnp.bfloat16)
        out_copy(q, q, n_out, 1).start()
        return None

    lax.fori_loop(0, NUNIT, finish, None)
    for u in range(NUNIT - 2, NUNIT):
        out_copy(jnp.int32(u), jnp.int32(0), n_out, 1).wait()


def solution(mesh):
    def local_step(attn_blk, w_blk, res_blk, gain_blk):
        kb = attn_blk.shape[1]
        rows, cols = res_blk.shape
        unit = rows // NUNIT
        any_spec = pl.BlockSpec(memory_space=pl.ANY)
        bf16, f32 = jnp.bfloat16, jnp.float32
        dma = pltpu.SemaphoreType.DMA
        outs = pl.pallas_call(
            kernel,
            out_shape=(
                jax.ShapeDtypeStruct((rows, cols), bf16),
                jax.ShapeDtypeStruct((rows, cols), bf16),
                jax.ShapeDtypeStruct((NCH, 2, rows // NCH, kb), bf16),
                jax.ShapeDtypeStruct((rows, kb), bf16),
            ),
            in_specs=[any_spec, any_spec, any_spec, pl.BlockSpec(memory_space=pltpu.VMEM)],
            out_specs=(any_spec,) * 4,
            scratch_shapes=[
                pltpu.VMEM((2, kb, cols), bf16),
                pltpu.VMEM((2, kb, cols), bf16),
                pltpu.VMEM((rows, cols), f32),
                pltpu.VMEM((2, 2, unit, kb), bf16),
                pltpu.VMEM((2, unit, cols), bf16),
                pltpu.VMEM((2, unit, cols), bf16),
                pltpu.VMEM((NUNIT, unit // 128, 128), f32),
                pltpu.VMEM((4, NUNIT, unit // 128, 128), f32),
                dma((NCH,)), dma, dma, dma, dma,
                dma((NWC,)), dma((NWC,)), dma, dma, dma,
                dma, dma, dma, dma,
                dma((2, 3)), dma, dma((2,)),
                dma((3,)), dma((4,)),
            ],
            compiler_params=pltpu.CompilerParams(
                collective_id=0, has_side_effects=True, vmem_limit_bytes=64 * 1024 * 1024 - 65536),
            name="gather_project_norm",
        )(attn_blk, w_blk, res_blk, gain_blk.reshape(1, cols))
        return outs[0], outs[1]

    row_spec = P(("dp", "tp"), "tp2")
    return jax.shard_map(local_step, mesh=mesh, in_specs=(P("dp", "tp"), P("tp", "tp2"), row_spec, P("tp2")), out_specs=(row_spec, row_spec), check_vma=False)
```

```python
import functools

import jax
import jax.numpy as jnp
from jax import lax
from jax.experimental import pallas as pl
from jax.experimental.pallas import tpu as pltpu
from jax.sharding import PartitionSpec as P

EPS_NORM = 1e-6
MESH = pl.DeviceIdType.MESH
NCH = 32
NWC = 8
GRP = 4
NUNIT = NCH // GRP
AHEAD = 3
NSLOT = 21
LOCAL0 = 2


def step_count(i, slots):
    n = jnp.int32(0)
    for s in slots:
        n = n + jnp.where(i >= s, 1, 0)
    return n


END_UNITS = (10, 10, 12, 13, 16, 17, 19, 20)
MID_UNITS = (17, 18, 19, 19, 19, 20, 20, 20)


def kernel(a, w, r, acc, ss_all, ax, ap, wl, wr, abuf, rbuf, ss_loc,
           recv_a, send_ya, send_yw, send_zi, send_zo, recv_wy, recv_wx, recv_wd, send_wx, send_wd,
           recv_da, recv_dw, send_da, send_dw, load_sem, load_w, send_ss, recv_ss):
    x = lax.axis_index("dp")
    z = lax.axis_index("tp2")
    t = lax.axis_index("tp")
    y = t // 2
    c = t % 2
    rows, cols = acc.shape
    kb = w.shape[0]
    ch = rows // NCH
    wch = kb // 2 // NWC
    unit = ch * GRP
    side = z // 2
    end = (z == 0) | (z == 3)
    mid = (z == 1) | (z == 2)
    base = side * (NCH // 2)
    other = (1 - side) * (NCH // 2)
    z_in = jnp.where(side == 0, z + 1, z - 1)
    z_out = jnp.where(side == 0, z - 1, z + 1)

    partner = (x, z, y * 2 + 1 - c)
    x_peer = (1 - x, z, t)
    y_same = (x, z, (1 - y) * 2 + c)
    y_cross = (x, z, (1 - y) * 2 + 1 - c)

    def remote(src, dst, send, recv, dev):
        return pltpu.make_async_remote_copy(
            src_ref=src, dst_ref=dst, send_sem=send, recv_sem=recv, device_id=dev, device_id_type=MESH)

    def wait_bytes(ref, sem):
        pltpu.make_async_copy(ref, ref, sem).wait()

    barrier = pltpu.get_barrier_semaphore()
    for dev in (partner, x_peer, y_same, y_cross):
        pl.semaphore_signal(barrier, inc=1, device_id=dev, device_id_type=MESH)
    for k in range(1, 4):
        pl.semaphore_signal(barrier, inc=1, device_id=(x, lax.rem(z + k, 4), t), device_id_type=MESH)
    pl.semaphore_wait(barrier, 7)

    def mp(start, j):
        return start + NCH // 4 + lax.rem(j + NCH // 8, NCH // 4)

    def send_y_a(q):
        for cc in range(2):
            row = ((1 - y) * 2 + cc) * rows + q * ch
            remote(a.at[pl.ds(pl.multiple_of(row, ch), ch)], ax.at[q, c], send_ya, recv_a.at[q],
                   (x, z, (1 - y) * 2 + cc)).start()

    def w_rows(half, i):
        return pl.ds(pl.multiple_of(half * (kb // 2) + i * wch, wch), wch)

    def send_y_w(i):
        remote(w.at[w_rows(x, i)], wr.at[c, w_rows(x, i)], send_yw, recv_wy.at[i], y_same).start()

    def y_sends(i):
        @pl.when(end & (i < NWC))
        def _():
            send_y_w(i)

        @pl.when(end & (i >= NWC) & (i < NWC + 12))
        def _():
            send_y_a(base + i - NWC)

        @pl.when(mid & (i < 8))
        def _():
            send_y_a(mp(base, i))

        @pl.when(mid & (i >= 8) & (i < 8 + NWC))
        def _():
            send_y_w(i - 8)

    lax.fori_loop(0, AHEAD, lambda i, _: (y_sends(i), None)[1], None)

    remote(w, wl.at[1], send_dw, recv_dw, partner).start()
    prow = pl.ds(pl.multiple_of((y * 2 + 1 - c) * rows, rows), rows)
    remote(a.at[prow], ap, send_da, recv_da, partner).start()
    own_w = pltpu.make_async_copy(w, wl.at[0], load_w)
    own_w.start()

    def arrive(q):
        wait_bytes(ax.at[q], recv_a.at[q])

    def pass_in(q):
        remote(ax.at[q], ax.at[q], send_zi, recv_a.at[q], (x, z_in, t)).start()

    def pass_out(q):
        remote(ax.at[q], ax.at[q], send_zo, recv_a.at[q], (x, z_out, t)).start()

    def w_from_y(i):
        part = wr.at[c, w_rows(x, i)]
        wait_bytes(part, recv_wy.at[i])
        remote(part, part, send_wx, recv_wx.at[i], x_peer).start()
        remote(part, part, send_wd, recv_wd, partner).start()

    def w_from_x(i):
        part = wr.at[c, w_rows(1 - x, i)]
        wait_bytes(part, recv_wx.at[i])
        remote(part, part, send_wd, recv_wd, partner).start()

    def comm(i):
        y_sends(i + AHEAD)

        @pl.when(end)
        def _():
            @pl.when(i < NWC)
            def _():
                w_from_y(i)

            @pl.when((i >= NWC) & (i < NWC + 12))
            def _():
                q = base + i - NWC
                arrive(q)

                @pl.when(i < NWC + 8)
                def _():
                    pass_in(q)

            @pl.when((i >= 1) & (i < 1 + NWC))
            def _():
                w_from_x(i - 1)

            j = i - 1

            @pl.when((j >= 0) & (j < 4))
            def _():
                arrive(mp(base, j))

            @pl.when((j >= 4) & (j < 12))
            def _():
                arrive(mp(other, j - 4))

            @pl.when((j >= 12) & (j < 20))
            def _():
                arrive(other + j - 12)

        @pl.when(mid)
        def _():
            @pl.when(i < 8)
            def _():
                q = mp(base, i)
                arrive(q)

                @pl.when(i < 4)
                def _():
                    pass_out(q)

                pass_in(q)

            @pl.when((i >= 1) & (i < 9))
            def _():
                q = mp(other, i - 1)
                arrive(q)
                pass_out(q)

            @pl.when((i >= 9) & (i < 17))
            def _():
                q = base + i - 9
                arrive(q)
                pass_in(q)

            @pl.when((i >= 10) & (i < 18))
            def _():
                q = other + i - 10
                arrive(q)
                pass_out(q)

            @pl.when((i >= 8) & (i < 8 + NWC))
            def _():
                w_from_y(i - 8)

            @pl.when((i >= 9) & (i < 9 + NWC))
            def _():
                w_from_x(i - 9)

    tn = min(512, cols)
    ntile = cols // tn

    def local_loads(u):
        slot = lax.rem(u, 2)
        here = pl.ds(pl.multiple_of(u * unit, unit), unit)
        mine = pl.ds(pl.multiple_of(t * rows + u * unit, unit), unit)
        return (pltpu.make_async_copy(a.at[mine], abuf.at[slot, 0], load_sem.at[slot, 0]),
                pltpu.make_async_copy(ap.at[here], abuf.at[slot, 1], load_sem.at[slot, 1]),
                pltpu.make_async_copy(r.at[here], rbuf.at[slot], load_sem.at[slot, 2]))

    def local_unit(u):
        slot = lax.rem(u, 2)
        here = pl.ds(pl.multiple_of(u * unit, unit), unit)
        for cp in local_loads(u):
            cp.wait()

        @pl.when(u + 1 < NUNIT)
        def _():
            for cp in local_loads(u + 1):
                cp.start()

        def tile(n, _):
            cs = pl.ds(pl.multiple_of(n * tn, tn), tn)
            p0 = jnp.dot(abuf[slot, 0], wl[0, :, cs], preferred_element_type=jnp.float32)
            p1 = jnp.dot(abuf[slot, 1], wl[1, :, cs], preferred_element_type=jnp.float32)
            acc[here, cs] = (rbuf[slot, :, cs].astype(jnp.float32) + p0.astype(jnp.bfloat16).astype(jnp.float32)
                             + p1.astype(jnp.bfloat16).astype(jnp.float32))
            return None

        lax.fori_loop(0, ntile, tile, None)

    def unit_of(u):
        gs = NUNIT // 2
        b = side * gs
        o = (1 - side) * gs
        end_order = (b + 3, o + 3, b, o + 2, b + 1, o, b + 2, o + 1)
        mid_order = (b + 3, b + 2, o + 3, o + 2, b, o, b + 1, o + 1)
        q = jnp.int32(0)
        for k in range(NUNIT):
            q = q + jnp.where(u == k, jnp.where(end, end_order[k], mid_order[k]), 0)
        return q

    def remote_unit(u, _):
        q = unit_of(u)
        here = pl.ds(pl.multiple_of(q * unit, unit), unit)
        slot = lax.rem(u, 2)
        loads = [pltpu.make_async_copy(ax.at[pl.ds(q * GRP, GRP), b], abuf.at[slot, b].reshape(GRP, ch, kb),
                                       load_sem.at[slot, b]) for b in range(2)]
        for cp in loads:
            cp.start()

        for cp in loads:
            cp.wait()

        def tile(n, part):
            cs = pl.ds(pl.multiple_of(n * tn, tn), tn)
            p0 = jnp.dot(abuf[slot, 0], wr[0, :, cs], preferred_element_type=jnp.float32)
            p1 = jnp.dot(abuf[slot, 1], wr[1, :, cs], preferred_element_type=jnp.float32)
            v = acc[here, cs] + (p0.astype(jnp.bfloat16).astype(jnp.float32) + p1.astype(jnp.bfloat16).astype(jnp.float32))
            acc[here, cs] = v
            sq = v * v
            for k in range(tn // 128):
                part = part + sq[:, k * 128:(k + 1) * 128]
            return part

        part = lax.fori_loop(0, ntile, tile, jnp.zeros((unit, 128), jnp.float32))
        for k in range(unit // 128):
            ss_loc[q, k:k + 1, :] = jnp.sum(part[k * 128:(k + 1) * 128, :].T, axis=0, keepdims=True)
        return None

    def slot_body(i, _):
        comm(i)

        @pl.when(i == LOCAL0 - 1)
        def _():
            own_w.wait()
            wait_bytes(wl.at[1], recv_dw)
            wait_bytes(ap, recv_da)
            for cp in local_loads(0):
                cp.start()

        @pl.when((i >= LOCAL0) & (i < LOCAL0 + NUNIT))
        def _():
            local_unit(i - LOCAL0)

        @pl.when(i == jnp.where(end, END_UNITS[0], MID_UNITS[0]))
        def _():
            wait_bytes(wr.at[1 - c], recv_wd)

        lo = jnp.where(end, step_count(i - 1, END_UNITS), step_count(i - 1, MID_UNITS))
        hi = jnp.where(end, step_count(i, END_UNITS), step_count(i, MID_UNITS))
        lax.fori_loop(lo, hi, remote_unit, None)
        return None

    lax.fori_loop(0, NSLOT, slot_body, None)

    for k in range(1, 4):
        remote(ss_loc, ss_all.at[z], send_ss.at[k - 1], recv_ss.at[z], (x, lax.rem(z + k, 4), t)).start()
    wait_bytes(wl.at[1], send_dw)
    wait_bytes(ap, send_da)
    wait_bytes(wr.at[0], send_wd)
    wait_bytes(wr.at[0, pl.ds(0, kb // 2)], send_wx)
    wait_bytes(wr.at[0, pl.ds(0, kb // 2)], send_yw)

    @pl.when(end)
    def _():
        wait_bytes(ax.at[pl.ds(0, 12)], send_ya)
        wait_bytes(ax.at[pl.ds(0, 8)], send_zi)

    @pl.when(mid)
    def _():
        wait_bytes(ax.at[pl.ds(0, 8)], send_ya)
        wait_bytes(ax.at[pl.ds(0, 16)], send_zi)
        wait_bytes(ax.at[pl.ds(0, 20)], send_zo)

    for k in range(1, 4):
        src = lax.rem(z + k, 4)
        remote(ss_loc, ss_all.at[src], send_ss.at[k - 1], recv_ss.at[src], (x, src, t)).wait_recv()
        remote(ss_loc, ss_all.at[src], send_ss.at[k - 1], recv_ss.at[src], (x, src, t)).wait_send()
    ss_all[z] = ss_loc[...]

def finish_kernel(h, ss, g, h_out, n_out, hbuf, nbuf, sem):
    rows, cols = h.shape
    unit = rows // NUNIT
    nfin = NUNIT

    def copies(q):
        slot = lax.rem(q, 2)
        here = pl.ds(pl.multiple_of(q * unit, unit), unit)
        return (pltpu.make_async_copy(hbuf.at[slot], h_out.at[here], sem.at[slot, 0]),
                pltpu.make_async_copy(nbuf.at[slot], n_out.at[here], sem.at[slot, 1]))

    def step(q, _):
        slot = lax.rem(q, 2)

        @pl.when(q >= 2)
        def _():
            for cp in copies(q - 2):
                cp.wait()

        total = ss[0, q] + ss[1, q] + ss[2, q] + ss[3, q]
        inv = lax.rsqrt(total / (cols * 4) + EPS_NORM)
        for k in range(unit // 128):
            col = jnp.broadcast_to(inv[k:k + 1, :], (128, 128)).T
            rs = pl.ds(pl.multiple_of(q * unit + k * 128, 128), 128)
            for m in range(cols // 128):
                cs = slice(m * 128, (m + 1) * 128)
                v = h[rs, cs]
                hbuf[slot, k * 128:(k + 1) * 128, cs] = v.astype(jnp.bfloat16)
                nbuf[slot, k * 128:(k + 1) * 128, cs] = (v * col * g[:, cs]).astype(jnp.bfloat16)
        for cp in copies(q):
            cp.start()
        return None

    lax.fori_loop(0, nfin, step, None)
    for q in (nfin - 2, nfin - 1):
        for cp in copies(jnp.int32(q)):
            cp.wait()


def solution(mesh):
    def local_step(attn_blk, w_blk, res_blk, gain_blk):
        kb = attn_blk.shape[1]
        rows, cols = res_blk.shape
        unit = rows // NUNIT
        any_spec = pl.BlockSpec(memory_space=pl.ANY)
        vmem_spec = pl.BlockSpec(memory_space=pltpu.VMEM)
        bf16, f32 = jnp.bfloat16, jnp.float32
        dma = pltpu.SemaphoreType.DMA
        h, ss, _, _ = pl.pallas_call(
            kernel,
            out_shape=(
                pltpu.VMEM((rows, cols), f32),
                pltpu.VMEM((4, NUNIT, unit // 128, 128), f32),
                jax.ShapeDtypeStruct((NCH, 2, rows // NCH, kb), bf16),
                jax.ShapeDtypeStruct((rows, kb), bf16),
            ),
            in_specs=[any_spec, any_spec, any_spec],
            out_specs=(vmem_spec, vmem_spec, any_spec, any_spec),
            scratch_shapes=[
                pltpu.VMEM((2, kb, cols), bf16),
                pltpu.VMEM((2, kb, cols), bf16),
                pltpu.VMEM((2, 2, unit, kb), bf16),
                pltpu.VMEM((2, unit, cols), bf16),
                pltpu.VMEM((NUNIT, unit // 128, 128), f32),
                dma((NCH,)), dma, dma, dma, dma,
                dma((NWC,)), dma((NWC,)), dma, dma, dma,
                dma, dma, dma, dma,
                dma((2, 3)), dma,
                dma((3,)), dma((4,)),
            ],
            compiler_params=pltpu.CompilerParams(
                collective_id=0, has_side_effects=True, vmem_limit_bytes=44 * 1024 * 1024),
            name="gather_project",
        )(attn_blk, w_blk, res_blk)
        return pl.pallas_call(
            finish_kernel,
            out_shape=(jax.ShapeDtypeStruct((rows, cols), bf16),) * 2,
            in_specs=[vmem_spec, vmem_spec, vmem_spec],
            out_specs=(any_spec, any_spec),
            scratch_shapes=[pltpu.VMEM((2, unit, cols), bf16), pltpu.VMEM((2, unit, cols), bf16), dma((2, 2))],
            compiler_params=pltpu.CompilerParams(vmem_limit_bytes=8 * 1024 * 1024),
            name="norm_store",
        )(h, ss, gain_blk.reshape(1, cols))

    row_spec = P(("dp", "tp"), "tp2")
    return jax.shard_map(local_step, mesh=mesh, in_specs=(P("dp", "tp"), P("tp", "tp2"), row_spec, P("tp2")), out_specs=(row_spec, row_spec), check_vma=False)
```

```python
import functools

import jax
import jax.numpy as jnp
from jax import lax
from jax.experimental import pallas as pl
from jax.experimental.pallas import tpu as pltpu
from jax.sharding import PartitionSpec as P

EPS_NORM = 1e-6
MESH = pl.DeviceIdType.MESH
NCH = 64
FAR = NCH // 4
NEAR = NCH // 8
NWC = 8
WS = 2 * NWC
NUNIT = 8
GRP = NCH // NUNIT
AHEAD = 6
NSLOT = 2 * FAR + NEAR + 1
LOCAL0 = 6
LOADS = 16
WREADY = WS + 2
COLS0 = FAR + 4


def step_count(i, slots):
    n = jnp.int32(0)
    for s in slots:
        n = n + jnp.where(i >= s, 1, 0)
    return n


END_UNITS = (19, 20, 24, 25, 32, 33, 39, 40)
MID_UNITS = (35, 36, 37, 38)


def kernel(a, w, r, acc, ss_all, ax, ap, wl, wr, abuf, rbuf, ss_loc,
           recv_a, send_ya, send_yw, send_zi, send_zo, recv_wy, recv_wx, recv_wd, send_wx, send_wd,
           recv_da, recv_dw, send_da, send_dw, load_sem, load_w, load_a, send_ss, recv_ss):
    x = lax.axis_index("dp")
    z = lax.axis_index("tp2")
    t = lax.axis_index("tp")
    y = t // 2
    c = t % 2
    rows, cols = acc.shape
    kb = w.shape[0]
    ch = rows // NCH
    wch = cols // NWC
    unit = ch * GRP
    side = z // 2
    end = (z == 0) | (z == 3)
    mid = (z == 1) | (z == 2)
    base = side * (NCH // 2)
    other = (1 - side) * (NCH // 2)
    z_in = jnp.where(side == 0, z + 1, z - 1)
    z_out = jnp.where(side == 0, z - 1, z + 1)

    partner = (x, z, y * 2 + 1 - c)
    x_peer = (1 - x, z, t)
    y_same = (x, z, (1 - y) * 2 + c)
    y_cross = (x, z, (1 - y) * 2 + 1 - c)

    def remote(src, dst, send, recv, dev):
        return pltpu.make_async_remote_copy(
            src_ref=src, dst_ref=dst, send_sem=send, recv_sem=recv, device_id=dev, device_id_type=MESH)

    def wait_bytes(ref, sem):
        pltpu.make_async_copy(ref, ref, sem).wait()

    barrier = pltpu.get_barrier_semaphore()
    for dev in (partner, x_peer, y_same, y_cross):
        pl.semaphore_signal(barrier, inc=1, device_id=dev, device_id_type=MESH)
    for k in range(1, 4):
        pl.semaphore_signal(barrier, inc=1, device_id=(x, lax.rem(z + k, 4), t), device_id_type=MESH)
    pl.semaphore_wait(barrier, 7)

    def mp(start, j):
        return start + FAR + lax.rem(j + NEAR, FAR)

    def send_y_a(q):
        for cc in range(2):
            row = ((1 - y) * 2 + cc) * rows + q * ch
            remote(a.at[pl.ds(pl.multiple_of(row, ch), ch)], ax.at[q, c], send_ya, recv_a.at[q],
                   (x, z, (1 - y) * 2 + cc)).start()

    def w_part(half, n):
        return (pl.ds(pl.multiple_of(half * (kb // 2), kb // 2), kb // 2), pl.ds(pl.multiple_of(n * wch, wch), wch))

    def send_y_w(n):
        rs, cs = w_part(x, n)
        remote(w.at[rs, cs], wr.at[c, rs, cs], send_yw, recv_wy.at[n], y_same).start()

    def y_sends(i):
        iw = jnp.where(end, i, i - FAR)
        ia = jnp.where(end, i - WS, i)

        @pl.when((iw >= 0) & (iw < WS) & (lax.rem(iw, 2) == 0))
        def _():
            send_y_w(iw // 2)

        @pl.when(end & (ia >= 0) & (ia < FAR + NEAR))
        def _():
            send_y_a(base + ia)

        @pl.when(mid & (ia < FAR))
        def _():
            send_y_a(mp(base, ia))

    lax.fori_loop(0, AHEAD, lambda i, _: (y_sends(i), None)[1], None)

    remote(w, wl.at[1], send_dw, recv_dw, partner).start()
    prow = pl.ds(pl.multiple_of((y * 2 + 1 - c) * rows, rows), rows)
    remote(a.at[prow], ap, send_da, recv_da, partner).start()
    own_w = pltpu.make_async_copy(w, wl.at[0], load_w)
    own_w.start()

    def load(q):
        here = pl.ds(pl.multiple_of(q * ch, ch), ch)
        for b in range(2):
            pltpu.make_async_copy(ax.at[q, b], wl.at[b, here], load_a.at[q // GRP]).start()

    def arrive(q, i):
        wait_bytes(ax.at[q], recv_a.at[q])

        @pl.when(i >= LOADS)
        def _():
            load(q)

    def pass_in(q):
        remote(ax.at[q], ax.at[q], send_zi, recv_a.at[q], (x, z_in, t)).start()

    def pass_out(q):
        remote(ax.at[q], ax.at[q], send_zo, recv_a.at[q], (x, z_out, t)).start()

    def w_from_y(n):
        rs, cs = w_part(x, n)
        part = wr.at[c, rs, cs]
        wait_bytes(part, recv_wy.at[n])
        remote(part, part, send_wx, recv_wx.at[n], x_peer).start()
        remote(part, part, send_wd, recv_wd.at[n], partner).start()

    def w_from_x(n):
        rs, cs = w_part(1 - x, n)
        part = wr.at[c, rs, cs]
        wait_bytes(part, recv_wx.at[n])
        remote(part, part, send_wd, recv_wd.at[n], partner).start()

    def w_from_partner(n):
        cs = pl.ds(pl.multiple_of(n * wch, wch), wch)
        wait_bytes(wr.at[1 - c, :, cs], recv_wd.at[n])

    def z_chunk(j):
        return jnp.where(j < NEAR, mp(base, j), jnp.where(j < NEAR + FAR, mp(other, j - NEAR), other + j - NEAR - FAR))

    def comm(i):
        y_sends(i + AHEAD)
        iw = jnp.where(end, i, i - FAR)
        odd = lax.rem(i, 2) == 1

        @pl.when(odd & (iw >= 1) & (iw < WS))
        def _():
            w_from_y(iw // 2)

        @pl.when(odd & (iw >= 3) & (iw < WS + 2))
        def _():
            w_from_x((iw - 3) // 2)

        @pl.when(end)
        def _():
            @pl.when((i >= WS) & (i < WS + FAR + NEAR))
            def _():
                q = base + i - WS
                arrive(q, i)

                @pl.when(i < WS + FAR)
                def _():
                    pass_in(q)

            @pl.when((i >= 1) & (i < 1 + 2 * FAR + NEAR))
            def _():
                arrive(z_chunk(i - 1), i)

        @pl.when(mid)
        def _():
            @pl.when(i < FAR)
            def _():
                q = mp(base, i)
                arrive(q, i)

                @pl.when(i < NEAR)
                def _():
                    pass_out(q)

                pass_in(q)

            @pl.when((i >= 1) & (i < 1 + FAR))
            def _():
                q = mp(other, i - 1)
                arrive(q, i)
                pass_out(q)

            @pl.when((i >= WS + 1) & (i < WS + 1 + FAR))
            def _():
                q = base + i - WS - 1
                arrive(q, i)
                pass_in(q)

            @pl.when((i >= WS + 2) & (i < WS + 2 + FAR))
            def _():
                q = other + i - WS - 2
                arrive(q, i)
                pass_out(q)

    def early_loads():
        def from_z(j, _):
            load(jnp.where(end, z_chunk(j), mp(other, j)))
            return None

        lax.fori_loop(0, LOADS - 1, from_z, None)

        def from_y(j, _):
            load(mp(base, j))
            return None

        lax.fori_loop(0, jnp.where(end, 0, LOADS), from_y, None)

    tn = min(512, cols)
    ntile = cols // tn

    def local_loads(u):
        slot = lax.rem(u, 2)
        here = pl.ds(pl.multiple_of(u * unit, unit), unit)
        mine = pl.ds(pl.multiple_of(t * rows + u * unit, unit), unit)
        return (pltpu.make_async_copy(a.at[mine], abuf.at[slot, 0], load_sem.at[slot, 0]),
                pltpu.make_async_copy(ap.at[here], abuf.at[slot, 1], load_sem.at[slot, 1]),
                pltpu.make_async_copy(r.at[here], rbuf.at[slot], load_sem.at[slot, 2]))

    def local_unit(u):
        slot = lax.rem(u, 2)
        here = pl.ds(pl.multiple_of(u * unit, unit), unit)
        for cp in local_loads(u):
            cp.wait()

        @pl.when(u + 1 < NUNIT)
        def _():
            for cp in local_loads(u + 1):
                cp.start()

        def tile(n, _):
            cs = pl.ds(pl.multiple_of(n * tn, tn), tn)
            p0 = jnp.dot(abuf[slot, 0], wl[0, :, cs], preferred_element_type=jnp.float32)
            p1 = jnp.dot(abuf[slot, 1], wl[1, :, cs], preferred_element_type=jnp.float32)
            acc[here, cs] = (rbuf[slot, :, cs].astype(jnp.float32) + p0.astype(jnp.bfloat16).astype(jnp.float32)
                             + p1.astype(jnp.bfloat16).astype(jnp.float32))
            return None

        lax.fori_loop(0, ntile, tile, None)

    gs = NUNIT // 2

    def unit_of(u):
        b = side * gs
        o = (1 - side) * gs
        end_order = (b + 3, o + 3, b, o + 2, b + 1, o, b + 2, o + 1)
        mid_order = (b, o, b + 1, o + 1, 0, 0, 0, 0)
        q = jnp.int32(0)
        for k in range(NUNIT):
            q = q + jnp.where(u == k, jnp.where(end, end_order[k], mid_order[k]), 0)
        return q

    def wait_load(q):
        here = pl.ds(pl.multiple_of(q * unit, unit), unit)
        wait_bytes(wl.at[:, here], load_a.at[q])

    def far_product(here, cs):
        p0 = jnp.dot(wl[0, here, :], wr[0, :, cs], preferred_element_type=jnp.float32)
        p1 = jnp.dot(wl[1, here, :], wr[1, :, cs], preferred_element_type=jnp.float32)
        v = acc[here, cs] + (p0.astype(jnp.bfloat16).astype(jnp.float32) + p1.astype(jnp.bfloat16).astype(jnp.float32))
        acc[here, cs] = v
        return v

    def squares(v):
        sq = v * v
        part = sq[:, :128]
        for k in range(1, sq.shape[1] // 128):
            part = part + sq[:, k * 128:(k + 1) * 128]
        return part

    def keep_squares(q, part):
        for k in range(unit // 128):
            ss_loc[q, k:k + 1, :] = jnp.sum(part[k * 128:(k + 1) * 128, :].T, axis=0, keepdims=True)

    def remote_unit(u, _):
        q = unit_of(u)
        here = pl.ds(pl.multiple_of(q * unit, unit), unit)
        wait_load(q)

        def tile(n, part):
            cs = pl.ds(pl.multiple_of(n * tn, tn), tn)
            return part + squares(far_product(here, cs))

        keep_squares(q, lax.fori_loop(0, ntile, tile, jnp.zeros((unit, 128), jnp.float32)))
        return None

    def column_unit(k):
        return jnp.where(k < 2, side, 1 - side) * gs + 2 + lax.rem(k, 2)

    def column_step(n):
        w_from_partner(n)

        @pl.when(n == 0)
        def _():
            for k in range(4):
                wait_load(column_unit(jnp.int32(k)))

        cs = pl.ds(pl.multiple_of(n * wch, wch), wch)

        def rows_of(k, _):
            here = pl.ds(pl.multiple_of(column_unit(k) * unit, unit), unit)
            far_product(here, cs)
            return None

        lax.fori_loop(0, 4, rows_of, None)

        @pl.when(n == NWC - 1)
        def _():
            def sums(k, _):
                q = column_unit(k)
                here = pl.ds(pl.multiple_of(q * unit, unit), unit)

                def tile(m, part):
                    return part + squares(acc[here, pl.ds(pl.multiple_of(m * tn, tn), tn)])

                keep_squares(q, lax.fori_loop(0, ntile, tile, jnp.zeros((unit, 128), jnp.float32)))
                return None

            lax.fori_loop(0, 4, sums, None)

    def slot_body(i, _):
        @pl.when(i == LOADS)
        def _():
            early_loads()

        comm(i)

        @pl.when(i == LOCAL0 - 1)
        def _():
            own_w.wait()
            wait_bytes(wl.at[1], recv_dw)
            wait_bytes(ap, recv_da)
            for cp in local_loads(0):
                cp.start()

        @pl.when((i >= LOCAL0) & (i < LOCAL0 + NUNIT))
        def _():
            local_unit(i - LOCAL0)

        @pl.when(end & (i == WREADY))
        def _():
            lax.fori_loop(0, NWC, lambda n, _: (w_from_partner(n), None)[1], None)

        jc = i - COLS0

        @pl.when(mid & (jc >= 0) & (jc < WS) & (lax.rem(jc, 2) == 0))
        def _():
            column_step(jc // 2)

        lo = jnp.where(end, step_count(i - 1, END_UNITS), step_count(i - 1, MID_UNITS))
        hi = jnp.where(end, step_count(i, END_UNITS), step_count(i, MID_UNITS))
        lax.fori_loop(lo, hi, remote_unit, None)
        return None

    lax.fori_loop(0, NSLOT, slot_body, None)

    for k in range(1, 4):
        remote(ss_loc, ss_all.at[z], send_ss.at[k - 1], recv_ss.at[z], (x, lax.rem(z + k, 4), t)).start()
    wait_bytes(wl.at[1], send_dw)
    wait_bytes(ap, send_da)
    wait_bytes(wr.at[0], send_wd)
    wait_bytes(wr.at[0, pl.ds(0, kb // 2)], send_wx)
    wait_bytes(wr.at[0, pl.ds(0, kb // 2)], send_yw)

    @pl.when(end)
    def _():
        wait_bytes(ax.at[pl.ds(0, FAR + NEAR)], send_ya)
        wait_bytes(ax.at[pl.ds(0, FAR)], send_zi)

    @pl.when(mid)
    def _():
        wait_bytes(ax.at[pl.ds(0, FAR)], send_ya)
        wait_bytes(ax.at[pl.ds(0, 2 * FAR)], send_zi)
        wait_bytes(ax.at[pl.ds(0, 2 * FAR + NEAR)], send_zo)

    for k in range(1, 4):
        src = lax.rem(z + k, 4)
        remote(ss_loc, ss_all.at[src], send_ss.at[k - 1], recv_ss.at[src], (x, src, t)).wait_recv()
        remote(ss_loc, ss_all.at[src], send_ss.at[k - 1], recv_ss.at[src], (x, src, t)).wait_send()
    ss_all[z] = ss_loc[...]

def finish_kernel(h, ss, g, h_out, n_out, hbuf, nbuf, sem):
    rows, cols = h.shape
    unit = rows // NUNIT
    nfin = NUNIT

    def copies(q):
        slot = lax.rem(q, 2)
        here = pl.ds(pl.multiple_of(q * unit, unit), unit)
        return (pltpu.make_async_copy(hbuf.at[slot], h_out.at[here], sem.at[slot, 0]),
                pltpu.make_async_copy(nbuf.at[slot], n_out.at[here], sem.at[slot, 1]))

    def step(q, _):
        slot = lax.rem(q, 2)

        @pl.when(q >= 2)
        def _():
            for cp in copies(q - 2):
                cp.wait()

        total = ss[0, q] + ss[1, q] + ss[2, q] + ss[3, q]
        inv = lax.rsqrt(total / (cols * 4) + EPS_NORM)
        for k in range(unit // 128):
            col = jnp.broadcast_to(inv[k:k + 1, :], (128, 128)).T
            rs = pl.ds(pl.multiple_of(q * unit + k * 128, 128), 128)
            for m in range(cols // 128):
                cs = slice(m * 128, (m + 1) * 128)
                v = h[rs, cs]
                hbuf[slot, k * 128:(k + 1) * 128, cs] = v.astype(jnp.bfloat16)
                nbuf[slot, k * 128:(k + 1) * 128, cs] = (v * col * g[:, cs]).astype(jnp.bfloat16)
        for cp in copies(q):
            cp.start()
        return None

    lax.fori_loop(0, nfin, step, None)
    for q in (nfin - 2, nfin - 1):
        for cp in copies(jnp.int32(q)):
            cp.wait()


def solution(mesh):
    def local_step(attn_blk, w_blk, res_blk, gain_blk):
        kb = attn_blk.shape[1]
        rows, cols = res_blk.shape
        unit = rows // NUNIT
        any_spec = pl.BlockSpec(memory_space=pl.ANY)
        vmem_spec = pl.BlockSpec(memory_space=pltpu.VMEM)
        bf16, f32 = jnp.bfloat16, jnp.float32
        dma = pltpu.SemaphoreType.DMA
        h, ss, _, _ = pl.pallas_call(
            kernel,
            out_shape=(
                pltpu.VMEM((rows, cols), f32),
                pltpu.VMEM((4, NUNIT, unit // 128, 128), f32),
                jax.ShapeDtypeStruct((NCH, 2, rows // NCH, kb), bf16),
                jax.ShapeDtypeStruct((rows, kb), bf16),
            ),
            in_specs=[any_spec, any_spec, any_spec],
            out_specs=(vmem_spec, vmem_spec, any_spec, any_spec),
            scratch_shapes=[
                pltpu.VMEM((2, kb, cols), bf16),
                pltpu.VMEM((2, kb, cols), bf16),
                pltpu.VMEM((2, 2, unit, kb), bf16),
                pltpu.VMEM((2, unit, cols), bf16),
                pltpu.VMEM((NUNIT, unit // 128, 128), f32),
                dma((NCH,)), dma, dma, dma, dma,
                dma((NWC,)), dma((NWC,)), dma((NWC,)), dma, dma,
                dma, dma, dma, dma,
                dma((2, 3)), dma, dma((NUNIT,)),
                dma((3,)), dma((4,)),
            ],
            compiler_params=pltpu.CompilerParams(
                collective_id=0, has_side_effects=True, vmem_limit_bytes=44 * 1024 * 1024),
            name="gather_project",
        )(attn_blk, w_blk, res_blk)
        return pl.pallas_call(
            finish_kernel,
            out_shape=(jax.ShapeDtypeStruct((rows, cols), bf16),) * 2,
            in_specs=[vmem_spec, vmem_spec, vmem_spec],
            out_specs=(any_spec, any_spec),
            scratch_shapes=[pltpu.VMEM((2, unit, cols), bf16), pltpu.VMEM((2, unit, cols), bf16), dma((2, 2))],
            compiler_params=pltpu.CompilerParams(vmem_limit_bytes=8 * 1024 * 1024),
            name="norm_store",
        )(h, ss, gain_blk.reshape(1, cols))

    row_spec = P(("dp", "tp"), "tp2")
    return jax.shard_map(local_step, mesh=mesh, in_specs=(P("dp", "tp"), P("tp", "tp2"), row_spec, P("tp2")), out_specs=(row_spec, row_spec), check_vma=False)
```

```python
import functools

import jax
import jax.numpy as jnp
from jax import lax
from jax.experimental import pallas as pl
from jax.experimental.pallas import tpu as pltpu
from jax.sharding import PartitionSpec as P

EPS_NORM = 1e-6
MESH = pl.DeviceIdType.MESH
NCH = 64
FAR = NCH // 4
NEAR = NCH // 8
NWC = 8
WS = 2 * NWC
NUNIT = 8
GRP = NCH // NUNIT
AHEAD = 12
NSLOT = 2 * FAR + NEAR + 1
LOCAL0 = 6
LOADS = 16
WREADY = WS + 2
COLS0 = FAR + 4


def step_count(i, slots):
    n = jnp.int32(0)
    for s in slots:
        n = n + jnp.where(i >= s, 1, 0)
    return n


END_UNITS = (19, 20, 24, 25, 32, 33, 39, 40)
MID_UNITS = (35, 36, 37, 38)


def kernel(a, w, r, acc, ss_all, ax, ap, wl, wr, abuf, rbuf, ss_loc,
           recv_a, send_ya, send_yw, send_zi, send_zo, recv_wy, recv_wx, recv_wd, send_wx, send_wd,
           recv_da, recv_dw, send_da, send_dw, load_sem, load_w, load_a, send_ss, recv_ss):
    x = lax.axis_index("dp")
    z = lax.axis_index("tp2")
    t = lax.axis_index("tp")
    y = t // 2
    c = t % 2
    rows, cols = acc.shape
    kb = w.shape[0]
    ch = rows // NCH
    wch = cols // NWC
    unit = ch * GRP
    side = z // 2
    end = (z == 0) | (z == 3)
    mid = (z == 1) | (z == 2)
    base = side * (NCH // 2)
    other = (1 - side) * (NCH // 2)
    z_in = jnp.where(side == 0, z + 1, z - 1)
    z_out = jnp.where(side == 0, z - 1, z + 1)

    partner = (x, z, y * 2 + 1 - c)
    x_peer = (1 - x, z, t)
    y_same = (x, z, (1 - y) * 2 + c)
    y_cross = (x, z, (1 - y) * 2 + 1 - c)

    def remote(src, dst, send, recv, dev):
        return pltpu.make_async_remote_copy(
            src_ref=src, dst_ref=dst, send_sem=send, recv_sem=recv, device_id=dev, device_id_type=MESH)

    def wait_bytes(ref, sem):
        pltpu.make_async_copy(ref, ref, sem).wait()

    barrier = pltpu.get_barrier_semaphore()
    for dev in (partner, x_peer, y_same, y_cross):
        pl.semaphore_signal(barrier, inc=1, device_id=dev, device_id_type=MESH)
    for k in range(1, 4):
        pl.semaphore_signal(barrier, inc=1, device_id=(x, lax.rem(z + k, 4), t), device_id_type=MESH)
    pl.semaphore_wait(barrier, 7)

    def mp(start, j):
        return start + FAR + lax.rem(j + NEAR, FAR)

    def send_y_a(q):
        for cc in range(2):
            row = ((1 - y) * 2 + cc) * rows + q * ch
            remote(a.at[pl.ds(pl.multiple_of(row, ch), ch)], ax.at[q, c], send_ya, recv_a.at[q],
                   (x, z, (1 - y) * 2 + cc)).start()

    def w_part(half, n):
        return (pl.ds(pl.multiple_of(half * (kb // 2), kb // 2), kb // 2), pl.ds(pl.multiple_of(n * wch, wch), wch))

    def send_y_w(n):
        rs, cs = w_part(x, n)
        remote(w.at[rs, cs], wr.at[c, rs, cs], send_yw, recv_wy.at[n], y_same).start()

    def y_sends(i):
        iw = jnp.where(end, i, i - FAR)
        ia = jnp.where(end, i - WS, i)

        @pl.when((iw >= 0) & (iw < WS) & (lax.rem(iw, 2) == 0))
        def _():
            send_y_w(iw // 2)

        @pl.when(end & (ia >= 0) & (ia < FAR + NEAR))
        def _():
            send_y_a(base + ia)

        @pl.when(mid & (ia < FAR))
        def _():
            send_y_a(mp(base, ia))

    lax.fori_loop(0, AHEAD, lambda i, _: (y_sends(i), None)[1], None)

    remote(w, wl.at[1], send_dw, recv_dw, partner).start()
    prow = pl.ds(pl.multiple_of((y * 2 + 1 - c) * rows, rows), rows)
    remote(a.at[prow], ap, send_da, recv_da, partner).start()
    own_w = pltpu.make_async_copy(w, wl.at[0], load_w)
    own_w.start()

    def load(q):
        here = pl.ds(pl.multiple_of(q * ch, ch), ch)
        for b in range(2):
            pltpu.make_async_copy(ax.at[q, b], wl.at[b, here], load_a.at[q // GRP]).start()

    def arrive(q, i):
        wait_bytes(ax.at[q], recv_a.at[q])

        @pl.when(i >= LOADS)
        def _():
            load(q)

    def pass_in(q):
        remote(ax.at[q], ax.at[q], send_zi, recv_a.at[q], (x, z_in, t)).start()

    def pass_out(q):
        remote(ax.at[q], ax.at[q], send_zo, recv_a.at[q], (x, z_out, t)).start()

    def w_from_y(n):
        rs, cs = w_part(x, n)
        part = wr.at[c, rs, cs]
        wait_bytes(part, recv_wy.at[n])
        remote(part, part, send_wx, recv_wx.at[n], x_peer).start()
        remote(part, part, send_wd, recv_wd.at[n], partner).start()

    def w_from_x(n):
        rs, cs = w_part(1 - x, n)
        part = wr.at[c, rs, cs]
        wait_bytes(part, recv_wx.at[n])
        remote(part, part, send_wd, recv_wd.at[n], partner).start()

    def w_from_partner(n):
        cs = pl.ds(pl.multiple_of(n * wch, wch), wch)
        wait_bytes(wr.at[1 - c, :, cs], recv_wd.at[n])

    def z_chunk(j):
        own = (j == 0) | (lax.rem(j, 2) == 1)
        first = jnp.where(own, mp(base, (j + 1) // 2), mp(other, j // 2 - 1))
        return jnp.where(j < 2 * NEAR - 1, first, jnp.where(j < NEAR + FAR, mp(other, j - NEAR), other + j - NEAR - FAR))

    def comm(i):
        y_sends(i + AHEAD)
        iw = jnp.where(end, i, i - FAR)
        odd = lax.rem(i, 2) == 1

        @pl.when(odd & (iw >= 1) & (iw < WS))
        def _():
            w_from_y(iw // 2)

        @pl.when(odd & (iw >= 3) & (iw < WS + 2))
        def _():
            w_from_x((iw - 3) // 2)

        @pl.when(end)
        def _():
            @pl.when((i >= WS) & (i < WS + FAR + NEAR))
            def _():
                q = base + i - WS
                arrive(q, i)

                @pl.when(i < WS + FAR)
                def _():
                    pass_in(q)

            @pl.when((i >= 1) & (i < 1 + 2 * FAR + NEAR))
            def _():
                arrive(z_chunk(i - 1), i)

        @pl.when(mid)
        def _():
            @pl.when(i < FAR)
            def _():
                q = mp(base, i)
                arrive(q, i)

                @pl.when(i < NEAR)
                def _():
                    pass_out(q)

                pass_in(q)

            @pl.when((i >= 1) & (i < 1 + FAR))
            def _():
                q = mp(other, i - 1)
                arrive(q, i)
                pass_out(q)

            @pl.when((i >= WS + 1) & (i < WS + 1 + FAR))
            def _():
                q = base + i - WS - 1
                arrive(q, i)
                pass_in(q)

            @pl.when((i >= WS + 2) & (i < WS + 2 + FAR))
            def _():
                q = other + i - WS - 2
                arrive(q, i)
                pass_out(q)

    def early_loads():
        def from_z(j, _):
            load(jnp.where(end, z_chunk(j), mp(other, j)))
            return None

        lax.fori_loop(0, LOADS - 1, from_z, None)

        def from_y(j, _):
            load(mp(base, j))
            return None

        lax.fori_loop(0, jnp.where(end, 0, LOADS), from_y, None)

    tn = min(512, cols)
    ntile = cols // tn

    def local_loads(u):
        slot = lax.rem(u, 2)
        here = pl.ds(pl.multiple_of(u * unit, unit), unit)
        mine = pl.ds(pl.multiple_of(t * rows + u * unit, unit), unit)
        return (pltpu.make_async_copy(a.at[mine], abuf.at[slot, 0], load_sem.at[slot, 0]),
                pltpu.make_async_copy(ap.at[here], abuf.at[slot, 1], load_sem.at[slot, 1]),
                pltpu.make_async_copy(r.at[here], rbuf.at[slot], load_sem.at[slot, 2]))

    def local_unit(u):
        slot = lax.rem(u, 2)
        here = pl.ds(pl.multiple_of(u * unit, unit), unit)
        for cp in local_loads(u):
            cp.wait()

        @pl.when(u + 1 < NUNIT)
        def _():
            for cp in local_loads(u + 1):
                cp.start()

        def tile(n, _):
            cs = pl.ds(pl.multiple_of(n * tn, tn), tn)
            p0 = jnp.dot(abuf[slot, 0], wl[0, :, cs], preferred_element_type=jnp.float32)
            p1 = jnp.dot(abuf[slot, 1], wl[1, :, cs], preferred_element_type=jnp.float32)
            acc[here, cs] = (rbuf[slot, :, cs].astype(jnp.float32) + p0.astype(jnp.bfloat16).astype(jnp.float32)
                             + p1.astype(jnp.bfloat16).astype(jnp.float32))
            return None

        lax.fori_loop(0, ntile, tile, None)

    gs = NUNIT // 2

    def unit_of(u):
        b = side * gs
        o = (1 - side) * gs
        end_order = (b + 3, o + 3, b, o + 2, b + 1, o, b + 2, o + 1)
        mid_order = (b, o, b + 1, o + 1, 0, 0, 0, 0)
        q = jnp.int32(0)
        for k in range(NUNIT):
            q = q + jnp.where(u == k, jnp.where(end, end_order[k], mid_order[k]), 0)
        return q

    def wait_load(q):
        here = pl.ds(pl.multiple_of(q * unit, unit), unit)
        wait_bytes(wl.at[:, here], load_a.at[q])

    def far_product(here, cs):
        p0 = jnp.dot(wl[0, here, :], wr[0, :, cs], preferred_element_type=jnp.float32)
        p1 = jnp.dot(wl[1, here, :], wr[1, :, cs], preferred_element_type=jnp.float32)
        v = acc[here, cs] + (p0.astype(jnp.bfloat16).astype(jnp.float32) + p1.astype(jnp.bfloat16).astype(jnp.float32))
        acc[here, cs] = v
        return v

    def squares(v):
        sq = v * v
        part = sq[:, :128]
        for k in range(1, sq.shape[1] // 128):
            part = part + sq[:, k * 128:(k + 1) * 128]
        return part

    def keep_squares(q, part):
        for k in range(unit // 128):
            ss_loc[q, k:k + 1, :] = jnp.sum(part[k * 128:(k + 1) * 128, :].T, axis=0, keepdims=True)

    def remote_unit(u, _):
        q = unit_of(u)
        here = pl.ds(pl.multiple_of(q * unit, unit), unit)
        wait_load(q)

        def tile(n, part):
            cs = pl.ds(pl.multiple_of(n * tn, tn), tn)
            return part + squares(far_product(here, cs))

        keep_squares(q, lax.fori_loop(0, ntile, tile, jnp.zeros((unit, 128), jnp.float32)))
        return None

    def column_unit(k):
        return jnp.where(k < 2, side, 1 - side) * gs + 2 + lax.rem(k, 2)

    def column_step(n):
        w_from_partner(n)

        @pl.when(n == 0)
        def _():
            for k in range(4):
                wait_load(column_unit(jnp.int32(k)))

        cs = pl.ds(pl.multiple_of(n * wch, wch), wch)

        def rows_of(k, _):
            here = pl.ds(pl.multiple_of(column_unit(k) * unit, unit), unit)
            far_product(here, cs)
            return None

        lax.fori_loop(0, 4, rows_of, None)

        @pl.when(n == NWC - 1)
        def _():
            def sums(k, _):
                q = column_unit(k)
                here = pl.ds(pl.multiple_of(q * unit, unit), unit)

                def tile(m, part):
                    return part + squares(acc[here, pl.ds(pl.multiple_of(m * tn, tn), tn)])

                keep_squares(q, lax.fori_loop(0, ntile, tile, jnp.zeros((unit, 128), jnp.float32)))
                return None

            lax.fori_loop(0, 4, sums, None)

    def slot_body(i, _):
        @pl.when(i == LOADS)
        def _():
            early_loads()

        comm(i)

        @pl.when(i == LOCAL0 - 1)
        def _():
            own_w.wait()
            wait_bytes(wl.at[1], recv_dw)
            wait_bytes(ap, recv_da)
            for cp in local_loads(0):
                cp.start()

        @pl.when((i >= LOCAL0) & (i < LOCAL0 + NUNIT))
        def _():
            local_unit(i - LOCAL0)

        @pl.when(end & (i == WREADY))
        def _():
            lax.fori_loop(0, NWC, lambda n, _: (w_from_partner(n), None)[1], None)

        jc = i - COLS0

        @pl.when(mid & (jc >= 0) & (jc < WS) & (lax.rem(jc, 2) == 0))
        def _():
            column_step(jc // 2)

        lo = jnp.where(end, step_count(i - 1, END_UNITS), step_count(i - 1, MID_UNITS))
        hi = jnp.where(end, step_count(i, END_UNITS), step_count(i, MID_UNITS))
        lax.fori_loop(lo, hi, remote_unit, None)
        return None

    lax.fori_loop(0, NSLOT, slot_body, None)

    for k in range(1, 4):
        remote(ss_loc, ss_all.at[z], send_ss.at[k - 1], recv_ss.at[z], (x, lax.rem(z + k, 4), t)).start()
    wait_bytes(wl.at[1], send_dw)
    wait_bytes(ap, send_da)
    wait_bytes(wr.at[0], send_wd)
    wait_bytes(wr.at[0, pl.ds(0, kb // 2)], send_wx)
    wait_bytes(wr.at[0, pl.ds(0, kb // 2)], send_yw)

    @pl.when(end)
    def _():
        wait_bytes(ax.at[pl.ds(0, FAR + NEAR)], send_ya)
        wait_bytes(ax.at[pl.ds(0, FAR)], send_zi)

    @pl.when(mid)
    def _():
        wait_bytes(ax.at[pl.ds(0, FAR)], send_ya)
        wait_bytes(ax.at[pl.ds(0, 2 * FAR)], send_zi)
        wait_bytes(ax.at[pl.ds(0, 2 * FAR + NEAR)], send_zo)

    for k in range(1, 4):
        src = lax.rem(z + k, 4)
        remote(ss_loc, ss_all.at[src], send_ss.at[k - 1], recv_ss.at[src], (x, src, t)).wait_recv()
        remote(ss_loc, ss_all.at[src], send_ss.at[k - 1], recv_ss.at[src], (x, src, t)).wait_send()
    ss_all[z] = ss_loc[...]

def finish_kernel(h, ss, g, h_out, n_out, hbuf, nbuf, sem):
    rows, cols = h.shape
    unit = rows // NUNIT
    nfin = NUNIT

    def copies(q):
        slot = lax.rem(q, 2)
        here = pl.ds(pl.multiple_of(q * unit, unit), unit)
        return (pltpu.make_async_copy(hbuf.at[slot], h_out.at[here], sem.at[slot, 0]),
                pltpu.make_async_copy(nbuf.at[slot], n_out.at[here], sem.at[slot, 1]))

    def step(q, _):
        slot = lax.rem(q, 2)

        @pl.when(q >= 2)
        def _():
            for cp in copies(q - 2):
                cp.wait()

        total = ss[0, q] + ss[1, q] + ss[2, q] + ss[3, q]
        inv = lax.rsqrt(total / (cols * 4) + EPS_NORM)
        for k in range(unit // 128):
            col = jnp.broadcast_to(inv[k:k + 1, :], (128, 128)).T
            rs = pl.ds(pl.multiple_of(q * unit + k * 128, 128), 128)
            for m in range(cols // 128):
                cs = slice(m * 128, (m + 1) * 128)
                v = h[rs, cs]
                hbuf[slot, k * 128:(k + 1) * 128, cs] = v.astype(jnp.bfloat16)
                nbuf[slot, k * 128:(k + 1) * 128, cs] = (v * col * g[:, cs]).astype(jnp.bfloat16)
        for cp in copies(q):
            cp.start()
        return None

    lax.fori_loop(0, nfin, step, None)
    for q in (nfin - 2, nfin - 1):
        for cp in copies(jnp.int32(q)):
            cp.wait()


def solution(mesh):
    def local_step(attn_blk, w_blk, res_blk, gain_blk):
        kb = attn_blk.shape[1]
        rows, cols = res_blk.shape
        unit = rows // NUNIT
        any_spec = pl.BlockSpec(memory_space=pl.ANY)
        vmem_spec = pl.BlockSpec(memory_space=pltpu.VMEM)
        bf16, f32 = jnp.bfloat16, jnp.float32
        dma = pltpu.SemaphoreType.DMA
        h, ss, _, _ = pl.pallas_call(
            kernel,
            out_shape=(
                pltpu.VMEM((rows, cols), f32),
                pltpu.VMEM((4, NUNIT, unit // 128, 128), f32),
                jax.ShapeDtypeStruct((NCH, 2, rows // NCH, kb), bf16),
                jax.ShapeDtypeStruct((rows, kb), bf16),
            ),
            in_specs=[any_spec, any_spec, any_spec],
            out_specs=(vmem_spec, vmem_spec, any_spec, any_spec),
            scratch_shapes=[
                pltpu.VMEM((2, kb, cols), bf16),
                pltpu.VMEM((2, kb, cols), bf16),
                pltpu.VMEM((2, 2, unit, kb), bf16),
                pltpu.VMEM((2, unit, cols), bf16),
                pltpu.VMEM((NUNIT, unit // 128, 128), f32),
                dma((NCH,)), dma, dma, dma, dma,
                dma((NWC,)), dma((NWC,)), dma((NWC,)), dma, dma,
                dma, dma, dma, dma,
                dma((2, 3)), dma, dma((NUNIT,)),
                dma((3,)), dma((4,)),
            ],
            compiler_params=pltpu.CompilerParams(
                collective_id=0, has_side_effects=True, vmem_limit_bytes=44 * 1024 * 1024),
            name="gather_project",
        )(attn_blk, w_blk, res_blk)
        return pl.pallas_call(
            finish_kernel,
            out_shape=(jax.ShapeDtypeStruct((rows, cols), bf16),) * 2,
            in_specs=[vmem_spec, vmem_spec, vmem_spec],
            out_specs=(any_spec, any_spec),
            scratch_shapes=[pltpu.VMEM((2, unit, cols), bf16), pltpu.VMEM((2, unit, cols), bf16), dma((2, 2))],
            compiler_params=pltpu.CompilerParams(vmem_limit_bytes=8 * 1024 * 1024),
            name="norm_store",
        )(h, ss, gain_blk.reshape(1, cols))

    row_spec = P(("dp", "tp"), "tp2")
    return jax.shard_map(local_step, mesh=mesh, in_specs=(P("dp", "tp"), P("tp", "tp2"), row_spec, P("tp2")), out_specs=(row_spec, row_spec), check_vma=False)
```

```python
import functools

import jax
import jax.numpy as jnp
from jax import lax
from jax.experimental import pallas as pl
from jax.experimental.pallas import tpu as pltpu
from jax.sharding import PartitionSpec as P

EPS_NORM = 1e-6
MESH = pl.DeviceIdType.MESH
NCH = 64
FAR = NCH // 4
NEAR = NCH // 8
NWC = 8
WS = 2 * NWC
NUNIT = 8
NHALF = 2 * NUNIT
GRP = NCH // NUNIT
HGRP = NCH // NHALF
NBUF = 4
NSUB = 4
AHEAD = 12
NSLOT = 2 * FAR + NEAR + 1
LOCAL0 = 6
LOADS = 16
WREADY = WS + 2
COLS0 = FAR + 4


def step_count(i, slots):
    n = jnp.int32(0)
    for s in slots:
        n = n + jnp.where(i >= s, 1, 0)
    return n


END_UNITS = (19, 19, 20, 20, 21, 22, 24, 25, 28, 29, 32, 33, 36, 37, 39, 40)
MID_UNITS = (35, 35, 36, 36, 37, 37, 38, 38)


def kernel(a, w, r, acc, ss_all, ax, ap, wl, wr, abuf, rbuf, ss_loc,
           recv_a, send_ya, send_yw, send_zi, send_zo, recv_wy, recv_wx, recv_wd, send_wx, send_wd,
           recv_da, recv_dw, send_da, send_dw, load_sem, load_w, load_a, recv_sub, send_ss, recv_ss):
    x = lax.axis_index("dp")
    z = lax.axis_index("tp2")
    t = lax.axis_index("tp")
    y = t // 2
    c = t % 2
    rows, cols = acc.shape
    kb = w.shape[0]
    ch = rows // NCH
    wch = cols // NWC
    unit = ch * GRP
    half = ch * HGRP
    sub = ch // NSUB
    side = z // 2
    end = (z == 0) | (z == 3)
    mid = (z == 1) | (z == 2)
    base = side * (NCH // 2)
    other = (1 - side) * (NCH // 2)
    z_in = jnp.where(side == 0, z + 1, z - 1)
    z_out = jnp.where(side == 0, z - 1, z + 1)

    partner = (x, z, y * 2 + 1 - c)
    x_peer = (1 - x, z, t)
    y_same = (x, z, (1 - y) * 2 + c)
    y_cross = (x, z, (1 - y) * 2 + 1 - c)

    def remote(src, dst, send, recv, dev):
        return pltpu.make_async_remote_copy(
            src_ref=src, dst_ref=dst, send_sem=send, recv_sem=recv, device_id=dev, device_id_type=MESH)

    def wait_bytes(ref, sem):
        pltpu.make_async_copy(ref, ref, sem).wait()

    barrier = pltpu.get_barrier_semaphore()
    for dev in (partner, x_peer, y_same, y_cross):
        pl.semaphore_signal(barrier, inc=1, device_id=dev, device_id_type=MESH)
    for k in range(1, 4):
        pl.semaphore_signal(barrier, inc=1, device_id=(x, lax.rem(z + k, 4), t), device_id_type=MESH)
    pl.semaphore_wait(barrier, 7)

    def mp(start, j):
        return start + FAR + lax.rem(j + NEAR, FAR)

    def send_y_a(q):
        for cc in range(2):
            row = ((1 - y) * 2 + cc) * rows + q * ch
            remote(a.at[pl.ds(pl.multiple_of(row, ch), ch)], ax.at[q, c], send_ya, recv_a.at[q],
                   (x, z, (1 - y) * 2 + cc)).start()

    def send_y_first(q):
        for k in range(NSUB):
            for cc in range(2):
                row = ((1 - y) * 2 + cc) * rows + q * ch + k * sub
                remote(a.at[pl.ds(pl.multiple_of(row, sub), sub)], ax.at[q, c, pl.ds(k * sub, sub)], send_ya,
                       recv_sub.at[k], (x, z, (1 - y) * 2 + cc)).start()

    def w_part(part, n):
        return (pl.ds(pl.multiple_of(part * (kb // 2), kb // 2), kb // 2), pl.ds(pl.multiple_of(n * wch, wch), wch))

    def send_y_w(n):
        rs, cs = w_part(x, n)
        remote(w.at[rs, cs], wr.at[c, rs, cs], send_yw, recv_wy.at[n], y_same).start()

    def y_sends(i):
        iw = jnp.where(end, i, i - FAR)
        ia = jnp.where(end, i - WS, i)

        @pl.when((iw >= 0) & (iw < WS) & (lax.rem(iw, 2) == 0))
        def _():
            send_y_w(iw // 2)

        @pl.when(end & (ia >= 0) & (ia < FAR + NEAR))
        def _():
            send_y_a(base + ia)

        @pl.when(mid & (ia == 0))
        def _():
            send_y_first(mp(base, 0))

        @pl.when(mid & (ia >= 1) & (ia < FAR))
        def _():
            send_y_a(mp(base, ia))

    lax.fori_loop(0, AHEAD, lambda i, _: (y_sends(i), None)[1], None)

    remote(w, wl.at[1], send_dw, recv_dw, partner).start()
    prow = pl.ds(pl.multiple_of((y * 2 + 1 - c) * rows, rows), rows)
    remote(a.at[prow], ap, send_da, recv_da, partner).start()
    own_w = pltpu.make_async_copy(w, wl.at[0], load_w)
    own_w.start()

    def load(q):
        here = pl.ds(pl.multiple_of(q * ch, ch), ch)
        for b in range(2):
            pltpu.make_async_copy(ax.at[q, b], wl.at[b, here], load_a.at[q // HGRP]).start()

    def arrive(q, i):
        wait_bytes(ax.at[q], recv_a.at[q])

        @pl.when(i >= LOADS)
        def _():
            load(q)

    def pass_in(q):
        remote(ax.at[q], ax.at[q], send_zi, recv_a.at[q], (x, z_in, t)).start()

    def pass_out(q):
        remote(ax.at[q], ax.at[q], send_zo, recv_a.at[q], (x, z_out, t)).start()

    def w_from_y(n):
        rs, cs = w_part(x, n)
        part = wr.at[c, rs, cs]
        wait_bytes(part, recv_wy.at[n])
        remote(part, part, send_wx, recv_wx.at[n], x_peer).start()
        remote(part, part, send_wd, recv_wd.at[n], partner).start()

    def w_from_x(n):
        rs, cs = w_part(1 - x, n)
        part = wr.at[c, rs, cs]
        wait_bytes(part, recv_wx.at[n])
        remote(part, part, send_wd, recv_wd.at[n], partner).start()

    def w_from_partner(n):
        cs = pl.ds(pl.multiple_of(n * wch, wch), wch)
        wait_bytes(wr.at[1 - c, :, cs], recv_wd.at[n])

    def z_chunk(j):
        own = (j == 0) | (lax.rem(j, 2) == 1)
        first = jnp.where(own, mp(base, (j + 1) // 2), mp(other, j // 2 - 1))
        return jnp.where(j < 2 * NEAR - 1, first, jnp.where(j < NEAR + FAR, mp(other, j - NEAR), other + j - NEAR - FAR))

    def comm(i):
        y_sends(i + AHEAD)
        iw = jnp.where(end, i, i - FAR)
        odd = lax.rem(i, 2) == 1

        @pl.when(odd & (iw >= 1) & (iw < WS))
        def _():
            w_from_y(iw // 2)

        @pl.when(odd & (iw >= 3) & (iw < WS + 2))
        def _():
            w_from_x((iw - 3) // 2)

        @pl.when(end)
        def _():
            @pl.when((i >= WS) & (i < WS + FAR + NEAR))
            def _():
                q = base + i - WS
                arrive(q, i)

                @pl.when(i < WS + FAR)
                def _():
                    pass_in(q)

            @pl.when((i >= 1) & (i < 1 + 2 * FAR + NEAR))
            def _():
                arrive(z_chunk(i - 1), i)

        @pl.when(mid)
        def _():
            @pl.when(i == 0)
            def _():
                q = mp(base, 0)
                for k in range(NSUB):
                    piece = ax.at[q, :, pl.ds(k * sub, sub)]
                    wait_bytes(piece, recv_sub.at[k])
                    remote(piece, piece, send_zo, recv_a.at[q], (x, z_out, t)).start()
                pass_in(q)

            @pl.when((i >= 1) & (i < FAR))
            def _():
                q = mp(base, i)
                arrive(q, i)

                @pl.when(i < NEAR)
                def _():
                    pass_out(q)

                pass_in(q)

            @pl.when((i >= 1) & (i < 1 + FAR))
            def _():
                q = mp(other, i - 1)
                arrive(q, i)
                pass_out(q)

            @pl.when((i >= WS + 1) & (i < WS + 1 + FAR))
            def _():
                q = base + i - WS - 1
                arrive(q, i)
                pass_in(q)

            @pl.when((i >= WS + 2) & (i < WS + 2 + FAR))
            def _():
                q = other + i - WS - 2
                arrive(q, i)
                pass_out(q)

    def early_loads():
        def from_z(j, _):
            load(jnp.where(end, z_chunk(j), mp(other, j)))
            return None

        lax.fori_loop(0, LOADS - 1, from_z, None)

        def from_y(j, _):
            load(mp(base, j))
            return None

        lax.fori_loop(0, jnp.where(end, 0, LOADS), from_y, None)

    tn = min(512, cols)
    ntile = cols // tn

    def local_loads(u):
        slot = lax.rem(u, 2)
        here = pl.ds(pl.multiple_of(u * unit, unit), unit)
        mine = pl.ds(pl.multiple_of(t * rows + u * unit, unit), unit)
        return (pltpu.make_async_copy(a.at[mine], abuf.at[slot, 0], load_sem.at[slot, 0]),
                pltpu.make_async_copy(ap.at[here], abuf.at[slot, 1], load_sem.at[slot, 1]),
                pltpu.make_async_copy(r.at[here], rbuf.at[slot], load_sem.at[slot, 2]))

    def local_unit(u):
        slot = lax.rem(u, 2)
        here = pl.ds(pl.multiple_of(u * unit, unit), unit)
        for cp in local_loads(u):
            cp.wait()

        @pl.when(u + 1 < NUNIT)
        def _():
            for cp in local_loads(u + 1):
                cp.start()

        def tile(n, _):
            cs = pl.ds(pl.multiple_of(n * tn, tn), tn)
            p0 = jnp.dot(abuf[slot, 0], wl[0, :, cs], preferred_element_type=jnp.float32)
            p1 = jnp.dot(abuf[slot, 1], wl[1, :, cs], preferred_element_type=jnp.float32)
            acc[here, cs] = (rbuf[slot, :, cs].astype(jnp.float32) + p0.astype(jnp.bfloat16).astype(jnp.float32)
                             + p1.astype(jnp.bfloat16).astype(jnp.float32))
            return None

        lax.fori_loop(0, ntile, tile, None)

    gs = NUNIT // 2

    def unit_of(u):
        b = side * NUNIT
        o = (1 - side) * NUNIT
        end_order = (b + 6, b + 7, o + 6, o + 7, b, o + 4, b + 1, o + 5, b + 2, o, b + 3, o + 1, b + 4, o + 2, b + 5, o + 3)
        mid_order = (b, b + 1, o, o + 1, b + 2, b + 3, o + 2, o + 3) + (0,) * NUNIT
        q = jnp.int32(0)
        for k in range(NHALF):
            q = q + jnp.where(u == k, jnp.where(end, end_order[k], mid_order[k]), 0)
        return q

    def wait_load(q):
        here = pl.ds(pl.multiple_of(q * half, half), half)
        wait_bytes(wl.at[:, here], load_a.at[q])

    def far_product(here, cs):
        p0 = jnp.dot(wl[0, here, :], wr[0, :, cs], preferred_element_type=jnp.float32)
        p1 = jnp.dot(wl[1, here, :], wr[1, :, cs], preferred_element_type=jnp.float32)
        v = acc[here, cs] + (p0.astype(jnp.bfloat16).astype(jnp.float32) + p1.astype(jnp.bfloat16).astype(jnp.float32))
        acc[here, cs] = v
        return v

    def squares(v):
        sq = v * v
        part = sq[:, :128]
        for k in range(1, sq.shape[1] // 128):
            part = part + sq[:, k * 128:(k + 1) * 128]
        return part

    def keep_squares(q, part):
        ss_loc[q] = jnp.sum(part.T, axis=0, keepdims=True)

    def remote_unit(u, _):
        q = unit_of(u)
        here = pl.ds(pl.multiple_of(q * half, half), half)
        wait_load(q)

        def tile(n, part):
            cs = pl.ds(pl.multiple_of(n * tn, tn), tn)
            return part + squares(far_product(here, cs))

        keep_squares(q, lax.fori_loop(0, ntile, tile, jnp.zeros((half, 128), jnp.float32)))
        return None

    def column_unit(k):
        return jnp.where(k < 2, side, 1 - side) * gs + 2 + lax.rem(k, 2)

    def column_step(n):
        w_from_partner(n)

        @pl.when(n == 0)
        def _():
            for k in range(4):
                for e in range(2):
                    wait_load(column_unit(jnp.int32(k)) * 2 + e)

        cs = pl.ds(pl.multiple_of(n * wch, wch), wch)

        def rows_of(k, _):
            here = pl.ds(pl.multiple_of(column_unit(k) * unit, unit), unit)
            far_product(here, cs)
            return None

        lax.fori_loop(0, 4, rows_of, None)

        @pl.when(n == NWC - 1)
        def _():
            def sums(k, _):
                q = column_unit(k // 2) * 2 + lax.rem(k, 2)
                here = pl.ds(pl.multiple_of(q * half, half), half)

                def tile(m, part):
                    return part + squares(acc[here, pl.ds(pl.multiple_of(m * tn, tn), tn)])

                keep_squares(q, lax.fori_loop(0, ntile, tile, jnp.zeros((half, 128), jnp.float32)))
                return None

            lax.fori_loop(0, 8, sums, None)

    def slot_body(i, _):
        @pl.when(i == LOADS)
        def _():
            early_loads()

        comm(i)

        @pl.when(i == LOCAL0 - 1)
        def _():
            own_w.wait()
            wait_bytes(wl.at[1], recv_dw)
            wait_bytes(ap, recv_da)
            for cp in local_loads(0):
                cp.start()

        @pl.when((i >= LOCAL0) & (i < LOCAL0 + NUNIT))
        def _():
            local_unit(i - LOCAL0)

        @pl.when(end & (i == WREADY))
        def _():
            lax.fori_loop(0, NWC, lambda n, _: (w_from_partner(n), None)[1], None)

        jc = i - COLS0

        @pl.when(mid & (jc >= 0) & (jc < WS) & (lax.rem(jc, 2) == 0))
        def _():
            column_step(jc // 2)

        lo = jnp.where(end, step_count(i - 1, END_UNITS), step_count(i - 1, MID_UNITS))
        hi = jnp.where(end, step_count(i, END_UNITS), step_count(i, MID_UNITS))
        lax.fori_loop(lo, hi, remote_unit, None)
        return None

    lax.fori_loop(0, NSLOT, slot_body, None)

    for k in range(1, 4):
        remote(ss_loc, ss_all.at[z], send_ss.at[k - 1], recv_ss.at[z], (x, lax.rem(z + k, 4), t)).start()
    wait_bytes(wl.at[1], send_dw)
    wait_bytes(ap, send_da)
    wait_bytes(wr.at[0], send_wd)
    wait_bytes(wr.at[0, pl.ds(0, kb // 2)], send_wx)
    wait_bytes(wr.at[0, pl.ds(0, kb // 2)], send_yw)

    @pl.when(end)
    def _():
        wait_bytes(ax.at[pl.ds(0, FAR + NEAR)], send_ya)
        wait_bytes(ax.at[pl.ds(0, FAR)], send_zi)

    @pl.when(mid)
    def _():
        wait_bytes(ax.at[pl.ds(0, FAR)], send_ya)
        wait_bytes(ax.at[pl.ds(0, 2 * FAR)], send_zi)
        wait_bytes(ax.at[pl.ds(0, 2 * FAR + NEAR)], send_zo)

    for k in range(1, 4):
        src = lax.rem(z + k, 4)
        remote(ss_loc, ss_all.at[src], send_ss.at[k - 1], recv_ss.at[src], (x, src, t)).wait_recv()
        remote(ss_loc, ss_all.at[src], send_ss.at[k - 1], recv_ss.at[src], (x, src, t)).wait_send()
    ss_all[z] = ss_loc[...]

def finish_kernel(h, ss, g, h_out, n_out, hbuf, nbuf, sem):
    rows, cols = h.shape
    step_rows = rows // NHALF

    def copies(q):
        slot = lax.rem(q, NBUF)
        here = pl.ds(pl.multiple_of(q * step_rows, step_rows), step_rows)
        return (pltpu.make_async_copy(hbuf.at[slot], h_out.at[here], sem.at[slot, 0]),
                pltpu.make_async_copy(nbuf.at[slot], n_out.at[here], sem.at[slot, 1]))

    def step(q, _):
        slot = lax.rem(q, NBUF)

        @pl.when(q >= NBUF)
        def _():
            for cp in copies(q - NBUF):
                cp.wait()

        total = ss[0, q] + ss[1, q] + ss[2, q] + ss[3, q]
        inv = lax.rsqrt(total / (cols * 4) + EPS_NORM)
        col = jnp.broadcast_to(inv, (128, 128)).T
        rs = pl.ds(pl.multiple_of(q * 128, 128), 128)
        for m in range(cols // 128):
            cs = slice(m * 128, (m + 1) * 128)
            v = h[rs, cs]
            hbuf[slot, :, cs] = v.astype(jnp.bfloat16)
            nbuf[slot, :, cs] = (v * col * g[:, cs]).astype(jnp.bfloat16)
        for cp in copies(q):
            cp.start()
        return None

    lax.fori_loop(0, NHALF, step, None)

    def drain(q, _):
        for cp in copies(q):
            cp.wait()
        return None

    lax.fori_loop(NHALF - NBUF, NHALF, drain, None)


def solution(mesh):
    def local_step(attn_blk, w_blk, res_blk, gain_blk):
        kb = attn_blk.shape[1]
        rows, cols = res_blk.shape
        unit = rows // NUNIT
        any_spec = pl.BlockSpec(memory_space=pl.ANY)
        vmem_spec = pl.BlockSpec(memory_space=pltpu.VMEM)
        bf16, f32 = jnp.bfloat16, jnp.float32
        dma = pltpu.SemaphoreType.DMA
        h, ss, _, _ = pl.pallas_call(
            kernel,
            out_shape=(
                pltpu.VMEM((rows, cols), f32),
                pltpu.VMEM((4, NHALF, 1, 128), f32),
                jax.ShapeDtypeStruct((NCH, 2, rows // NCH, kb), bf16),
                jax.ShapeDtypeStruct((rows, kb), bf16),
            ),
            in_specs=[any_spec, any_spec, any_spec],
            out_specs=(vmem_spec, vmem_spec, any_spec, any_spec),
            scratch_shapes=[
                pltpu.VMEM((2, kb, cols), bf16),
                pltpu.VMEM((2, kb, cols), bf16),
                pltpu.VMEM((2, 2, unit, kb), bf16),
                pltpu.VMEM((2, unit, cols), bf16),
                pltpu.VMEM((NHALF, 1, 128), f32),
                dma((NCH,)), dma, dma, dma, dma,
                dma((NWC,)), dma((NWC,)), dma((NWC,)), dma, dma,
                dma, dma, dma, dma,
                dma((2, 3)), dma, dma((NHALF,)), dma((NSUB,)),
                dma((3,)), dma((4,)),
            ],
            compiler_params=pltpu.CompilerParams(
                collective_id=0, has_side_effects=True, vmem_limit_bytes=44 * 1024 * 1024),
            name="gather_project",
        )(attn_blk, w_blk, res_blk)
        return pl.pallas_call(
            finish_kernel,
            out_shape=(jax.ShapeDtypeStruct((rows, cols), bf16),) * 2,
            in_specs=[vmem_spec, vmem_spec, vmem_spec],
            out_specs=(any_spec, any_spec),
            scratch_shapes=[pltpu.VMEM((NBUF, rows // NHALF, cols), bf16)] * 2 + [dma((NBUF, 2))],
            compiler_params=pltpu.CompilerParams(vmem_limit_bytes=8 * 1024 * 1024),
            name="norm_store",
        )(h, ss, gain_blk.reshape(1, cols))

    row_spec = P(("dp", "tp"), "tp2")
    return jax.shard_map(local_step, mesh=mesh, in_specs=(P("dp", "tp"), P("tp", "tp2"), row_spec, P("tp2")), out_specs=(row_spec, row_spec), check_vma=False)
```

```python
import functools

import jax
import jax.numpy as jnp
from jax import lax
from jax.experimental import pallas as pl
from jax.experimental.pallas import tpu as pltpu
from jax.sharding import PartitionSpec as P

EPS_NORM = 1e-6
MESH = pl.DeviceIdType.MESH
NCH = 64
FAR = NCH // 4
NEAR = NCH // 8
NWC = 8
WS = 2 * NWC
NUNIT = 8
NHALF = 2 * NUNIT
GRP = NCH // NUNIT
HGRP = NCH // NHALF
LATE = FAR // 2
NBUF = 4
NDIRECT = 2
NSUB = 4
AHEAD = 12
NSLOT = 2 * FAR + NEAR + 1
LOCAL0 = 6
LOADS = 16
WREADY = WS + 2
COLS0 = FAR + 4


def step_count(i, slots):
    n = jnp.int32(0)
    for s in slots:
        n = n + jnp.where(i >= s, 1, 0)
    return n


END_UNITS = (19, 19, 20, 20, 21, 22, 24, 25, 28, 29, 32, 33, 36, 37, 39, 40)
MID_UNITS = (35, 35, 36, 36, 37, 37, 38, 38)


def kernel(a, w, r, acc, ss_all, ax, ap, wl, wr, abuf, rbuf, ss_loc,
           recv_a, send_ya, send_yw, send_zi, send_zo, recv_wy, recv_wx, recv_wd, send_wx, send_wd,
           recv_da, recv_dw, send_da, send_dw, load_sem, load_w, load_a, recv_sub, send_first, credit_z, credit_y, send_ss, recv_ss):
    x = lax.axis_index("dp")
    z = lax.axis_index("tp2")
    t = lax.axis_index("tp")
    y = t // 2
    c = t % 2
    rows, cols = acc.shape
    kb = w.shape[0]
    ch = rows // NCH
    wch = cols // NWC
    unit = ch * GRP
    half = ch * HGRP
    sub = ch // NSUB
    side = z // 2
    end = (z == 0) | (z == 3)
    mid = (z == 1) | (z == 2)
    base = side * (NCH // 2)
    other = (1 - side) * (NCH // 2)
    z_in = jnp.where(side == 0, z + 1, z - 1)
    z_out = jnp.where(side == 0, z - 1, z + 1)

    partner = (x, z, y * 2 + 1 - c)
    x_peer = (1 - x, z, t)
    y_same = (x, z, (1 - y) * 2 + c)
    y_cross = (x, z, (1 - y) * 2 + 1 - c)

    def remote(src, dst, send, recv, dev):
        return pltpu.make_async_remote_copy(
            src_ref=src, dst_ref=dst, send_sem=send, recv_sem=recv, device_id=dev, device_id_type=MESH)

    def wait_bytes(ref, sem):
        pltpu.make_async_copy(ref, ref, sem).wait()

    barrier = pltpu.get_barrier_semaphore()
    for dev in (partner, x_peer, y_same, y_cross):
        pl.semaphore_signal(barrier, inc=1, device_id=dev, device_id_type=MESH)
    for k in range(1, 4):
        pl.semaphore_signal(barrier, inc=1, device_id=(x, lax.rem(z + k, 4), t), device_id_type=MESH)
    z_mate = jnp.where(end, z_in, z_out)
    for cc in range(2):
        pl.semaphore_signal(barrier, inc=1, device_id=(x, z_mate, (1 - y) * 2 + cc), device_id_type=MESH)
    pl.semaphore_wait(barrier, 9)

    def mp(start, j):
        return start + FAR + lax.rem(j + NEAR, FAR)

    def chunk_rows(q):
        return pl.ds(pl.multiple_of(q * ch, ch), ch)

    def send_y_a(q, dst=None):
        dst = ax.at[q, c] if dst is None else dst
        for cc in range(2):
            row = ((1 - y) * 2 + cc) * rows + q * ch
            remote(a.at[pl.ds(pl.multiple_of(row, ch), ch)], dst, send_ya, recv_a.at[q],
                   (x, z, (1 - y) * 2 + cc)).start()

    def send_y_first(q):
        for k in range(NDIRECT):
            for cc in range(2):
                row = ((1 - y) * 2 + cc) * rows + q * ch + k * sub
                remote(a.at[pl.ds(pl.multiple_of(row, sub), sub)], ax.at[q, c, pl.ds(k * sub, sub)], send_first,
                       recv_a.at[q], (x, z_out, (1 - y) * 2 + cc)).start()
        for k in range(NSUB):
            for cc in range(2):
                row = ((1 - y) * 2 + cc) * rows + q * ch + k * sub
                remote(a.at[pl.ds(pl.multiple_of(row, sub), sub)], ax.at[q, c, pl.ds(k * sub, sub)], send_ya,
                       recv_sub.at[k], (x, z, (1 - y) * 2 + cc)).start()

    def w_part(part, n):
        return (pl.ds(pl.multiple_of(part * (kb // 2), kb // 2), kb // 2), pl.ds(pl.multiple_of(n * wch, wch), wch))

    def send_y_w(n):
        rs, cs = w_part(x, n)
        remote(w.at[rs, cs], wr.at[c, rs, cs], send_yw, recv_wy.at[n], y_same).start()

    def y_sends(i):
        iw = jnp.where(end, i, i - FAR)
        ia = jnp.where(end, i - WS, i)

        @pl.when((iw >= 0) & (iw < WS) & (lax.rem(iw, 2) == 0))
        def _():
            send_y_w(iw // 2)

        @pl.when(end & (ia >= 0) & (ia < FAR))
        def _():
            send_y_a(base + ia)

        @pl.when(end & (ia == FAR))
        def _():
            pl.semaphore_wait(credit_y, 2)

        @pl.when(end & (ia >= FAR) & (ia < FAR + NEAR))
        def _():
            send_y_a(base + ia, wl.at[c, chunk_rows(base + ia)])

        @pl.when(mid & (ia == 0))
        def _():
            send_y_first(mp(base, 0))

        @pl.when(mid & (ia >= 1) & (ia < FAR))
        def _():
            send_y_a(mp(base, ia))

    lax.fori_loop(0, AHEAD, lambda i, _: (y_sends(i), None)[1], None)

    remote(w, wl.at[1], send_dw, recv_dw, partner).start()
    prow = pl.ds(pl.multiple_of((y * 2 + 1 - c) * rows, rows), rows)
    remote(a.at[prow], ap, send_da, recv_da, partner).start()
    own_w = pltpu.make_async_copy(w, wl.at[0], load_w)
    own_w.start()

    def load(q):
        here = pl.ds(pl.multiple_of(q * ch, ch), ch)
        for b in range(2):
            pltpu.make_async_copy(ax.at[q, b], wl.at[b, here], load_a.at[q // HGRP]).start()

    def arrive(q, i):
        wait_bytes(ax.at[q], recv_a.at[q])

        @pl.when(i >= LOADS)
        def _():
            load(q)

    def arrive_late(q):
        wait_bytes(wl.at[:, chunk_rows(q)], recv_a.at[q])

    def pass_out_late(q):
        remote(ax.at[q], wl.at[:, chunk_rows(q)], send_zo, recv_a.at[q], (x, z_out, t)).start()

    def pass_in(q):
        remote(ax.at[q], ax.at[q], send_zi, recv_a.at[q], (x, z_in, t)).start()

    def pass_out(q):
        remote(ax.at[q], ax.at[q], send_zo, recv_a.at[q], (x, z_out, t)).start()

    def w_from_y(n):
        rs, cs = w_part(x, n)
        part = wr.at[c, rs, cs]
        wait_bytes(part, recv_wy.at[n])
        remote(part, part, send_wx, recv_wx.at[n], x_peer).start()
        remote(part, part, send_wd, recv_wd.at[n], partner).start()

    def w_from_x(n):
        rs, cs = w_part(1 - x, n)
        part = wr.at[c, rs, cs]
        wait_bytes(part, recv_wx.at[n])
        remote(part, part, send_wd, recv_wd.at[n], partner).start()

    def w_from_partner(n):
        cs = pl.ds(pl.multiple_of(n * wch, wch), wch)
        wait_bytes(wr.at[1 - c, :, cs], recv_wd.at[n])

    def z_chunk(j):
        own = (j == 0) | (lax.rem(j, 2) == 1)
        first = jnp.where(own, mp(base, (j + 1) // 2), mp(other, j // 2 - 1))
        return jnp.where(j < 2 * NEAR - 1, first, jnp.where(j < NEAR + FAR, mp(other, j - NEAR), other + j - NEAR - FAR))

    def comm(i):
        y_sends(i + AHEAD)
        iw = jnp.where(end, i, i - FAR)
        odd = lax.rem(i, 2) == 1

        @pl.when(odd & (iw >= 1) & (iw < WS))
        def _():
            w_from_y(iw // 2)

        @pl.when(odd & (iw >= 3) & (iw < WS + 2))
        def _():
            w_from_x((iw - 3) // 2)

        @pl.when(end)
        def _():
            @pl.when((i >= WS) & (i < WS + FAR))
            def _():
                q = base + i - WS
                arrive(q, i)
                pass_in(q)

            @pl.when((i >= WS + FAR) & (i < WS + FAR + NEAR))
            def _():
                arrive_late(base + i - WS)

            nlate = 1 + 2 * FAR + NEAR - LATE

            @pl.when((i >= 1) & (i < nlate))
            def _():
                arrive(z_chunk(i - 1), i)

            @pl.when((i >= nlate) & (i < nlate + LATE))
            def _():
                arrive_late(z_chunk(i - 1))

        @pl.when(mid)
        def _():
            @pl.when(i == 0)
            def _():
                q = mp(base, 0)
                for k in range(NSUB):
                    piece = ax.at[q, :, pl.ds(k * sub, sub)]
                    wait_bytes(piece, recv_sub.at[k])
                    if k >= NDIRECT:
                        remote(piece, piece, send_first, recv_a.at[q], (x, z_out, t)).start()
                pass_in(q)

            @pl.when((i >= 1) & (i < FAR))
            def _():
                q = mp(base, i)
                arrive(q, i)

                @pl.when(i < NEAR)
                def _():
                    pass_out(q)

                pass_in(q)

            @pl.when((i >= 1) & (i < 1 + FAR))
            def _():
                q = mp(other, i - 1)
                arrive(q, i)
                pass_out(q)

            @pl.when((i >= WS + 1) & (i < WS + 1 + FAR))
            def _():
                q = base + i - WS - 1
                arrive(q, i)
                pass_in(q)

            @pl.when((i >= WS + 2) & (i < WS + 2 + FAR))
            def _():
                q = other + i - WS - 2
                arrive(q, i)

                @pl.when(i < WS + 2 + FAR - LATE)
                def _():
                    pass_out(q)

                @pl.when(i == WS + 2 + FAR - LATE)
                def _():
                    pl.semaphore_wait(credit_z, 1)

                @pl.when(i >= WS + 2 + FAR - LATE)
                def _():
                    pass_out_late(q)

    def early_loads():
        def from_z(j, _):
            load(jnp.where(end, z_chunk(j), mp(other, j)))
            return None

        lax.fori_loop(0, LOADS - 1, from_z, None)

        def from_y(j, _):
            load(mp(base, j))
            return None

        lax.fori_loop(0, jnp.where(end, 0, LOADS), from_y, None)

    tn = min(512, cols)
    ntile = cols // tn

    def local_loads(u):
        slot = lax.rem(u, 2)
        here = pl.ds(pl.multiple_of(u * unit, unit), unit)
        mine = pl.ds(pl.multiple_of(t * rows + u * unit, unit), unit)
        return (pltpu.make_async_copy(a.at[mine], abuf.at[slot, 0], load_sem.at[slot, 0]),
                pltpu.make_async_copy(ap.at[here], abuf.at[slot, 1], load_sem.at[slot, 1]),
                pltpu.make_async_copy(r.at[here], rbuf.at[slot], load_sem.at[slot, 2]))

    def local_unit(u):
        slot = lax.rem(u, 2)
        here = pl.ds(pl.multiple_of(u * unit, unit), unit)
        for cp in local_loads(u):
            cp.wait()

        @pl.when(u + 1 < NUNIT)
        def _():
            for cp in local_loads(u + 1):
                cp.start()

        def tile(n, _):
            cs = pl.ds(pl.multiple_of(n * tn, tn), tn)
            p0 = jnp.dot(abuf[slot, 0], wl[0, :, cs], preferred_element_type=jnp.float32)
            p1 = jnp.dot(abuf[slot, 1], wl[1, :, cs], preferred_element_type=jnp.float32)
            acc[here, cs] = (rbuf[slot, :, cs].astype(jnp.float32) + p0.astype(jnp.bfloat16).astype(jnp.float32)
                             + p1.astype(jnp.bfloat16).astype(jnp.float32))
            return None

        lax.fori_loop(0, ntile, tile, None)

    gs = NUNIT // 2

    def unit_of(u):
        b = side * NUNIT
        o = (1 - side) * NUNIT
        end_order = (b + 6, b + 7, o + 6, o + 7, b, o + 4, b + 1, o + 5, b + 2, o, b + 3, o + 1, b + 4, o + 2, b + 5, o + 3)
        mid_order = (b, b + 1, o, o + 1, b + 2, b + 3, o + 2, o + 3) + (0,) * NUNIT
        q = jnp.int32(0)
        for k in range(NHALF):
            q = q + jnp.where(u == k, jnp.where(end, end_order[k], mid_order[k]), 0)
        return q

    def wait_load(q):
        here = pl.ds(pl.multiple_of(q * half, half), half)
        wait_bytes(wl.at[:, here], load_a.at[q])

    def far_product(here, cs):
        p0 = jnp.dot(wl[0, here, :], wr[0, :, cs], preferred_element_type=jnp.float32)
        p1 = jnp.dot(wl[1, here, :], wr[1, :, cs], preferred_element_type=jnp.float32)
        v = acc[here, cs] + (p0.astype(jnp.bfloat16).astype(jnp.float32) + p1.astype(jnp.bfloat16).astype(jnp.float32))
        acc[here, cs] = v
        return v

    def squares(v):
        sq = v * v
        part = sq[:, :128]
        for k in range(1, sq.shape[1] // 128):
            part = part + sq[:, k * 128:(k + 1) * 128]
        return part

    def keep_squares(q, part):
        ss_loc[q] = jnp.sum(part.T, axis=0, keepdims=True)

    def remote_unit(u, _):
        q = unit_of(u)
        here = pl.ds(pl.multiple_of(q * half, half), half)

        @pl.when(mid | (u < NHALF - 4))
        def _():
            wait_load(q)

        def tile(n, part):
            cs = pl.ds(pl.multiple_of(n * tn, tn), tn)
            return part + squares(far_product(here, cs))

        keep_squares(q, lax.fori_loop(0, ntile, tile, jnp.zeros((half, 128), jnp.float32)))
        return None

    def column_unit(k):
        return jnp.where(k < 2, side, 1 - side) * gs + 2 + lax.rem(k, 2)

    def column_step(n):
        w_from_partner(n)

        @pl.when(n == 0)
        def _():
            for k in range(4):
                for e in range(2):
                    wait_load(column_unit(jnp.int32(k)) * 2 + e)

        cs = pl.ds(pl.multiple_of(n * wch, wch), wch)

        def rows_of(k, _):
            here = pl.ds(pl.multiple_of(column_unit(k) * unit, unit), unit)
            far_product(here, cs)
            return None

        lax.fori_loop(0, 4, rows_of, None)

        @pl.when(n == NWC - 1)
        def _():
            def sums(k, _):
                q = column_unit(k // 2) * 2 + lax.rem(k, 2)
                here = pl.ds(pl.multiple_of(q * half, half), half)

                def tile(m, part):
                    return part + squares(acc[here, pl.ds(pl.multiple_of(m * tn, tn), tn)])

                keep_squares(q, lax.fori_loop(0, ntile, tile, jnp.zeros((half, 128), jnp.float32)))
                return None

            lax.fori_loop(0, 8, sums, None)

    def slot_body(i, _):
        @pl.when(i == LOADS)
        def _():
            early_loads()

        @pl.when(end & (i == LOADS))
        def _():
            pl.semaphore_signal(credit_z, inc=1, device_id=(x, z_in, t), device_id_type=MESH)
            for cc in range(2):
                pl.semaphore_signal(credit_y, inc=1, device_id=(x, z, (1 - y) * 2 + cc), device_id_type=MESH)

        comm(i)

        @pl.when(i == LOCAL0 - 1)
        def _():
            own_w.wait()
            wait_bytes(wl.at[1], recv_dw)
            wait_bytes(ap, recv_da)
            for cp in local_loads(0):
                cp.start()

        @pl.when((i >= LOCAL0) & (i < LOCAL0 + NUNIT))
        def _():
            local_unit(i - LOCAL0)

        @pl.when(end & (i == WREADY))
        def _():
            lax.fori_loop(0, NWC, lambda n, _: (w_from_partner(n), None)[1], None)

        jc = i - COLS0

        @pl.when(mid & (jc >= 0) & (jc < WS) & (lax.rem(jc, 2) == 0))
        def _():
            column_step(jc // 2)

        lo = jnp.where(end, step_count(i - 1, END_UNITS), step_count(i - 1, MID_UNITS))
        hi = jnp.where(end, step_count(i, END_UNITS), step_count(i, MID_UNITS))
        lax.fori_loop(lo, hi, remote_unit, None)
        return None

    lax.fori_loop(0, NSLOT, slot_body, None)

    for k in range(1, 4):
        remote(ss_loc, ss_all.at[z], send_ss.at[k - 1], recv_ss.at[z], (x, lax.rem(z + k, 4), t)).start()
    wait_bytes(wl.at[1], send_dw)
    wait_bytes(ap, send_da)
    wait_bytes(wr.at[0], send_wd)
    wait_bytes(wr.at[0, pl.ds(0, kb // 2)], send_wx)
    wait_bytes(wr.at[0, pl.ds(0, kb // 2)], send_yw)

    @pl.when(end)
    def _():
        wait_bytes(ax.at[pl.ds(0, FAR + NEAR)], send_ya)
        wait_bytes(ax.at[pl.ds(0, FAR)], send_zi)

    @pl.when(mid)
    def _():
        wait_bytes(ax.at[pl.ds(0, FAR)], send_ya)
        wait_bytes(ax.at[pl.ds(0, 2 * FAR)], send_zi)
        wait_bytes(ax.at[pl.ds(0, 2 * FAR + NEAR - 1)], send_zo)
        wait_bytes(ax.at[0], send_first)

    for k in range(1, 4):
        src = lax.rem(z + k, 4)
        remote(ss_loc, ss_all.at[src], send_ss.at[k - 1], recv_ss.at[src], (x, src, t)).wait_recv()
        remote(ss_loc, ss_all.at[src], send_ss.at[k - 1], recv_ss.at[src], (x, src, t)).wait_send()
    ss_all[z] = ss_loc[...]

def finish_kernel(h, ss, g, h_out, n_out, hbuf, nbuf, sem):
    rows, cols = h.shape
    step_rows = rows // NHALF

    def copies(q):
        slot = lax.rem(q, NBUF)
        here = pl.ds(pl.multiple_of(q * step_rows, step_rows), step_rows)
        return (pltpu.make_async_copy(hbuf.at[slot], h_out.at[here], sem.at[slot, 0]),
                pltpu.make_async_copy(nbuf.at[slot], n_out.at[here], sem.at[slot, 1]))

    def step(q, _):
        slot = lax.rem(q, NBUF)

        @pl.when(q >= NBUF)
        def _():
            for cp in copies(q - NBUF):
                cp.wait()

        total = ss[0, q] + ss[1, q] + ss[2, q] + ss[3, q]
        inv = lax.rsqrt(total / (cols * 4) + EPS_NORM)
        col = jnp.broadcast_to(inv, (128, 128)).T
        rs = pl.ds(pl.multiple_of(q * 128, 128), 128)
        for m in range(cols // 128):
            cs = slice(m * 128, (m + 1) * 128)
            v = h[rs, cs]
            hbuf[slot, :, cs] = v.astype(jnp.bfloat16)
            nbuf[slot, :, cs] = (v * col * g[:, cs]).astype(jnp.bfloat16)
        for cp in copies(q):
            cp.start()
        return None

    lax.fori_loop(0, NHALF, step, None)

    def drain(q, _):
        for cp in copies(q):
            cp.wait()
        return None

    lax.fori_loop(NHALF - NBUF, NHALF, drain, None)


def solution(mesh):
    def local_step(attn_blk, w_blk, res_blk, gain_blk):
        kb = attn_blk.shape[1]
        rows, cols = res_blk.shape
        unit = rows // NUNIT
        any_spec = pl.BlockSpec(memory_space=pl.ANY)
        vmem_spec = pl.BlockSpec(memory_space=pltpu.VMEM)
        bf16, f32 = jnp.bfloat16, jnp.float32
        dma = pltpu.SemaphoreType.DMA
        h, ss, _, _ = pl.pallas_call(
            kernel,
            out_shape=(
                pltpu.VMEM((rows, cols), f32),
                pltpu.VMEM((4, NHALF, 1, 128), f32),
                jax.ShapeDtypeStruct((NCH, 2, rows // NCH, kb), bf16),
                jax.ShapeDtypeStruct((rows, kb), bf16),
            ),
            in_specs=[any_spec, any_spec, any_spec],
            out_specs=(vmem_spec, vmem_spec, any_spec, any_spec),
            scratch_shapes=[
                pltpu.VMEM((2, kb, cols), bf16),
                pltpu.VMEM((2, kb, cols), bf16),
                pltpu.VMEM((2, 2, unit, kb), bf16),
                pltpu.VMEM((2, unit, cols), bf16),
                pltpu.VMEM((NHALF, 1, 128), f32),
                dma((NCH,)), dma, dma, dma, dma,
                dma((NWC,)), dma((NWC,)), dma((NWC,)), dma, dma,
                dma, dma, dma, dma,
                dma((2, 3)), dma, dma((NHALF,)), dma((NSUB,)), dma,
                pltpu.SemaphoreType.REGULAR, pltpu.SemaphoreType.REGULAR,
                dma((3,)), dma((4,)),
            ],
            compiler_params=pltpu.CompilerParams(
                collective_id=0, has_side_effects=True, vmem_limit_bytes=44 * 1024 * 1024),
            name="gather_project",
        )(attn_blk, w_blk, res_blk)
        return pl.pallas_call(
            finish_kernel,
            out_shape=(jax.ShapeDtypeStruct((rows, cols), bf16),) * 2,
            in_specs=[vmem_spec, vmem_spec, vmem_spec],
            out_specs=(any_spec, any_spec),
            scratch_shapes=[pltpu.VMEM((NBUF, rows // NHALF, cols), bf16)] * 2 + [dma((NBUF, 2))],
            compiler_params=pltpu.CompilerParams(vmem_limit_bytes=8 * 1024 * 1024),
            name="norm_store",
        )(h, ss, gain_blk.reshape(1, cols))

    row_spec = P(("dp", "tp"), "tp2")
    return jax.shard_map(local_step, mesh=mesh, in_specs=(P("dp", "tp"), P("tp", "tp2"), row_spec, P("tp2")), out_specs=(row_spec, row_spec), check_vma=False)
```

```python
import functools

import jax
import jax.numpy as jnp
from jax import lax
from jax.experimental import pallas as pl
from jax.experimental.pallas import tpu as pltpu
from jax.sharding import PartitionSpec as P

EPS_NORM = 1e-6
MESH = pl.DeviceIdType.MESH
NCH = 64
FAR = NCH // 4
NEAR = NCH // 8
NWC = 8
WS = 2 * NWC
NUNIT = 8
NHALF = 2 * NUNIT
GRP = NCH // NUNIT
HGRP = NCH // NHALF
LATE = FAR // 2
NBUF = 4
NDIRECT = 2
PIECES = (2, 3, 0, 1)
NSUB = 4
AHEAD = 12
NSLOT = 2 * FAR + NEAR + 1
LOCAL0 = 6
LOADS = 16
WREADY = WS + 2
COLS0 = FAR + 4


def step_count(i, slots):
    n = jnp.int32(0)
    for s in slots:
        n = n + jnp.where(i >= s, 1, 0)
    return n


END_UNITS = (19, 19, 20, 20, 21, 22, 24, 25, 28, 29, 32, 33, 36, 37, 39, 40)
MID_UNITS = (35, 35, 36, 36, 37, 37, 38, 38)


def kernel(a, w, r, acc, ss_all, ax, ap, wl, wr, abuf, rbuf, ss_loc,
           recv_a, send_ya, send_yw, send_zi, send_zo, recv_wy, recv_wx, recv_wd, send_wx, send_wd,
           recv_da, recv_dw, send_da, send_dw, load_sem, load_w, load_a, recv_sub, send_first, send_pieces, credit_z, credit_y, send_ss, recv_ss):
    x = lax.axis_index("dp")
    z = lax.axis_index("tp2")
    t = lax.axis_index("tp")
    y = t // 2
    c = t % 2
    rows, cols = acc.shape
    kb = w.shape[0]
    ch = rows // NCH
    wch = cols // NWC
    unit = ch * GRP
    half = ch * HGRP
    sub = ch // NSUB
    side = z // 2
    end = (z == 0) | (z == 3)
    mid = (z == 1) | (z == 2)
    base = side * (NCH // 2)
    other = (1 - side) * (NCH // 2)
    z_in = jnp.where(side == 0, z + 1, z - 1)
    z_out = jnp.where(side == 0, z - 1, z + 1)

    partner = (x, z, y * 2 + 1 - c)
    x_peer = (1 - x, z, t)
    y_same = (x, z, (1 - y) * 2 + c)
    y_cross = (x, z, (1 - y) * 2 + 1 - c)

    def remote(src, dst, send, recv, dev):
        return pltpu.make_async_remote_copy(
            src_ref=src, dst_ref=dst, send_sem=send, recv_sem=recv, device_id=dev, device_id_type=MESH)

    def wait_bytes(ref, sem):
        pltpu.make_async_copy(ref, ref, sem).wait()

    barrier = pltpu.get_barrier_semaphore()
    for dev in (partner, x_peer, y_same, y_cross):
        pl.semaphore_signal(barrier, inc=1, device_id=dev, device_id_type=MESH)
    for k in range(1, 4):
        pl.semaphore_signal(barrier, inc=1, device_id=(x, lax.rem(z + k, 4), t), device_id_type=MESH)
    pl.semaphore_wait(barrier, 7)

    def mp(start, j):
        return start + FAR + lax.rem(j + NEAR, FAR)

    def chunk_rows(q):
        return pl.ds(pl.multiple_of(q * ch, ch), ch)

    def send_y_a(q, dst=None):
        dst = ax.at[q, c] if dst is None else dst
        for cc in range(2):
            row = ((1 - y) * 2 + cc) * rows + q * ch
            remote(a.at[pl.ds(pl.multiple_of(row, ch), ch)], dst, send_ya, recv_a.at[q],
                   (x, z, (1 - y) * 2 + cc)).start()

    def send_y_pieces(q, pieces, recv):
        for k in pieces:
            for cc in range(2):
                row = ((1 - y) * 2 + cc) * rows + q * ch + k * sub
                remote(a.at[pl.ds(pl.multiple_of(row, sub), sub)], ax.at[q, c, pl.ds(k * sub, sub)], send_first,
                       recv(k), (x, z, (1 - y) * 2 + cc)).start()

    def w_part(part, n):
        return (pl.ds(pl.multiple_of(part * (kb // 2), kb // 2), kb // 2), pl.ds(pl.multiple_of(n * wch, wch), wch))

    def send_y_w(n):
        rs, cs = w_part(x, n)
        remote(w.at[rs, cs], wr.at[c, rs, cs], send_yw, recv_wy.at[n], y_same).start()

    def y_sends(i):
        iw = jnp.where(end, i, i - FAR)
        ia = jnp.where(end, i - WS, i)

        @pl.when((iw >= 0) & (iw < WS) & (lax.rem(iw, 2) == 0))
        def _():
            send_y_w(iw // 2)

        @pl.when(end & (ia >= 0) & (ia < FAR))
        def _():
            send_y_a(base + ia)

        @pl.when(end & (ia == FAR))
        def _():
            pl.semaphore_wait(credit_y, 2)

        @pl.when(end & (ia >= FAR) & (ia < FAR + NEAR))
        def _():
            send_y_a(base + ia, wl.at[c, chunk_rows(base + ia)])

        @pl.when(mid & (ia == 0))
        def _():
            q = mp(base, 0)
            send_y_pieces(q, PIECES, lambda k: recv_sub.at[k])

        @pl.when(end & (i == 0))
        def _():
            q = mp(base, 0)
            send_y_pieces(q, range(NDIRECT), lambda k: recv_a.at[q])

        @pl.when(mid & (ia >= 1) & (ia < FAR))
        def _():
            send_y_a(mp(base, ia))

    lax.fori_loop(0, AHEAD, lambda i, _: (y_sends(i), None)[1], None)

    remote(w, wl.at[1], send_dw, recv_dw, partner).start()
    prow = pl.ds(pl.multiple_of((y * 2 + 1 - c) * rows, rows), rows)
    remote(a.at[prow], ap, send_da, recv_da, partner).start()
    own_w = pltpu.make_async_copy(w, wl.at[0], load_w)
    own_w.start()

    def load(q):
        here = pl.ds(pl.multiple_of(q * ch, ch), ch)
        for b in range(2):
            pltpu.make_async_copy(ax.at[q, b], wl.at[b, here], load_a.at[q // HGRP]).start()

    def arrive(q, i):
        wait_bytes(ax.at[q], recv_a.at[q])

        @pl.when(i >= LOADS)
        def _():
            load(q)

    def arrive_late(q):
        wait_bytes(wl.at[:, chunk_rows(q)], recv_a.at[q])

    def pass_out_late(q):
        remote(ax.at[q], wl.at[:, chunk_rows(q)], send_zo, recv_a.at[q], (x, z_out, t)).start()

    def pass_in(q):
        remote(ax.at[q], ax.at[q], send_zi, recv_a.at[q], (x, z_in, t)).start()

    def pass_out(q):
        remote(ax.at[q], ax.at[q], send_zo, recv_a.at[q], (x, z_out, t)).start()

    def w_from_y(n):
        rs, cs = w_part(x, n)
        part = wr.at[c, rs, cs]
        wait_bytes(part, recv_wy.at[n])
        remote(part, part, send_wx, recv_wx.at[n], x_peer).start()
        remote(part, part, send_wd, recv_wd.at[n], partner).start()

    def w_from_x(n):
        rs, cs = w_part(1 - x, n)
        part = wr.at[c, rs, cs]
        wait_bytes(part, recv_wx.at[n])
        remote(part, part, send_wd, recv_wd.at[n], partner).start()

    def w_from_partner(n):
        cs = pl.ds(pl.multiple_of(n * wch, wch), wch)
        wait_bytes(wr.at[1 - c, :, cs], recv_wd.at[n])

    def z_chunk(j):
        own = (j == 0) | (lax.rem(j, 2) == 1)
        first = jnp.where(own, mp(base, (j + 1) // 2), mp(other, j // 2 - 1))
        return jnp.where(j < 2 * NEAR - 1, first, jnp.where(j < NEAR + FAR, mp(other, j - NEAR), other + j - NEAR - FAR))

    def comm(i):
        y_sends(i + AHEAD)
        iw = jnp.where(end, i, i - FAR)
        odd = lax.rem(i, 2) == 1

        @pl.when(odd & (iw >= 1) & (iw < WS))
        def _():
            w_from_y(iw // 2)

        @pl.when(odd & (iw >= 3) & (iw < WS + 2))
        def _():
            w_from_x((iw - 3) // 2)

        @pl.when(end)
        def _():
            @pl.when((i >= WS) & (i < WS + FAR))
            def _():
                q = base + i - WS
                arrive(q, i)
                pass_in(q)

            @pl.when((i >= WS + FAR) & (i < WS + FAR + NEAR))
            def _():
                arrive_late(base + i - WS)

            nlate = 1 + 2 * FAR + NEAR - LATE

            @pl.when((i >= 1) & (i < nlate))
            def _():
                arrive(z_chunk(i - 1), i)

            @pl.when((i >= nlate) & (i < nlate + LATE))
            def _():
                arrive_late(z_chunk(i - 1))

        @pl.when(mid)
        def _():
            @pl.when(i == 0)
            def _():
                q = mp(base, 0)
                for k in PIECES:
                    piece = ax.at[q, :, pl.ds(k * sub, sub)]
                    wait_bytes(piece, recv_sub.at[k])
                    if k >= NDIRECT:
                        remote(piece, piece, send_pieces, recv_a.at[q], (x, z_out, t)).start()
                pass_in(q)

            @pl.when((i >= 1) & (i < FAR))
            def _():
                q = mp(base, i)
                arrive(q, i)

                @pl.when(i < NEAR)
                def _():
                    pass_out(q)

                pass_in(q)

            @pl.when((i >= 1) & (i < 1 + FAR))
            def _():
                q = mp(other, i - 1)
                arrive(q, i)
                pass_out(q)

            @pl.when((i >= WS + 1) & (i < WS + 1 + FAR))
            def _():
                q = base + i - WS - 1
                arrive(q, i)
                pass_in(q)

            @pl.when((i >= WS + 2) & (i < WS + 2 + FAR))
            def _():
                q = other + i - WS - 2
                arrive(q, i)

                @pl.when(i < WS + 2 + FAR - LATE)
                def _():
                    pass_out(q)

                @pl.when(i == WS + 2 + FAR - LATE)
                def _():
                    pl.semaphore_wait(credit_z, 1)

                @pl.when(i >= WS + 2 + FAR - LATE)
                def _():
                    pass_out_late(q)

    def early_loads():
        def from_z(j, _):
            load(jnp.where(end, z_chunk(j), mp(other, j)))
            return None

        lax.fori_loop(0, LOADS - 1, from_z, None)

        def from_y(j, _):
            load(mp(base, j))
            return None

        lax.fori_loop(0, jnp.where(end, 0, LOADS), from_y, None)

    tn = min(512, cols)
    ntile = cols // tn

    def local_loads(u):
        slot = lax.rem(u, 2)
        here = pl.ds(pl.multiple_of(u * unit, unit), unit)
        mine = pl.ds(pl.multiple_of(t * rows + u * unit, unit), unit)
        return (pltpu.make_async_copy(a.at[mine], abuf.at[slot, 0], load_sem.at[slot, 0]),
                pltpu.make_async_copy(ap.at[here], abuf.at[slot, 1], load_sem.at[slot, 1]),
                pltpu.make_async_copy(r.at[here], rbuf.at[slot], load_sem.at[slot, 2]))

    def local_unit(u):
        slot = lax.rem(u, 2)
        here = pl.ds(pl.multiple_of(u * unit, unit), unit)
        for cp in local_loads(u):
            cp.wait()

        @pl.when(u + 1 < NUNIT)
        def _():
            for cp in local_loads(u + 1):
                cp.start()

        def tile(n, _):
            cs = pl.ds(pl.multiple_of(n * tn, tn), tn)
            p0 = jnp.dot(abuf[slot, 0], wl[0, :, cs], preferred_element_type=jnp.float32)
            p1 = jnp.dot(abuf[slot, 1], wl[1, :, cs], preferred_element_type=jnp.float32)
            acc[here, cs] = (rbuf[slot, :, cs].astype(jnp.float32) + p0.astype(jnp.bfloat16).astype(jnp.float32)
                             + p1.astype(jnp.bfloat16).astype(jnp.float32))
            return None

        lax.fori_loop(0, ntile, tile, None)

    gs = NUNIT // 2

    def unit_of(u):
        b = side * NUNIT
        o = (1 - side) * NUNIT
        end_order = (b + 6, b + 7, o + 6, o + 7, b, o + 4, b + 1, o + 5, b + 2, o, b + 3, o + 1, b + 4, o + 2, b + 5, o + 3)
        mid_order = (b, b + 1, o, o + 1, b + 2, b + 3, o + 2, o + 3) + (0,) * NUNIT
        q = jnp.int32(0)
        for k in range(NHALF):
            q = q + jnp.where(u == k, jnp.where(end, end_order[k], mid_order[k]), 0)
        return q

    def wait_load(q):
        here = pl.ds(pl.multiple_of(q * half, half), half)
        wait_bytes(wl.at[:, here], load_a.at[q])

    def far_product(here, cs):
        p0 = jnp.dot(wl[0, here, :], wr[0, :, cs], preferred_element_type=jnp.float32)
        p1 = jnp.dot(wl[1, here, :], wr[1, :, cs], preferred_element_type=jnp.float32)
        v = acc[here, cs] + (p0.astype(jnp.bfloat16).astype(jnp.float32) + p1.astype(jnp.bfloat16).astype(jnp.float32))
        acc[here, cs] = v
        return v

    def squares(v):
        sq = v * v
        part = sq[:, :128]
        for k in range(1, sq.shape[1] // 128):
            part = part + sq[:, k * 128:(k + 1) * 128]
        return part

    def keep_squares(q, part):
        ss_loc[q] = jnp.sum(part.T, axis=0, keepdims=True)

    def remote_unit(u, _):
        q = unit_of(u)
        here = pl.ds(pl.multiple_of(q * half, half), half)

        @pl.when(mid | (u < NHALF - 4))
        def _():
            wait_load(q)

        def tile(n, part):
            cs = pl.ds(pl.multiple_of(n * tn, tn), tn)
            return part + squares(far_product(here, cs))

        keep_squares(q, lax.fori_loop(0, ntile, tile, jnp.zeros((half, 128), jnp.float32)))
        return None

    def column_unit(k):
        return jnp.where(k < 2, side, 1 - side) * gs + 2 + lax.rem(k, 2)

    def column_step(n):
        w_from_partner(n)

        @pl.when(n == 0)
        def _():
            for k in range(4):
                for e in range(2):
                    wait_load(column_unit(jnp.int32(k)) * 2 + e)

        cs = pl.ds(pl.multiple_of(n * wch, wch), wch)

        def rows_of(k, _):
            here = pl.ds(pl.multiple_of(column_unit(k) * unit, unit), unit)
            far_product(here, cs)
            return None

        lax.fori_loop(0, 4, rows_of, None)

        @pl.when(n == NWC - 1)
        def _():
            def sums(k, _):
                q = column_unit(k // 2) * 2 + lax.rem(k, 2)
                here = pl.ds(pl.multiple_of(q * half, half), half)

                def tile(m, part):
                    return part + squares(acc[here, pl.ds(pl.multiple_of(m * tn, tn), tn)])

                keep_squares(q, lax.fori_loop(0, ntile, tile, jnp.zeros((half, 128), jnp.float32)))
                return None

            lax.fori_loop(0, 8, sums, None)

    def slot_body(i, _):
        @pl.when(i == LOADS)
        def _():
            early_loads()

        @pl.when(end & (i == LOADS))
        def _():
            pl.semaphore_signal(credit_z, inc=1, device_id=(x, z_in, t), device_id_type=MESH)
            for cc in range(2):
                pl.semaphore_signal(credit_y, inc=1, device_id=(x, z, (1 - y) * 2 + cc), device_id_type=MESH)

        comm(i)

        @pl.when(i == LOCAL0 - 1)
        def _():
            own_w.wait()
            wait_bytes(wl.at[1], recv_dw)
            wait_bytes(ap, recv_da)
            for cp in local_loads(0):
                cp.start()

        @pl.when((i >= LOCAL0) & (i < LOCAL0 + NUNIT))
        def _():
            local_unit(i - LOCAL0)

        @pl.when(end & (i == WREADY))
        def _():
            lax.fori_loop(0, NWC, lambda n, _: (w_from_partner(n), None)[1], None)

        jc = i - COLS0

        @pl.when(mid & (jc >= 0) & (jc < WS) & (lax.rem(jc, 2) == 0))
        def _():
            column_step(jc // 2)

        lo = jnp.where(end, step_count(i - 1, END_UNITS), step_count(i - 1, MID_UNITS))
        hi = jnp.where(end, step_count(i, END_UNITS), step_count(i, MID_UNITS))
        lax.fori_loop(lo, hi, remote_unit, None)
        return None

    lax.fori_loop(0, NSLOT, slot_body, None)

    for k in range(1, 4):
        remote(ss_loc, ss_all.at[z], send_ss.at[k - 1], recv_ss.at[z], (x, lax.rem(z + k, 4), t)).start()
    wait_bytes(wl.at[1], send_dw)
    wait_bytes(ap, send_da)
    wait_bytes(wr.at[0], send_wd)
    wait_bytes(wr.at[0, pl.ds(0, kb // 2)], send_wx)
    wait_bytes(wr.at[0, pl.ds(0, kb // 2)], send_yw)

    @pl.when(end)
    def _():
        wait_bytes(ax.at[pl.ds(0, FAR + NEAR)], send_ya)
        wait_bytes(ax.at[0, :, pl.ds(0, NDIRECT * sub)], send_first)
        wait_bytes(ax.at[pl.ds(0, FAR)], send_zi)

    @pl.when(mid)
    def _():
        wait_bytes(ax.at[pl.ds(0, FAR - 1)], send_ya)
        wait_bytes(ax.at[pl.ds(0, 2 * FAR)], send_zi)
        wait_bytes(ax.at[pl.ds(0, 2 * FAR + NEAR - 1)], send_zo)
        wait_bytes(ax.at[0], send_first)
        wait_bytes(ax.at[0, :, pl.ds(0, (NSUB - NDIRECT) * sub)], send_pieces)

    for k in range(1, 4):
        src = lax.rem(z + k, 4)
        remote(ss_loc, ss_all.at[src], send_ss.at[k - 1], recv_ss.at[src], (x, src, t)).wait_recv()
        remote(ss_loc, ss_all.at[src], send_ss.at[k - 1], recv_ss.at[src], (x, src, t)).wait_send()
    ss_all[z] = ss_loc[...]

def finish_kernel(h, ss, g, h_out, n_out, hbuf, nbuf, sem):
    rows, cols = h.shape
    step_rows = rows // NHALF

    def copies(q):
        slot = lax.rem(q, NBUF)
        here = pl.ds(pl.multiple_of(q * step_rows, step_rows), step_rows)
        return (pltpu.make_async_copy(hbuf.at[slot], h_out.at[here], sem.at[slot, 0]),
                pltpu.make_async_copy(nbuf.at[slot], n_out.at[here], sem.at[slot, 1]))

    def step(q, _):
        slot = lax.rem(q, NBUF)

        @pl.when(q >= NBUF)
        def _():
            for cp in copies(q - NBUF):
                cp.wait()

        total = ss[0, q] + ss[1, q] + ss[2, q] + ss[3, q]
        inv = lax.rsqrt(total / (cols * 4) + EPS_NORM)
        col = jnp.broadcast_to(inv, (128, 128)).T
        rs = pl.ds(pl.multiple_of(q * 128, 128), 128)
        for m in range(cols // 128):
            cs = slice(m * 128, (m + 1) * 128)
            v = h[rs, cs]
            hbuf[slot, :, cs] = v.astype(jnp.bfloat16)
            nbuf[slot, :, cs] = (v * col * g[:, cs]).astype(jnp.bfloat16)
        for cp in copies(q):
            cp.start()
        return None

    lax.fori_loop(0, NHALF, step, None)

    def drain(q, _):
        for cp in copies(q):
            cp.wait()
        return None

    lax.fori_loop(NHALF - NBUF, NHALF, drain, None)


def solution(mesh):
    def local_step(attn_blk, w_blk, res_blk, gain_blk):
        kb = attn_blk.shape[1]
        rows, cols = res_blk.shape
        unit = rows // NUNIT
        any_spec = pl.BlockSpec(memory_space=pl.ANY)
        vmem_spec = pl.BlockSpec(memory_space=pltpu.VMEM)
        bf16, f32 = jnp.bfloat16, jnp.float32
        dma = pltpu.SemaphoreType.DMA
        h, ss, _, _ = pl.pallas_call(
            kernel,
            out_shape=(
                pltpu.VMEM((rows, cols), f32),
                pltpu.VMEM((4, NHALF, 1, 128), f32),
                jax.ShapeDtypeStruct((NCH, 2, rows // NCH, kb), bf16),
                jax.ShapeDtypeStruct((rows, kb), bf16),
            ),
            in_specs=[any_spec, any_spec, any_spec],
            out_specs=(vmem_spec, vmem_spec, any_spec, any_spec),
            scratch_shapes=[
                pltpu.VMEM((2, kb, cols), bf16),
                pltpu.VMEM((2, kb, cols), bf16),
                pltpu.VMEM((2, 2, unit, kb), bf16),
                pltpu.VMEM((2, unit, cols), bf16),
                pltpu.VMEM((NHALF, 1, 128), f32),
                dma((NCH,)), dma, dma, dma, dma,
                dma((NWC,)), dma((NWC,)), dma((NWC,)), dma, dma,
                dma, dma, dma, dma,
                dma((2, 3)), dma, dma((NHALF,)), dma((NSUB,)), dma, dma,
                pltpu.SemaphoreType.REGULAR, pltpu.SemaphoreType.REGULAR,
                dma((3,)), dma((4,)),
            ],
            compiler_params=pltpu.CompilerParams(
                collective_id=0, has_side_effects=True, vmem_limit_bytes=44 * 1024 * 1024),
            name="gather_project",
        )(attn_blk, w_blk, res_blk)
        return pl.pallas_call(
            finish_kernel,
            out_shape=(jax.ShapeDtypeStruct((rows, cols), bf16),) * 2,
            in_specs=[vmem_spec, vmem_spec, vmem_spec],
            out_specs=(any_spec, any_spec),
            scratch_shapes=[pltpu.VMEM((NBUF, rows // NHALF, cols), bf16)] * 2 + [dma((NBUF, 2))],
            compiler_params=pltpu.CompilerParams(vmem_limit_bytes=8 * 1024 * 1024),
            name="norm_store",
        )(h, ss, gain_blk.reshape(1, cols))

    row_spec = P(("dp", "tp"), "tp2")
    return jax.shard_map(local_step, mesh=mesh, in_specs=(P("dp", "tp"), P("tp", "tp2"), row_spec, P("tp2")), out_specs=(row_spec, row_spec), check_vma=False)
```

```python
import functools

import jax
import jax.numpy as jnp
from jax import lax
from jax.experimental import pallas as pl
from jax.experimental.pallas import tpu as pltpu
from jax.sharding import PartitionSpec as P

EPS_NORM = 1e-6
MESH = pl.DeviceIdType.MESH
NCH = 64
FAR = NCH // 4
NEAR = NCH // 8
NWC = 8
WS = 2 * NWC
NUNIT = 8
NHALF = 2 * NUNIT
GRP = NCH // NUNIT
HGRP = NCH // NHALF
LATE = FAR // 2
NBUF = 4
NDIRECT = 2
PIECES = (2, 3, 0, 1)
NSUB = 4
AHEAD = 12
NSLOT = 2 * FAR + NEAR + 1
LOCAL0 = 6
LOADS = 16
WREADY = WS + 2
COLS0 = FAR + 4


def step_count(i, slots):
    n = jnp.int32(0)
    for s in slots:
        n = n + jnp.where(i >= s, 1, 0)
    return n


END_UNITS = (19, 19, 20, 20, 21, 22, 24, 25, 28, 29, 32, 33, 35, 36, 38, 40)
MID_UNITS = (35, 35, 36, 36, 37, 37, 38, 38)


def kernel(a, w, r, acc, ss_all, ax, ap, wl, wr, abuf, rbuf, ss_loc,
           recv_a, send_ya, send_yw, send_zi, send_zo, recv_wy, recv_wx, recv_wd, send_wx, send_wd,
           recv_da, recv_dw, send_da, send_dw, load_sem, load_w, load_a, recv_sub, send_first, send_pieces, credit_z, credit_y, send_ss, recv_ss):
    x = lax.axis_index("dp")
    z = lax.axis_index("tp2")
    t = lax.axis_index("tp")
    y = t // 2
    c = t % 2
    rows, cols = acc.shape
    kb = w.shape[0]
    ch = rows // NCH
    wch = cols // NWC
    unit = ch * GRP
    half = ch * HGRP
    sub = ch // NSUB
    side = z // 2
    end = (z == 0) | (z == 3)
    mid = (z == 1) | (z == 2)
    base = side * (NCH // 2)
    other = (1 - side) * (NCH // 2)
    z_in = jnp.where(side == 0, z + 1, z - 1)
    z_out = jnp.where(side == 0, z - 1, z + 1)

    partner = (x, z, y * 2 + 1 - c)
    x_peer = (1 - x, z, t)
    y_same = (x, z, (1 - y) * 2 + c)
    y_cross = (x, z, (1 - y) * 2 + 1 - c)

    def remote(src, dst, send, recv, dev):
        return pltpu.make_async_remote_copy(
            src_ref=src, dst_ref=dst, send_sem=send, recv_sem=recv, device_id=dev, device_id_type=MESH)

    def wait_bytes(ref, sem):
        pltpu.make_async_copy(ref, ref, sem).wait()

    barrier = pltpu.get_barrier_semaphore()
    for dev in (partner, x_peer, y_same, y_cross):
        pl.semaphore_signal(barrier, inc=1, device_id=dev, device_id_type=MESH)
    for k in range(1, 4):
        pl.semaphore_signal(barrier, inc=1, device_id=(x, lax.rem(z + k, 4), t), device_id_type=MESH)
    pl.semaphore_wait(barrier, 7)

    def mp(start, j):
        return start + FAR + lax.rem(j + NEAR, FAR)

    def private(m):
        return base + FAR + jnp.where(m < NEAR // 2, m, NEAR // 2 + lax.rem(m + NEAR // 4, NEAR // 2))

    def chunk_rows(q):
        return pl.ds(pl.multiple_of(q * ch, ch), ch)

    def send_y_a(q, dst=None):
        dst = ax.at[q, c] if dst is None else dst
        for cc in range(2):
            row = ((1 - y) * 2 + cc) * rows + q * ch
            remote(a.at[pl.ds(pl.multiple_of(row, ch), ch)], dst, send_ya, recv_a.at[q],
                   (x, z, (1 - y) * 2 + cc)).start()

    def send_y_pieces(q, pieces, recv):
        for k in pieces:
            for cc in range(2):
                row = ((1 - y) * 2 + cc) * rows + q * ch + k * sub
                remote(a.at[pl.ds(pl.multiple_of(row, sub), sub)], ax.at[q, c, pl.ds(k * sub, sub)], send_first,
                       recv(k), (x, z, (1 - y) * 2 + cc)).start()

    def w_part(part, n):
        return (pl.ds(pl.multiple_of(part * (kb // 2), kb // 2), kb // 2), pl.ds(pl.multiple_of(n * wch, wch), wch))

    def send_y_w(n):
        rs, cs = w_part(x, n)
        remote(w.at[rs, cs], wr.at[c, rs, cs], send_yw, recv_wy.at[n], y_same).start()

    def y_sends(i):
        iw = jnp.where(end, i, i - FAR)
        ia = jnp.where(end, i - WS, i)

        @pl.when((iw >= 0) & (iw < WS) & (lax.rem(iw, 2) == 0))
        def _():
            send_y_w(iw // 2)

        @pl.when(end & (ia >= 0) & (ia < FAR))
        def _():
            send_y_a(base + ia)

        @pl.when(end & (ia == FAR))
        def _():
            pl.semaphore_wait(credit_y, 2)

        @pl.when(end & (ia >= FAR) & (ia < FAR + NEAR))
        def _():
            q = private(ia - FAR)
            send_y_a(q, wl.at[c, chunk_rows(q)])

        @pl.when(mid & (ia == 0))
        def _():
            q = mp(base, 0)
            send_y_pieces(q, PIECES, lambda k: recv_sub.at[k])

        @pl.when(end & (i == 0))
        def _():
            q = mp(base, 0)
            send_y_pieces(q, range(NDIRECT), lambda k: recv_a.at[q])

        @pl.when(mid & (ia >= 1) & (ia < FAR))
        def _():
            send_y_a(mp(base, ia))

    lax.fori_loop(0, AHEAD, lambda i, _: (y_sends(i), None)[1], None)

    remote(w, wl.at[1], send_dw, recv_dw, partner).start()
    prow = pl.ds(pl.multiple_of((y * 2 + 1 - c) * rows, rows), rows)
    remote(a.at[prow], ap, send_da, recv_da, partner).start()
    own_w = pltpu.make_async_copy(w, wl.at[0], load_w)
    own_w.start()
    ss_loc[...] = jnp.zeros_like(ss_loc)

    def load(q):
        here = pl.ds(pl.multiple_of(q * ch, ch), ch)
        for b in range(2):
            pltpu.make_async_copy(ax.at[q, b], wl.at[b, here], load_a.at[q // HGRP]).start()

    def arrive(q, i):
        wait_bytes(ax.at[q], recv_a.at[q])

        @pl.when(i >= LOADS)
        def _():
            load(q)

    def arrive_late(q):
        wait_bytes(wl.at[:, chunk_rows(q)], recv_a.at[q])

    def pass_out_late(q):
        remote(ax.at[q], wl.at[:, chunk_rows(q)], send_zo, recv_a.at[q], (x, z_out, t)).start()

    def pass_in(q):
        remote(ax.at[q], ax.at[q], send_zi, recv_a.at[q], (x, z_in, t)).start()

    def pass_out(q):
        remote(ax.at[q], ax.at[q], send_zo, recv_a.at[q], (x, z_out, t)).start()

    def w_from_y(n):
        rs, cs = w_part(x, n)
        part = wr.at[c, rs, cs]
        wait_bytes(part, recv_wy.at[n])
        remote(part, part, send_wx, recv_wx.at[n], x_peer).start()
        remote(part, part, send_wd, recv_wd.at[n], partner).start()

    def w_from_x(n):
        rs, cs = w_part(1 - x, n)
        part = wr.at[c, rs, cs]
        wait_bytes(part, recv_wx.at[n])
        remote(part, part, send_wd, recv_wd.at[n], partner).start()

    def w_from_partner(n):
        cs = pl.ds(pl.multiple_of(n * wch, wch), wch)
        wait_bytes(wr.at[1 - c, :, cs], recv_wd.at[n])

    def z_chunk(j):
        own = (j == 0) | (lax.rem(j, 2) == 1)
        first = jnp.where(own, mp(base, (j + 1) // 2), mp(other, j // 2 - 1))
        return jnp.where(j < 2 * NEAR - 1, first, jnp.where(j < NEAR + FAR, mp(other, j - NEAR), other + j - NEAR - FAR))

    def comm(i):
        y_sends(i + AHEAD)
        iw = jnp.where(end, i, i - FAR)
        odd = lax.rem(i, 2) == 1

        @pl.when(odd & (iw >= 1) & (iw < WS))
        def _():
            w_from_y(iw // 2)

        @pl.when(odd & (iw >= 3) & (iw < WS + 2))
        def _():
            w_from_x((iw - 3) // 2)

        @pl.when(end)
        def _():
            @pl.when((i >= WS) & (i < WS + FAR))
            def _():
                q = base + i - WS
                arrive(q, i)
                pass_in(q)

            @pl.when((i >= WS + FAR) & (i < WS + FAR + NEAR))
            def _():
                arrive_late(private(i - WS - FAR))

            nlate = 1 + 2 * FAR + NEAR - LATE

            @pl.when((i >= 1) & (i < nlate))
            def _():
                arrive(z_chunk(i - 1), i)

            @pl.when((i >= nlate) & (i < nlate + LATE))
            def _():
                arrive_late(z_chunk(i - 1))

        @pl.when(mid)
        def _():
            @pl.when(i == 0)
            def _():
                q = mp(base, 0)
                for k in PIECES:
                    piece = ax.at[q, :, pl.ds(k * sub, sub)]
                    wait_bytes(piece, recv_sub.at[k])
                    if k >= NDIRECT:
                        remote(piece, piece, send_pieces, recv_a.at[q], (x, z_out, t)).start()
                pass_in(q)

            @pl.when((i >= 1) & (i < FAR))
            def _():
                q = mp(base, i)
                arrive(q, i)

                @pl.when(i < NEAR)
                def _():
                    pass_out(q)

                pass_in(q)

            @pl.when((i >= 1) & (i < 1 + FAR))
            def _():
                q = mp(other, i - 1)
                arrive(q, i)
                pass_out(q)

            @pl.when((i >= WS + 1) & (i < WS + 1 + FAR))
            def _():
                q = base + i - WS - 1
                arrive(q, i)
                pass_in(q)

            @pl.when((i >= WS + 2) & (i < WS + 2 + FAR))
            def _():
                q = other + i - WS - 2
                arrive(q, i)

                @pl.when(i < WS + 2 + FAR - LATE)
                def _():
                    pass_out(q)

                @pl.when(i == WS + 2 + FAR - LATE)
                def _():
                    pl.semaphore_wait(credit_z, 1)

                @pl.when(i >= WS + 2 + FAR - LATE)
                def _():
                    pass_out_late(q)

    def early_loads():
        def from_z(j, _):
            load(jnp.where(end, z_chunk(j), mp(other, j)))
            return None

        lax.fori_loop(0, LOADS - 1, from_z, None)

        def from_y(j, _):
            load(mp(base, j))
            return None

        lax.fori_loop(0, jnp.where(end, 0, LOADS), from_y, None)

    tn = min(512, cols)
    ntile = cols // tn

    def local_loads(u):
        slot = lax.rem(u, 2)
        here = pl.ds(pl.multiple_of(u * unit, unit), unit)
        mine = pl.ds(pl.multiple_of(t * rows + u * unit, unit), unit)
        return (pltpu.make_async_copy(a.at[mine], abuf.at[slot, 0], load_sem.at[slot, 0]),
                pltpu.make_async_copy(ap.at[here], abuf.at[slot, 1], load_sem.at[slot, 1]),
                pltpu.make_async_copy(r.at[here], rbuf.at[slot], load_sem.at[slot, 2]))

    def local_unit(u):
        slot = lax.rem(u, 2)
        here = pl.ds(pl.multiple_of(u * unit, unit), unit)
        for cp in local_loads(u):
            cp.wait()

        @pl.when(u + 1 < NUNIT)
        def _():
            for cp in local_loads(u + 1):
                cp.start()

        def tile(n, _):
            cs = pl.ds(pl.multiple_of(n * tn, tn), tn)
            p0 = jnp.dot(abuf[slot, 0], wl[0, :, cs], preferred_element_type=jnp.float32)
            p1 = jnp.dot(abuf[slot, 1], wl[1, :, cs], preferred_element_type=jnp.float32)
            acc[here, cs] = (rbuf[slot, :, cs].astype(jnp.float32) + p0.astype(jnp.bfloat16).astype(jnp.float32)
                             + p1.astype(jnp.bfloat16).astype(jnp.float32))
            return None

        lax.fori_loop(0, ntile, tile, None)

    gs = NUNIT // 2

    def unit_of(u):
        b = side * NUNIT
        o = (1 - side) * NUNIT
        end_order = (b + 6, b + 7, o + 6, o + 7, b, o + 4, b + 1, o + 5, b + 2, o, b + 3, o + 1, b + 4, o + 2)
        mid_order = (b, b + 1, o, o + 1, b + 2, b + 3, o + 2, o + 3) + (0,) * NUNIT
        both = []
        for last in ((o + 3, b + 5), (b + 5, o + 3)):
            q = jnp.int32(0)
            for k in range(NHALF):
                q = q + jnp.where(u == k, jnp.where(end, (end_order + last)[k], mid_order[k]), 0)
            both.append(q)
        return both

    def wait_load(q):
        here = pl.ds(pl.multiple_of(q * half, half), half)
        wait_bytes(wl.at[:, here], load_a.at[q])

    def far_product(here, cs):
        p0 = jnp.dot(wl[0, here, :], wr[0, :, cs], preferred_element_type=jnp.float32)
        p1 = jnp.dot(wl[1, here, :], wr[1, :, cs], preferred_element_type=jnp.float32)
        v = acc[here, cs] + (p0.astype(jnp.bfloat16).astype(jnp.float32) + p1.astype(jnp.bfloat16).astype(jnp.float32))
        acc[here, cs] = v
        return v

    def squares(v):
        sq = v * v
        part = sq[:, :128]
        for k in range(1, sq.shape[1] // 128):
            part = part + sq[:, k * 128:(k + 1) * 128]
        return part

    def keep_squares(q0, q1, part):
        total = jnp.sum(part.T, axis=0, keepdims=True)
        low = lax.broadcasted_iota(jnp.int32, total.shape, 1) < total.shape[1] // 2
        ss_loc[q0] = jnp.where(low, total, ss_loc[q0])
        ss_loc[q1] = jnp.where(low, ss_loc[q1], total)

    def remote_unit(u, _):
        q0, q1 = unit_of(u)
        quarter = half // 2
        low = pl.ds(pl.multiple_of(q0 * half, quarter), quarter)
        high = pl.ds(pl.multiple_of(q1 * half + quarter, quarter), quarter)

        @pl.when(mid | (u < NHALF - 4))
        def _():
            wait_load(q0)

        def tile(n, part):
            cs = pl.ds(pl.multiple_of(n * tn, tn), tn)
            far = [jnp.dot(jnp.concatenate([wl[b, low, :], wl[b, high, :]], axis=0), wr[b, :, cs],
                           preferred_element_type=jnp.float32).astype(jnp.bfloat16).astype(jnp.float32) for b in range(2)]
            far = far[0] + far[1]
            v0 = acc[low, cs] + far[:quarter]
            v1 = acc[high, cs] + far[quarter:]
            acc[low, cs] = v0
            acc[high, cs] = v1
            return part + squares(jnp.concatenate([v0, v1], axis=0))

        keep_squares(q0, q1, lax.fori_loop(0, ntile, tile, jnp.zeros((half, 128), jnp.float32)))
        return None

    def column_unit(k):
        return jnp.where(k < 2, side, 1 - side) * gs + 2 + lax.rem(k, 2)

    def column_step(n):
        w_from_partner(n)

        @pl.when(n == 0)
        def _():
            for k in range(4):
                for e in range(2):
                    wait_load(column_unit(jnp.int32(k)) * 2 + e)

        cs = pl.ds(pl.multiple_of(n * wch, wch), wch)

        def rows_of(k, _):
            here = pl.ds(pl.multiple_of(column_unit(k) * unit, unit), unit)
            far_product(here, cs)
            return None

        lax.fori_loop(0, 4, rows_of, None)

        @pl.when(n == NWC - 1)
        def _():
            def sums(k, _):
                q = column_unit(k // 2) * 2 + lax.rem(k, 2)
                here = pl.ds(pl.multiple_of(q * half, half), half)

                def tile(m, part):
                    return part + squares(acc[here, pl.ds(pl.multiple_of(m * tn, tn), tn)])

                keep_squares(q, q, lax.fori_loop(0, ntile, tile, jnp.zeros((half, 128), jnp.float32)))
                return None

            lax.fori_loop(0, 8, sums, None)

    def slot_body(i, _):
        @pl.when(i == LOADS)
        def _():
            early_loads()

        @pl.when(end & (i == LOADS))
        def _():
            pl.semaphore_signal(credit_z, inc=1, device_id=(x, z_in, t), device_id_type=MESH)
            for cc in range(2):
                pl.semaphore_signal(credit_y, inc=1, device_id=(x, z, (1 - y) * 2 + cc), device_id_type=MESH)

        comm(i)

        @pl.when(i == LOCAL0 - 1)
        def _():
            own_w.wait()
            wait_bytes(wl.at[1], recv_dw)
            wait_bytes(ap, recv_da)
            for cp in local_loads(0):
                cp.start()

        @pl.when((i >= LOCAL0) & (i < LOCAL0 + NUNIT))
        def _():
            local_unit(i - LOCAL0)

        @pl.when(end & (i == WREADY))
        def _():
            lax.fori_loop(0, NWC, lambda n, _: (w_from_partner(n), None)[1], None)

        jc = i - COLS0

        @pl.when(mid & (jc >= 0) & (jc < WS) & (lax.rem(jc, 2) == 0))
        def _():
            column_step(jc // 2)

        lo = jnp.where(end, step_count(i - 1, END_UNITS), step_count(i - 1, MID_UNITS))
        hi = jnp.where(end, step_count(i, END_UNITS), step_count(i, MID_UNITS))
        lax.fori_loop(lo, hi, remote_unit, None)
        return None

    lax.fori_loop(0, NSLOT, slot_body, None)

    for k in range(1, 4):
        remote(ss_loc, ss_all.at[z], send_ss.at[k - 1], recv_ss.at[z], (x, lax.rem(z + k, 4), t)).start()
    wait_bytes(wl.at[1], send_dw)
    wait_bytes(ap, send_da)
    wait_bytes(wr.at[0], send_wd)
    wait_bytes(wr.at[0, pl.ds(0, kb // 2)], send_wx)
    wait_bytes(wr.at[0, pl.ds(0, kb // 2)], send_yw)

    @pl.when(end)
    def _():
        wait_bytes(ax.at[pl.ds(0, FAR + NEAR)], send_ya)
        wait_bytes(ax.at[0, :, pl.ds(0, NDIRECT * sub)], send_first)
        wait_bytes(ax.at[pl.ds(0, FAR)], send_zi)

    @pl.when(mid)
    def _():
        wait_bytes(ax.at[pl.ds(0, FAR - 1)], send_ya)
        wait_bytes(ax.at[pl.ds(0, 2 * FAR)], send_zi)
        wait_bytes(ax.at[pl.ds(0, 2 * FAR + NEAR - 1)], send_zo)
        wait_bytes(ax.at[0], send_first)
        wait_bytes(ax.at[0, :, pl.ds(0, (NSUB - NDIRECT) * sub)], send_pieces)

    for k in range(1, 4):
        src = lax.rem(z + k, 4)
        remote(ss_loc, ss_all.at[src], send_ss.at[k - 1], recv_ss.at[src], (x, src, t)).wait_recv()
        remote(ss_loc, ss_all.at[src], send_ss.at[k - 1], recv_ss.at[src], (x, src, t)).wait_send()
    ss_all[z] = ss_loc[...]

def finish_kernel(h, ss, g, h_out, n_out, hbuf, nbuf, sem):
    rows, cols = h.shape
    step_rows = rows // NHALF

    def copies(q):
        slot = lax.rem(q, NBUF)
        here = pl.ds(pl.multiple_of(q * step_rows, step_rows), step_rows)
        return (pltpu.make_async_copy(hbuf.at[slot], h_out.at[here], sem.at[slot, 0]),
                pltpu.make_async_copy(nbuf.at[slot], n_out.at[here], sem.at[slot, 1]))

    def step(q, _):
        slot = lax.rem(q, NBUF)

        @pl.when(q >= NBUF)
        def _():
            for cp in copies(q - NBUF):
                cp.wait()

        total = ss[0, q] + ss[1, q] + ss[2, q] + ss[3, q]
        inv = lax.rsqrt(total / (cols * 4) + EPS_NORM)
        col = jnp.broadcast_to(inv, (128, 128)).T
        rs = pl.ds(pl.multiple_of(q * 128, 128), 128)
        for m in range(cols // 128):
            cs = slice(m * 128, (m + 1) * 128)
            v = h[rs, cs]
            hbuf[slot, :, cs] = v.astype(jnp.bfloat16)
            nbuf[slot, :, cs] = (v * col * g[:, cs]).astype(jnp.bfloat16)
        for cp in copies(q):
            cp.start()
        return None

    lax.fori_loop(0, NHALF, step, None)

    def drain(q, _):
        for cp in copies(q):
            cp.wait()
        return None

    lax.fori_loop(NHALF - NBUF, NHALF, drain, None)


def solution(mesh):
    def local_step(attn_blk, w_blk, res_blk, gain_blk):
        kb = attn_blk.shape[1]
        rows, cols = res_blk.shape
        unit = rows // NUNIT
        any_spec = pl.BlockSpec(memory_space=pl.ANY)
        vmem_spec = pl.BlockSpec(memory_space=pltpu.VMEM)
        bf16, f32 = jnp.bfloat16, jnp.float32
        dma = pltpu.SemaphoreType.DMA
        h, ss, _, _ = pl.pallas_call(
            kernel,
            out_shape=(
                pltpu.VMEM((rows, cols), f32),
                pltpu.VMEM((4, NHALF, 1, 128), f32),
                jax.ShapeDtypeStruct((NCH, 2, rows // NCH, kb), bf16),
                jax.ShapeDtypeStruct((rows, kb), bf16),
            ),
            in_specs=[any_spec, any_spec, any_spec],
            out_specs=(vmem_spec, vmem_spec, any_spec, any_spec),
            scratch_shapes=[
                pltpu.VMEM((2, kb, cols), bf16),
                pltpu.VMEM((2, kb, cols), bf16),
                pltpu.VMEM((2, 2, unit, kb), bf16),
                pltpu.VMEM((2, unit, cols), bf16),
                pltpu.VMEM((NHALF, 1, 128), f32),
                dma((NCH,)), dma, dma, dma, dma,
                dma((NWC,)), dma((NWC,)), dma((NWC,)), dma, dma,
                dma, dma, dma, dma,
                dma((2, 3)), dma, dma((NHALF,)), dma((NSUB,)), dma, dma,
                pltpu.SemaphoreType.REGULAR, pltpu.SemaphoreType.REGULAR,
                dma((3,)), dma((4,)),
            ],
            compiler_params=pltpu.CompilerParams(
                collective_id=0, has_side_effects=True, vmem_limit_bytes=44 * 1024 * 1024),
            name="gather_project",
        )(attn_blk, w_blk, res_blk)
        return pl.pallas_call(
            finish_kernel,
            out_shape=(jax.ShapeDtypeStruct((rows, cols), bf16),) * 2,
            in_specs=[vmem_spec, vmem_spec, vmem_spec],
            out_specs=(any_spec, any_spec),
            scratch_shapes=[pltpu.VMEM((NBUF, rows // NHALF, cols), bf16)] * 2 + [dma((NBUF, 2))],
            compiler_params=pltpu.CompilerParams(vmem_limit_bytes=8 * 1024 * 1024),
            name="norm_store",
        )(h, ss, gain_blk.reshape(1, cols))

    row_spec = P(("dp", "tp"), "tp2")
    return jax.shard_map(local_step, mesh=mesh, in_specs=(P("dp", "tp"), P("tp", "tp2"), row_spec, P("tp2")), out_specs=(row_spec, row_spec), check_vma=False)
```

```python
import functools

import jax
import jax.numpy as jnp
from jax import lax
from jax.experimental import pallas as pl
from jax.experimental.pallas import tpu as pltpu
from jax.sharding import PartitionSpec as P

EPS_NORM = 1e-6
MESH = pl.DeviceIdType.MESH
NCH = 64
FAR = NCH // 4
NEAR = NCH // 8
NWC = 8
WS = 2 * NWC
NUNIT = 8
NHALF = 2 * NUNIT
GRP = NCH // NUNIT
HGRP = NCH // NHALF
LATE = FAR // 2
NBUF = 4
NDIRECT = 2
LAG = 6
NSUB = 4
AHEAD = 12
NSLOT = 2 * FAR + NEAR + 1
LOCAL0 = 6
LOADS = 16
WREADY = WS + 2
COLS0 = FAR + 4


def step_count(i, slots):
    n = jnp.int32(0)
    for s in slots:
        n = n + jnp.where(i >= s, 1, 0)
    return n


END_UNITS = (20, 20, 21, 22, 23, 24, 26, 28, 30, 31, 32, 33, 36, 37, 39, 40)
MID_UNITS = (35, 35, 36, 36, 37, 37, 38, 38)


def kernel(a, w, r, acc, ss_all, ax, ap, wl, wr, abuf, rbuf, ss_loc,
           recv_a, send_ya, send_yw, send_zi, send_zo, recv_wy, recv_wx, recv_wd, send_wx, send_wd,
           recv_da, recv_dw, send_da, send_dw, load_sem, load_w, load_a, recv_sub, send_first, credit_z, credit_y, send_ss, recv_ss):
    x = lax.axis_index("dp")
    z = lax.axis_index("tp2")
    t = lax.axis_index("tp")
    y = t // 2
    c = t % 2
    rows, cols = acc.shape
    kb = w.shape[0]
    ch = rows // NCH
    wch = cols // NWC
    unit = ch * GRP
    half = ch * HGRP
    sub = ch // NSUB
    side = z // 2
    end = (z == 0) | (z == 3)
    mid = (z == 1) | (z == 2)
    base = side * (NCH // 2)
    other = (1 - side) * (NCH // 2)
    z_in = jnp.where(side == 0, z + 1, z - 1)
    z_out = jnp.where(side == 0, z - 1, z + 1)

    partner = (x, z, y * 2 + 1 - c)
    x_peer = (1 - x, z, t)
    y_same = (x, z, (1 - y) * 2 + c)
    y_cross = (x, z, (1 - y) * 2 + 1 - c)

    def remote(src, dst, send, recv, dev):
        return pltpu.make_async_remote_copy(
            src_ref=src, dst_ref=dst, send_sem=send, recv_sem=recv, device_id=dev, device_id_type=MESH)

    def wait_bytes(ref, sem):
        pltpu.make_async_copy(ref, ref, sem).wait()

    barrier = pltpu.get_barrier_semaphore()
    for dev in (partner, x_peer, y_same, y_cross):
        pl.semaphore_signal(barrier, inc=1, device_id=dev, device_id_type=MESH)
    for k in range(1, 4):
        pl.semaphore_signal(barrier, inc=1, device_id=(x, lax.rem(z + k, 4), t), device_id_type=MESH)
    z_mate = jnp.where(end, z_in, z_out)
    for cc in range(2):
        pl.semaphore_signal(barrier, inc=1, device_id=(x, z_mate, (1 - y) * 2 + cc), device_id_type=MESH)
    pl.semaphore_wait(barrier, 9)

    def mp(start, j):
        return start + FAR + lax.rem(j + NEAR, FAR)

    def chunk_rows(q):
        return pl.ds(pl.multiple_of(q * ch, ch), ch)

    def send_y_a(q, dst=None):
        dst = ax.at[q, c] if dst is None else dst
        for cc in range(2):
            row = ((1 - y) * 2 + cc) * rows + q * ch
            remote(a.at[pl.ds(pl.multiple_of(row, ch), ch)], dst, send_ya, recv_a.at[q],
                   (x, z, (1 - y) * 2 + cc)).start()

    def send_y_first(q):
        for k in range(NDIRECT):
            for cc in range(2):
                row = ((1 - y) * 2 + cc) * rows + q * ch + k * sub
                remote(a.at[pl.ds(pl.multiple_of(row, sub), sub)], ax.at[q, c, pl.ds(k * sub, sub)], send_first,
                       recv_a.at[q], (x, z_out, (1 - y) * 2 + cc)).start()
        for k in range(NSUB):
            for cc in range(2):
                row = ((1 - y) * 2 + cc) * rows + q * ch + k * sub
                remote(a.at[pl.ds(pl.multiple_of(row, sub), sub)], ax.at[q, c, pl.ds(k * sub, sub)], send_ya,
                       recv_sub.at[k], (x, z, (1 - y) * 2 + cc)).start()

    def w_part(part, n):
        return (pl.ds(pl.multiple_of(part * (kb // 2), kb // 2), kb // 2), pl.ds(pl.multiple_of(n * wch, wch), wch))

    def send_y_w(n):
        rs, cs = w_part(x, n)
        remote(w.at[rs, cs], wr.at[c, rs, cs], send_yw, recv_wy.at[n], y_same).start()

    def y_sends(i):
        iw = jnp.where(end, i, i - FAR)
        ia = jnp.where(end, i - WS, i)

        @pl.when((iw >= 0) & (iw < WS) & (lax.rem(iw, 2) == 0))
        def _():
            send_y_w(iw // 2)

        @pl.when(end & (ia >= 0) & (ia < FAR))
        def _():
            send_y_a(base + ia)

        @pl.when(end & (ia == FAR))
        def _():
            pl.semaphore_wait(credit_y, 2)

        @pl.when(end & (ia >= FAR) & (ia < FAR + NEAR))
        def _():
            send_y_a(base + ia, wl.at[c, chunk_rows(base + ia)])

        @pl.when(mid & (ia == 0))
        def _():
            send_y_first(mp(base, 0))

        @pl.when(mid & (ia >= 1) & (ia < FAR))
        def _():
            send_y_a(mp(base, ia))

    lax.fori_loop(0, AHEAD, lambda i, _: (y_sends(i), None)[1], None)

    kpart = kb // NUNIT

    def partner_sends(i):
        @pl.when(i < NUNIT // 2)
        def _():
            for k in range(2):
                rs = pl.ds(pl.multiple_of((2 * i + k) * kpart, kpart), kpart)
                remote(w.at[rs], wl.at[1, rs], send_dw, recv_dw, partner).start()

        u = i - NUNIT // 2

        @pl.when((u >= 0) & (u < NUNIT))
        def _():
            src = pl.ds(pl.multiple_of((y * 2 + 1 - c) * rows + u * unit, unit), unit)
            remote(a.at[src], ap.at[pl.ds(pl.multiple_of(u * unit, unit), unit)], send_da, recv_da.at[u], partner).start()

    own_w = pltpu.make_async_copy(w, wl.at[0], load_w)
    own_w.start()

    def load(q):
        here = pl.ds(pl.multiple_of(q * ch, ch), ch)
        for b in range(2):
            pltpu.make_async_copy(ax.at[q, b], wl.at[b, here], load_a.at[q // HGRP]).start()

    def arrive(q, i):
        wait_bytes(ax.at[q], recv_a.at[q])

        @pl.when(i >= LOADS)
        def _():
            load(q)

    def arrive_late(q):
        wait_bytes(wl.at[:, chunk_rows(q)], recv_a.at[q])

    def pass_out_late(q):
        remote(ax.at[q], wl.at[:, chunk_rows(q)], send_zo, recv_a.at[q], (x, z_out, t)).start()

    def pass_in(q):
        remote(ax.at[q], ax.at[q], send_zi, recv_a.at[q], (x, z_in, t)).start()

    def pass_out(q):
        remote(ax.at[q], ax.at[q], send_zo, recv_a.at[q], (x, z_out, t)).start()

    def w_from_y(n):
        rs, cs = w_part(x, n)
        part = wr.at[c, rs, cs]
        wait_bytes(part, recv_wy.at[n])
        remote(part, part, send_wx, recv_wx.at[n], x_peer).start()
        remote(part, part, send_wd, recv_wd.at[n], partner).start()

    def w_from_x(n):
        rs, cs = w_part(1 - x, n)
        part = wr.at[c, rs, cs]
        wait_bytes(part, recv_wx.at[n])
        remote(part, part, send_wd, recv_wd.at[n], partner).start()

    def w_from_partner(n):
        cs = pl.ds(pl.multiple_of(n * wch, wch), wch)
        wait_bytes(wr.at[1 - c, :, cs], recv_wd.at[n])

    def z_chunk(j):
        own = (j == 0) | (lax.rem(j, 2) == 1)
        first = jnp.where(own, mp(base, (j + 1) // 2), mp(other, j // 2 - 1))
        return jnp.where(j < 2 * NEAR - 1, first, jnp.where(j < NEAR + FAR, mp(other, j - NEAR), other + j - NEAR - FAR))

    def comm(i):
        y_sends(i + AHEAD)
        iw = jnp.where(end, i, i - FAR)
        odd = lax.rem(i, 2) == 1

        @pl.when(odd & (iw >= 1) & (iw < WS))
        def _():
            w_from_y(iw // 2)

        @pl.when(odd & (iw >= 3) & (iw < WS + 2))
        def _():
            w_from_x((iw - 3) // 2)

        @pl.when(end)
        def _():
            @pl.when((i >= WS) & (i < WS + FAR))
            def _():
                q = base + i - WS
                arrive(q, i)
                pass_in(q)

            @pl.when((i >= WS + FAR) & (i < WS + FAR + NEAR))
            def _():
                arrive_late(base + i - WS)

            nlate = 1 + 2 * FAR + NEAR - LATE

            @pl.when((i >= 1 + LAG) & (i < nlate - 1))
            def _():
                arrive(z_chunk(i - 1 - LAG), i)

            @pl.when(i == nlate - 1)
            def _():
                lax.fori_loop(nlate - 2 - LAG, nlate - 1, lambda j, _: (arrive(z_chunk(j), i), None)[1], None)

            @pl.when((i >= nlate) & (i < nlate + LATE))
            def _():
                arrive_late(z_chunk(i - 1))

        @pl.when(mid)
        def _():
            @pl.when(i == 0)
            def _():
                q = mp(base, 0)
                for k in range(NSUB):
                    piece = ax.at[q, :, pl.ds(k * sub, sub)]
                    wait_bytes(piece, recv_sub.at[k])
                    if k >= NDIRECT:
                        remote(piece, piece, send_first, recv_a.at[q], (x, z_out, t)).start()
                pass_in(q)

            @pl.when((i >= 1) & (i < FAR))
            def _():
                q = mp(base, i)
                arrive(q, i)

                @pl.when(i < NEAR)
                def _():
                    pass_out(q)

                pass_in(q)

            @pl.when((i >= 1) & (i < 1 + FAR))
            def _():
                q = mp(other, i - 1)
                arrive(q, i)
                pass_out(q)

            @pl.when((i >= WS + 1) & (i < WS + 1 + FAR))
            def _():
                q = base + i - WS - 1
                arrive(q, i)
                pass_in(q)

            @pl.when((i >= WS + 2) & (i < WS + 2 + FAR))
            def _():
                q = other + i - WS - 2
                arrive(q, i)

                @pl.when(i < WS + 2 + FAR - LATE)
                def _():
                    pass_out(q)

                @pl.when(i == WS + 2 + FAR - LATE)
                def _():
                    pl.semaphore_wait(credit_z, 1)

                @pl.when(i >= WS + 2 + FAR - LATE)
                def _():
                    pass_out_late(q)

    def early_loads():
        def from_z(j, _):
            load(jnp.where(end, z_chunk(j), mp(other, j)))
            return None

        lax.fori_loop(0, jnp.where(end, LOADS - 1 - LAG, LOADS - 1), from_z, None)

        def from_y(j, _):
            load(mp(base, j))
            return None

        lax.fori_loop(0, jnp.where(end, 0, LOADS), from_y, None)

    tn = min(512, cols)
    ntile = cols // tn

    def local_loads(u):
        slot = lax.rem(u, 2)
        here = pl.ds(pl.multiple_of(u * unit, unit), unit)
        mine = pl.ds(pl.multiple_of(t * rows + u * unit, unit), unit)
        return (pltpu.make_async_copy(a.at[mine], abuf.at[slot, 0], load_sem.at[slot, 0]),
                pltpu.make_async_copy(ap.at[here], abuf.at[slot, 1], load_sem.at[slot, 1]),
                pltpu.make_async_copy(r.at[here], rbuf.at[slot], load_sem.at[slot, 2]))

    def local_unit(u):
        slot = lax.rem(u, 2)
        here = pl.ds(pl.multiple_of(u * unit, unit), unit)
        for cp in local_loads(u):
            cp.wait()

        @pl.when(u + 1 < NUNIT)
        def _():
            wait_bytes(ap.at[pl.ds(pl.multiple_of((u + 1) * unit, unit), unit)], recv_da.at[u + 1])
            for cp in local_loads(u + 1):
                cp.start()

        def tile(n, _):
            cs = pl.ds(pl.multiple_of(n * tn, tn), tn)
            p0 = jnp.dot(abuf[slot, 0], wl[0, :, cs], preferred_element_type=jnp.float32)
            p1 = jnp.dot(abuf[slot, 1], wl[1, :, cs], preferred_element_type=jnp.float32)
            acc[here, cs] = (rbuf[slot, :, cs].astype(jnp.float32) + p0.astype(jnp.bfloat16).astype(jnp.float32)
                             + p1.astype(jnp.bfloat16).astype(jnp.float32))
            return None

        lax.fori_loop(0, ntile, tile, None)

    gs = NUNIT // 2

    def unit_of(u):
        b = side * NUNIT
        o = (1 - side) * NUNIT
        end_order = (b + 6, b + 7, o + 6, o + 7, b, b + 1, o + 4, b + 2, o + 5, b + 3, o, o + 1, b + 4, o + 2, b + 5, o + 3)
        mid_order = (b, b + 1, o, o + 1, b + 2, b + 3, o + 2, o + 3) + (0,) * NUNIT
        q = jnp.int32(0)
        for k in range(NHALF):
            q = q + jnp.where(u == k, jnp.where(end, end_order[k], mid_order[k]), 0)
        return q

    def wait_load(q):
        here = pl.ds(pl.multiple_of(q * half, half), half)
        wait_bytes(wl.at[:, here], load_a.at[q])

    def far_product(here, cs):
        p0 = jnp.dot(wl[0, here, :], wr[0, :, cs], preferred_element_type=jnp.float32)
        p1 = jnp.dot(wl[1, here, :], wr[1, :, cs], preferred_element_type=jnp.float32)
        v = acc[here, cs] + (p0.astype(jnp.bfloat16).astype(jnp.float32) + p1.astype(jnp.bfloat16).astype(jnp.float32))
        acc[here, cs] = v
        return v

    def squares(v):
        sq = v * v
        part = sq[:, :128]
        for k in range(1, sq.shape[1] // 128):
            part = part + sq[:, k * 128:(k + 1) * 128]
        return part

    def keep_squares(q, part):
        ss_loc[q] = jnp.sum(part.T, axis=0, keepdims=True)

    def remote_unit(u, _):
        q = unit_of(u)
        here = pl.ds(pl.multiple_of(q * half, half), half)

        @pl.when(mid | (u < NHALF - 4))
        def _():
            wait_load(q)

        def tile(n, part):
            cs = pl.ds(pl.multiple_of(n * tn, tn), tn)
            return part + squares(far_product(here, cs))

        keep_squares(q, lax.fori_loop(0, ntile, tile, jnp.zeros((half, 128), jnp.float32)))
        return None

    def column_unit(k):
        return jnp.where(k < 2, side, 1 - side) * gs + 2 + lax.rem(k, 2)

    def column_step(n):
        w_from_partner(n)

        @pl.when(n == 0)
        def _():
            for k in range(4):
                for e in range(2):
                    wait_load(column_unit(jnp.int32(k)) * 2 + e)

        cs = pl.ds(pl.multiple_of(n * wch, wch), wch)

        def rows_of(k, _):
            here = pl.ds(pl.multiple_of(column_unit(k) * unit, unit), unit)
            far_product(here, cs)
            return None

        lax.fori_loop(0, 4, rows_of, None)

        @pl.when(n == NWC - 1)
        def _():
            def sums(k, _):
                q = column_unit(k // 2) * 2 + lax.rem(k, 2)
                here = pl.ds(pl.multiple_of(q * half, half), half)

                def tile(m, part):
                    return part + squares(acc[here, pl.ds(pl.multiple_of(m * tn, tn), tn)])

                keep_squares(q, lax.fori_loop(0, ntile, tile, jnp.zeros((half, 128), jnp.float32)))
                return None

            lax.fori_loop(0, 8, sums, None)

    def slot_body(i, _):
        partner_sends(i)

        @pl.when(i == LOADS)
        def _():
            early_loads()

        @pl.when(end & (i == LOADS))
        def _():
            pl.semaphore_signal(credit_z, inc=1, device_id=(x, z_in, t), device_id_type=MESH)
            for cc in range(2):
                pl.semaphore_signal(credit_y, inc=1, device_id=(x, z, (1 - y) * 2 + cc), device_id_type=MESH)

        comm(i)

        @pl.when(i == LOCAL0 - 1)
        def _():
            own_w.wait()
            wait_bytes(wl.at[1], recv_dw)
            wait_bytes(ap.at[pl.ds(0, unit)], recv_da.at[0])
            for cp in local_loads(0):
                cp.start()

        @pl.when((i >= LOCAL0) & (i < LOCAL0 + NUNIT))
        def _():
            local_unit(i - LOCAL0)

        @pl.when(end & (i == WREADY))
        def _():
            lax.fori_loop(0, NWC, lambda n, _: (w_from_partner(n), None)[1], None)

        jc = i - COLS0

        @pl.when(mid & (jc >= 0) & (jc < WS) & (lax.rem(jc, 2) == 0))
        def _():
            column_step(jc // 2)

        lo = jnp.where(end, step_count(i - 1, END_UNITS), step_count(i - 1, MID_UNITS))
        hi = jnp.where(end, step_count(i, END_UNITS), step_count(i, MID_UNITS))
        lax.fori_loop(lo, hi, remote_unit, None)
        return None

    lax.fori_loop(0, NSLOT, slot_body, None)

    for k in range(1, 4):
        remote(ss_loc, ss_all.at[z], send_ss.at[k - 1], recv_ss.at[z], (x, lax.rem(z + k, 4), t)).start()
    wait_bytes(wl.at[1], send_dw)
    wait_bytes(ap, send_da)
    wait_bytes(wr.at[0], send_wd)
    wait_bytes(wr.at[0, pl.ds(0, kb // 2)], send_wx)
    wait_bytes(wr.at[0, pl.ds(0, kb // 2)], send_yw)

    @pl.when(end)
    def _():
        wait_bytes(ax.at[pl.ds(0, FAR + NEAR)], send_ya)
        wait_bytes(ax.at[pl.ds(0, FAR)], send_zi)

    @pl.when(mid)
    def _():
        wait_bytes(ax.at[pl.ds(0, FAR)], send_ya)
        wait_bytes(ax.at[pl.ds(0, 2 * FAR)], send_zi)
        wait_bytes(ax.at[pl.ds(0, 2 * FAR + NEAR - 1)], send_zo)
        wait_bytes(ax.at[0], send_first)

    for k in range(1, 4):
        src = lax.rem(z + k, 4)
        remote(ss_loc, ss_all.at[src], send_ss.at[k - 1], recv_ss.at[src], (x, src, t)).wait_recv()
        remote(ss_loc, ss_all.at[src], send_ss.at[k - 1], recv_ss.at[src], (x, src, t)).wait_send()
    ss_all[z] = ss_loc[...]

def finish_kernel(h, ss, g, h_out, n_out, hbuf, nbuf, sem):
    rows, cols = h.shape
    step_rows = rows // NHALF

    def copies(q):
        slot = lax.rem(q, NBUF)
        here = pl.ds(pl.multiple_of(q * step_rows, step_rows), step_rows)
        return (pltpu.make_async_copy(hbuf.at[slot], h_out.at[here], sem.at[slot, 0]),
                pltpu.make_async_copy(nbuf.at[slot], n_out.at[here], sem.at[slot, 1]))

    def step(q, _):
        slot = lax.rem(q, NBUF)

        @pl.when(q >= NBUF)
        def _():
            for cp in copies(q - NBUF):
                cp.wait()

        total = ss[0, q] + ss[1, q] + ss[2, q] + ss[3, q]
        inv = lax.rsqrt(total / (cols * 4) + EPS_NORM)
        col = jnp.broadcast_to(inv, (128, 128)).T
        rs = pl.ds(pl.multiple_of(q * 128, 128), 128)
        for m in range(cols // 128):
            cs = slice(m * 128, (m + 1) * 128)
            v = h[rs, cs]
            hbuf[slot, :, cs] = v.astype(jnp.bfloat16)
            nbuf[slot, :, cs] = (v * col * g[:, cs]).astype(jnp.bfloat16)
        for cp in copies(q):
            cp.start()
        return None

    lax.fori_loop(0, NHALF, step, None)

    def drain(q, _):
        for cp in copies(q):
            cp.wait()
        return None

    lax.fori_loop(NHALF - NBUF, NHALF, drain, None)


def solution(mesh):
    def local_step(attn_blk, w_blk, res_blk, gain_blk):
        kb = attn_blk.shape[1]
        rows, cols = res_blk.shape
        unit = rows // NUNIT
        any_spec = pl.BlockSpec(memory_space=pl.ANY)
        vmem_spec = pl.BlockSpec(memory_space=pltpu.VMEM)
        bf16, f32 = jnp.bfloat16, jnp.float32
        dma = pltpu.SemaphoreType.DMA
        h, ss, _, _ = pl.pallas_call(
            kernel,
            out_shape=(
                pltpu.VMEM((rows, cols), f32),
                pltpu.VMEM((4, NHALF, 1, 128), f32),
                jax.ShapeDtypeStruct((NCH, 2, rows // NCH, kb), bf16),
                jax.ShapeDtypeStruct((rows, kb), bf16),
            ),
            in_specs=[any_spec, any_spec, any_spec],
            out_specs=(vmem_spec, vmem_spec, any_spec, any_spec),
            scratch_shapes=[
                pltpu.VMEM((2, kb, cols), bf16),
                pltpu.VMEM((2, kb, cols), bf16),
                pltpu.VMEM((2, 2, unit, kb), bf16),
                pltpu.VMEM((2, unit, cols), bf16),
                pltpu.VMEM((NHALF, 1, 128), f32),
                dma((NCH,)), dma, dma, dma, dma,
                dma((NWC,)), dma((NWC,)), dma((NWC,)), dma, dma,
                dma((NUNIT,)), dma, dma, dma,
                dma((2, 3)), dma, dma((NHALF,)), dma((NSUB,)), dma,
                pltpu.SemaphoreType.REGULAR, pltpu.SemaphoreType.REGULAR,
                dma((3,)), dma((4,)),
            ],
            compiler_params=pltpu.CompilerParams(
                collective_id=0, has_side_effects=True, vmem_limit_bytes=44 * 1024 * 1024),
            name="gather_project",
        )(attn_blk, w_blk, res_blk)
        return pl.pallas_call(
            finish_kernel,
            out_shape=(jax.ShapeDtypeStruct((rows, cols), bf16),) * 2,
            in_specs=[vmem_spec, vmem_spec, vmem_spec],
            out_specs=(any_spec, any_spec),
            scratch_shapes=[pltpu.VMEM((NBUF, rows // NHALF, cols), bf16)] * 2 + [dma((NBUF, 2))],
            compiler_params=pltpu.CompilerParams(vmem_limit_bytes=8 * 1024 * 1024),
            name="norm_store",
        )(h, ss, gain_blk.reshape(1, cols))

    row_spec = P(("dp", "tp"), "tp2")
    return jax.shard_map(local_step, mesh=mesh, in_specs=(P("dp", "tp"), P("tp", "tp2"), row_spec, P("tp2")), out_specs=(row_spec, row_spec), check_vma=False)
```

```python
import functools

import jax
import jax.numpy as jnp
from jax import lax
from jax.experimental import pallas as pl
from jax.experimental.pallas import tpu as pltpu
from jax.sharding import PartitionSpec as P

EPS_NORM = 1e-6
MESH = pl.DeviceIdType.MESH
NCH = 64
FAR = NCH // 4
NEAR = NCH // 8
NWC = 8
WS = 2 * NWC
NUNIT = 8
NHALF = 2 * NUNIT
GRP = NCH // NUNIT
HGRP = NCH // NHALF
LATE = FAR // 2
NBUF = 4
LAG = 6
NSUB = 4
AHEAD = 12
NSLOT = 2 * FAR + NEAR + 1
LOCAL0 = 6
LOADS = 16
WREADY = WS + 2
COLS0 = FAR + 4


def step_count(i, slots):
    n = jnp.int32(0)
    for s in slots:
        n = n + jnp.where(i >= s, 1, 0)
    return n


END_UNITS = (20, 20, 21, 22, 23, 24, 26, 28, 30, 31, 32, 33, 36, 37, 39, 40)
MID_UNITS = (35, 35, 36, 36, 37, 37, 38, 38)


def kernel(a, w, r, acc, ss_all, ax, ap, wl, wr, abuf, rbuf, ss_loc,
           recv_a, send_ya, send_yw, send_zi, send_zo, recv_wy, recv_wx, recv_wd, send_wx, send_wd,
           recv_da, recv_dw, send_da, send_dw, load_sem, load_w, load_a, recv_sub, send_first, credit_z, credit_y, send_ss, recv_ss):
    x = lax.axis_index("dp")
    z = lax.axis_index("tp2")
    t = lax.axis_index("tp")
    y = t // 2
    c = t % 2
    rows, cols = acc.shape
    kb = w.shape[0]
    ch = rows // NCH
    wch = cols // NWC
    unit = ch * GRP
    half = ch * HGRP
    sub = ch // NSUB
    side = z // 2
    end = (z == 0) | (z == 3)
    mid = (z == 1) | (z == 2)
    base = side * (NCH // 2)
    other = (1 - side) * (NCH // 2)
    z_in = jnp.where(side == 0, z + 1, z - 1)
    z_out = jnp.where(side == 0, z - 1, z + 1)

    partner = (x, z, y * 2 + 1 - c)
    x_peer = (1 - x, z, t)
    y_same = (x, z, (1 - y) * 2 + c)
    y_cross = (x, z, (1 - y) * 2 + 1 - c)

    def remote(src, dst, send, recv, dev):
        return pltpu.make_async_remote_copy(
            src_ref=src, dst_ref=dst, send_sem=send, recv_sem=recv, device_id=dev, device_id_type=MESH)

    def wait_bytes(ref, sem):
        pltpu.make_async_copy(ref, ref, sem).wait()

    barrier = pltpu.get_barrier_semaphore()
    for dev in (partner, x_peer, y_same, y_cross):
        pl.semaphore_signal(barrier, inc=1, device_id=dev, device_id_type=MESH)
    for k in range(1, 4):
        pl.semaphore_signal(barrier, inc=1, device_id=(x, lax.rem(z + k, 4), t), device_id_type=MESH)
    pl.semaphore_wait(barrier, 7)

    def mp(start, j):
        return start + FAR + lax.rem(j + NEAR, FAR)

    def chunk_rows(q):
        return pl.ds(pl.multiple_of(q * ch, ch), ch)

    def send_y_a(q, dst=None):
        dst = ax.at[q, c] if dst is None else dst
        for cc in range(2):
            row = ((1 - y) * 2 + cc) * rows + q * ch
            remote(a.at[pl.ds(pl.multiple_of(row, ch), ch)], dst, send_ya, recv_a.at[q],
                   (x, z, (1 - y) * 2 + cc)).start()

    def send_y_first(q):
        for k in range(NSUB):
            for cc in range(2):
                row = ((1 - y) * 2 + cc) * rows + q * ch + k * sub
                remote(a.at[pl.ds(pl.multiple_of(row, sub), sub)], ax.at[q, c, pl.ds(k * sub, sub)], send_ya,
                       recv_sub.at[k], (x, z, (1 - y) * 2 + cc)).start()

    def w_part(part, n):
        return (pl.ds(pl.multiple_of(part * (kb // 2), kb // 2), kb // 2), pl.ds(pl.multiple_of(n * wch, wch), wch))

    def send_y_w(n):
        rs, cs = w_part(x, n)
        remote(w.at[rs, cs], wr.at[c, rs, cs], send_yw, recv_wy.at[n], y_same).start()

    def y_sends(i):
        iw = jnp.where(end, i, i - FAR)
        ia = jnp.where(end, i - WS, i)

        @pl.when((iw >= 0) & (iw < WS) & (lax.rem(iw, 2) == 0))
        def _():
            send_y_w(iw // 2)

        @pl.when(end & (ia >= 0) & (ia < FAR))
        def _():
            send_y_a(base + ia)

        @pl.when(end & (ia == FAR))
        def _():
            pl.semaphore_wait(credit_y, 2)

        @pl.when(end & (ia >= FAR) & (ia < FAR + NEAR))
        def _():
            send_y_a(base + ia, wl.at[c, chunk_rows(base + ia)])

        @pl.when(mid & (ia == 0))
        def _():
            send_y_first(mp(base, 0))

        @pl.when(mid & (ia >= 1) & (ia < FAR))
        def _():
            send_y_a(mp(base, ia))

    lax.fori_loop(0, AHEAD, lambda i, _: (y_sends(i), None)[1], None)

    kpart = kb // NUNIT

    def partner_sends(i):
        @pl.when(i < NUNIT // 2)
        def _():
            for k in range(2):
                rs = pl.ds(pl.multiple_of((2 * i + k) * kpart, kpart), kpart)
                remote(w.at[rs], wl.at[1, rs], send_dw, recv_dw, partner).start()

        u = i - NUNIT // 2

        @pl.when((u >= 0) & (u < NUNIT))
        def _():
            src = pl.ds(pl.multiple_of((y * 2 + 1 - c) * rows + u * unit, unit), unit)
            remote(a.at[src], ap.at[pl.ds(pl.multiple_of(u * unit, unit), unit)], send_da, recv_da.at[u], partner).start()

    own_w = pltpu.make_async_copy(w, wl.at[0], load_w)
    own_w.start()

    def load(q):
        here = pl.ds(pl.multiple_of(q * ch, ch), ch)
        for b in range(2):
            pltpu.make_async_copy(ax.at[q, b], wl.at[b, here], load_a.at[q // HGRP]).start()

    def arrive(q, i):
        wait_bytes(ax.at[q], recv_a.at[q])

        @pl.when(i >= LOADS)
        def _():
            load(q)

    def arrive_late(q):
        wait_bytes(wl.at[:, chunk_rows(q)], recv_a.at[q])

    def pass_out_late(q):
        remote(ax.at[q], wl.at[:, chunk_rows(q)], send_zo, recv_a.at[q], (x, z_out, t)).start()

    def pass_in(q):
        remote(ax.at[q], ax.at[q], send_zi, recv_a.at[q], (x, z_in, t)).start()

    def pass_out(q):
        remote(ax.at[q], ax.at[q], send_zo, recv_a.at[q], (x, z_out, t)).start()

    def w_from_y(n):
        rs, cs = w_part(x, n)
        part = wr.at[c, rs, cs]
        wait_bytes(part, recv_wy.at[n])
        remote(part, part, send_wx, recv_wx.at[n], x_peer).start()
        remote(part, part, send_wd, recv_wd.at[n], partner).start()

    def w_from_x(n):
        rs, cs = w_part(1 - x, n)
        part = wr.at[c, rs, cs]
        wait_bytes(part, recv_wx.at[n])
        remote(part, part, send_wd, recv_wd.at[n], partner).start()

    def w_from_partner(n):
        cs = pl.ds(pl.multiple_of(n * wch, wch), wch)
        wait_bytes(wr.at[1 - c, :, cs], recv_wd.at[n])

    def z_chunk(j):
        own = (j == 0) | (lax.rem(j, 2) == 1)
        first = jnp.where(own, mp(base, (j + 1) // 2), mp(other, j // 2 - 1))
        return jnp.where(j < 2 * NEAR - 1, first, jnp.where(j < NEAR + FAR, mp(other, j - NEAR), other + j - NEAR - FAR))

    def comm(i):
        y_sends(i + AHEAD)
        iw = jnp.where(end, i, i - FAR)
        odd = lax.rem(i, 2) == 1

        @pl.when(odd & (iw >= 1) & (iw < WS))
        def _():
            w_from_y(iw // 2)

        @pl.when(odd & (iw >= 3) & (iw < WS + 2))
        def _():
            w_from_x((iw - 3) // 2)

        @pl.when(end)
        def _():
            @pl.when((i >= WS) & (i < WS + FAR))
            def _():
                q = base + i - WS
                arrive(q, i)
                pass_in(q)

            @pl.when((i >= WS + FAR) & (i < WS + FAR + NEAR))
            def _():
                arrive_late(base + i - WS)

            nlate = 1 + 2 * FAR + NEAR - LATE

            @pl.when((i >= 1 + LAG) & (i < nlate - 1))
            def _():
                arrive(z_chunk(i - 1 - LAG), i)

            @pl.when(i == nlate - 1)
            def _():
                lax.fori_loop(nlate - 2 - LAG, nlate - 1, lambda j, _: (arrive(z_chunk(j), i), None)[1], None)

            @pl.when((i >= nlate) & (i < nlate + LATE))
            def _():
                arrive_late(z_chunk(i - 1))

        @pl.when(mid)
        def _():
            @pl.when(i == 0)
            def _():
                q = mp(base, 0)
                for k in range(NSUB):
                    piece = ax.at[q, :, pl.ds(k * sub, sub)]
                    wait_bytes(piece, recv_sub.at[k])
                    remote(piece, piece, send_first, recv_a.at[q], (x, z_out, t)).start()
                pass_in(q)

            @pl.when((i >= 1) & (i < FAR))
            def _():
                q = mp(base, i)
                arrive(q, i)

                @pl.when(i < NEAR)
                def _():
                    pass_out(q)

                pass_in(q)

            @pl.when((i >= 1) & (i < 1 + FAR))
            def _():
                q = mp(other, i - 1)
                arrive(q, i)
                pass_out(q)

            @pl.when((i >= WS + 1) & (i < WS + 1 + FAR))
            def _():
                q = base + i - WS - 1
                arrive(q, i)
                pass_in(q)

            @pl.when((i >= WS + 2) & (i < WS + 2 + FAR))
            def _():
                q = other + i - WS - 2
                arrive(q, i)

                @pl.when(i < WS + 2 + FAR - LATE)
                def _():
                    pass_out(q)

                @pl.when(i == WS + 2 + FAR - LATE)
                def _():
                    pl.semaphore_wait(credit_z, 1)

                @pl.when(i >= WS + 2 + FAR - LATE)
                def _():
                    pass_out_late(q)

    def early_loads():
        def from_z(j, _):
            load(jnp.where(end, z_chunk(j), mp(other, j)))
            return None

        lax.fori_loop(0, jnp.where(end, LOADS - 1 - LAG, LOADS - 1), from_z, None)

        def from_y(j, _):
            load(mp(base, j))
            return None

        lax.fori_loop(0, jnp.where(end, 0, LOADS), from_y, None)

    tn = min(512, cols)
    ntile = cols // tn

    def local_loads(u):
        slot = lax.rem(u, 2)
        here = pl.ds(pl.multiple_of(u * unit, unit), unit)
        mine = pl.ds(pl.multiple_of(t * rows + u * unit, unit), unit)
        return (pltpu.make_async_copy(a.at[mine], abuf.at[slot, 0], load_sem.at[slot, 0]),
                pltpu.make_async_copy(ap.at[here], abuf.at[slot, 1], load_sem.at[slot, 1]),
                pltpu.make_async_copy(r.at[here], rbuf.at[slot], load_sem.at[slot, 2]))

    def local_unit(u):
        slot = lax.rem(u, 2)
        here = pl.ds(pl.multiple_of(u * unit, unit), unit)
        for cp in local_loads(u):
            cp.wait()

        @pl.when(u + 1 < NUNIT)
        def _():
            wait_bytes(ap.at[pl.ds(pl.multiple_of((u + 1) * unit, unit), unit)], recv_da.at[u + 1])
            for cp in local_loads(u + 1):
                cp.start()

        def tile(n, _):
            cs = pl.ds(pl.multiple_of(n * tn, tn), tn)
            p0 = jnp.dot(abuf[slot, 0], wl[0, :, cs], preferred_element_type=jnp.float32)
            p1 = jnp.dot(abuf[slot, 1], wl[1, :, cs], preferred_element_type=jnp.float32)
            acc[here, cs] = (rbuf[slot, :, cs].astype(jnp.float32) + p0.astype(jnp.bfloat16).astype(jnp.float32)
                             + p1.astype(jnp.bfloat16).astype(jnp.float32))
            return None

        lax.fori_loop(0, ntile, tile, None)

    gs = NUNIT // 2

    def unit_of(u):
        b = side * NUNIT
        o = (1 - side) * NUNIT
        end_order = (b + 6, b + 7, o + 6, o + 7, b, b + 1, o + 4, b + 2, o + 5, b + 3, o, o + 1, b + 4, o + 2, b + 5, o + 3)
        mid_order = (b, b + 1, o, o + 1, b + 2, b + 3, o + 2, o + 3) + (0,) * NUNIT
        q = jnp.int32(0)
        for k in range(NHALF):
            q = q + jnp.where(u == k, jnp.where(end, end_order[k], mid_order[k]), 0)
        return q

    def wait_load(q):
        here = pl.ds(pl.multiple_of(q * half, half), half)
        wait_bytes(wl.at[:, here], load_a.at[q])

    def far_product(here, cs):
        p0 = jnp.dot(wl[0, here, :], wr[0, :, cs], preferred_element_type=jnp.float32)
        p1 = jnp.dot(wl[1, here, :], wr[1, :, cs], preferred_element_type=jnp.float32)
        v = acc[here, cs] + (p0.astype(jnp.bfloat16).astype(jnp.float32) + p1.astype(jnp.bfloat16).astype(jnp.float32))
        acc[here, cs] = v
        return v

    def squares(v):
        sq = v * v
        part = sq[:, :128]
        for k in range(1, sq.shape[1] // 128):
            part = part + sq[:, k * 128:(k + 1) * 128]
        return part

    def keep_squares(q, part):
        ss_loc[q] = jnp.sum(part.T, axis=0, keepdims=True)

    def remote_unit(u, _):
        q = unit_of(u)
        here = pl.ds(pl.multiple_of(q * half, half), half)

        @pl.when(mid | (u < NHALF - 4))
        def _():
            wait_load(q)

        def tile(n, part):
            cs = pl.ds(pl.multiple_of(n * tn, tn), tn)
            return part + squares(far_product(here, cs))

        keep_squares(q, lax.fori_loop(0, ntile, tile, jnp.zeros((half, 128), jnp.float32)))
        return None

    def column_unit(k):
        return jnp.where(k < 2, side, 1 - side) * gs + 2 + lax.rem(k, 2)

    def column_step(n):
        w_from_partner(n)

        @pl.when(n == 0)
        def _():
            for k in range(4):
                for e in range(2):
                    wait_load(column_unit(jnp.int32(k)) * 2 + e)

        cs = pl.ds(pl.multiple_of(n * wch, wch), wch)

        def rows_of(k, _):
            here = pl.ds(pl.multiple_of(column_unit(k) * unit, unit), unit)
            far_product(here, cs)
            return None

        lax.fori_loop(0, 4, rows_of, None)

        @pl.when(n == NWC - 1)
        def _():
            def sums(k, _):
                q = column_unit(k // 2) * 2 + lax.rem(k, 2)
                here = pl.ds(pl.multiple_of(q * half, half), half)

                def tile(m, part):
                    return part + squares(acc[here, pl.ds(pl.multiple_of(m * tn, tn), tn)])

                keep_squares(q, lax.fori_loop(0, ntile, tile, jnp.zeros((half, 128), jnp.float32)))
                return None

            lax.fori_loop(0, 8, sums, None)

    def slot_body(i, _):
        partner_sends(i)

        @pl.when(i == LOADS)
        def _():
            early_loads()

        @pl.when(end & (i == LOADS))
        def _():
            pl.semaphore_signal(credit_z, inc=1, device_id=(x, z_in, t), device_id_type=MESH)
            for cc in range(2):
                pl.semaphore_signal(credit_y, inc=1, device_id=(x, z, (1 - y) * 2 + cc), device_id_type=MESH)

        comm(i)

        @pl.when(i == LOCAL0 - 1)
        def _():
            own_w.wait()
            wait_bytes(wl.at[1], recv_dw)
            wait_bytes(ap.at[pl.ds(0, unit)], recv_da.at[0])
            for cp in local_loads(0):
                cp.start()

        @pl.when((i >= LOCAL0) & (i < LOCAL0 + NUNIT))
        def _():
            local_unit(i - LOCAL0)

        @pl.when(end & (i == WREADY))
        def _():
            lax.fori_loop(0, NWC, lambda n, _: (w_from_partner(n), None)[1], None)

        jc = i - COLS0

        @pl.when(mid & (jc >= 0) & (jc < WS) & (lax.rem(jc, 2) == 0))
        def _():
            column_step(jc // 2)

        lo = jnp.where(end, step_count(i - 1, END_UNITS), step_count(i - 1, MID_UNITS))
        hi = jnp.where(end, step_count(i, END_UNITS), step_count(i, MID_UNITS))
        lax.fori_loop(lo, hi, remote_unit, None)
        return None

    lax.fori_loop(0, NSLOT, slot_body, None)

    for k in range(1, 4):
        remote(ss_loc, ss_all.at[z], send_ss.at[k - 1], recv_ss.at[z], (x, lax.rem(z + k, 4), t)).start()
    wait_bytes(wl.at[1], send_dw)
    wait_bytes(ap, send_da)
    wait_bytes(wr.at[0], send_wd)
    wait_bytes(wr.at[0, pl.ds(0, kb // 2)], send_wx)
    wait_bytes(wr.at[0, pl.ds(0, kb // 2)], send_yw)

    @pl.when(end)
    def _():
        wait_bytes(ax.at[pl.ds(0, FAR + NEAR)], send_ya)
        wait_bytes(ax.at[pl.ds(0, FAR)], send_zi)

    @pl.when(mid)
    def _():
        wait_bytes(ax.at[pl.ds(0, FAR)], send_ya)
        wait_bytes(ax.at[pl.ds(0, 2 * FAR)], send_zi)
        wait_bytes(ax.at[pl.ds(0, 2 * FAR + NEAR - 1)], send_zo)
        wait_bytes(ax.at[0], send_first)

    for k in range(1, 4):
        src = lax.rem(z + k, 4)
        remote(ss_loc, ss_all.at[src], send_ss.at[k - 1], recv_ss.at[src], (x, src, t)).wait_recv()
        remote(ss_loc, ss_all.at[src], send_ss.at[k - 1], recv_ss.at[src], (x, src, t)).wait_send()
    ss_all[z] = ss_loc[...]

def finish_kernel(h, ss, g, h_out, n_out, hbuf, nbuf, sem):
    rows, cols = h.shape
    step_rows = rows // NHALF

    def copies(q):
        slot = lax.rem(q, NBUF)
        here = pl.ds(pl.multiple_of(q * step_rows, step_rows), step_rows)
        return (pltpu.make_async_copy(hbuf.at[slot], h_out.at[here], sem.at[slot, 0]),
                pltpu.make_async_copy(nbuf.at[slot], n_out.at[here], sem.at[slot, 1]))

    def step(q, _):
        slot = lax.rem(q, NBUF)

        @pl.when(q >= NBUF)
        def _():
            for cp in copies(q - NBUF):
                cp.wait()

        total = ss[0, q] + ss[1, q] + ss[2, q] + ss[3, q]
        inv = lax.rsqrt(total / (cols * 4) + EPS_NORM)
        col = jnp.broadcast_to(inv, (128, 128)).T
        rs = pl.ds(pl.multiple_of(q * 128, 128), 128)
        for m in range(cols // 128):
            cs = slice(m * 128, (m + 1) * 128)
            v = h[rs, cs]
            hbuf[slot, :, cs] = v.astype(jnp.bfloat16)
            nbuf[slot, :, cs] = (v * col * g[:, cs]).astype(jnp.bfloat16)
        for cp in copies(q):
            cp.start()
        return None

    lax.fori_loop(0, NHALF, step, None)

    def drain(q, _):
        for cp in copies(q):
            cp.wait()
        return None

    lax.fori_loop(NHALF - NBUF, NHALF, drain, None)


def solution(mesh):
    def local_step(attn_blk, w_blk, res_blk, gain_blk):
        kb = attn_blk.shape[1]
        rows, cols = res_blk.shape
        unit = rows // NUNIT
        any_spec = pl.BlockSpec(memory_space=pl.ANY)
        vmem_spec = pl.BlockSpec(memory_space=pltpu.VMEM)
        bf16, f32 = jnp.bfloat16, jnp.float32
        dma = pltpu.SemaphoreType.DMA
        h, ss, _, _ = pl.pallas_call(
            kernel,
            out_shape=(
                pltpu.VMEM((rows, cols), f32),
                pltpu.VMEM((4, NHALF, 1, 128), f32),
                jax.ShapeDtypeStruct((NCH, 2, rows // NCH, kb), bf16),
                jax.ShapeDtypeStruct((rows, kb), bf16),
            ),
            in_specs=[any_spec, any_spec, any_spec],
            out_specs=(vmem_spec, vmem_spec, any_spec, any_spec),
            scratch_shapes=[
                pltpu.VMEM((2, kb, cols), bf16),
                pltpu.VMEM((2, kb, cols), bf16),
                pltpu.VMEM((2, 2, unit, kb), bf16),
                pltpu.VMEM((2, unit, cols), bf16),
                pltpu.VMEM((NHALF, 1, 128), f32),
                dma((NCH,)), dma, dma, dma, dma,
                dma((NWC,)), dma((NWC,)), dma((NWC,)), dma, dma,
                dma((NUNIT,)), dma, dma, dma,
                dma((2, 3)), dma, dma((NHALF,)), dma((NSUB,)), dma,
                pltpu.SemaphoreType.REGULAR, pltpu.SemaphoreType.REGULAR,
                dma((3,)), dma((4,)),
            ],
            compiler_params=pltpu.CompilerParams(
                collective_id=0, has_side_effects=True, vmem_limit_bytes=44 * 1024 * 1024),
            name="gather_project",
        )(attn_blk, w_blk, res_blk)
        return pl.pallas_call(
            finish_kernel,
            out_shape=(jax.ShapeDtypeStruct((rows, cols), bf16),) * 2,
            in_specs=[vmem_spec, vmem_spec, vmem_spec],
            out_specs=(any_spec, any_spec),
            scratch_shapes=[pltpu.VMEM((NBUF, rows // NHALF, cols), bf16)] * 2 + [dma((NBUF, 2))],
            compiler_params=pltpu.CompilerParams(vmem_limit_bytes=8 * 1024 * 1024),
            name="norm_store",
        )(h, ss, gain_blk.reshape(1, cols))

    row_spec = P(("dp", "tp"), "tp2")
    return jax.shard_map(local_step, mesh=mesh, in_specs=(P("dp", "tp"), P("tp", "tp2"), row_spec, P("tp2")), out_specs=(row_spec, row_spec), check_vma=False)
```

```python
import functools

import jax
import jax.numpy as jnp
from jax import lax
from jax.experimental import pallas as pl
from jax.experimental.pallas import tpu as pltpu
from jax.sharding import PartitionSpec as P

EPS_NORM = 1e-6
MESH = pl.DeviceIdType.MESH
NCH = 64
FAR = NCH // 4
NEAR = NCH // 8
NWC = 8
WS = 2 * NWC
NUNIT = 8
NHALF = 2 * NUNIT
GRP = NCH // NUNIT
HGRP = NCH // NHALF
LATE = FAR // 2
NBUF = 4
LAG = 6
NSUB = 4
AHEAD = 12
NSLOT = 2 * FAR + NEAR + 1
LOCAL0 = 6
LOADS = 16
WREADY = WS + 2
COLS0 = FAR + 4


def step_count(i, slots):
    n = jnp.int32(0)
    for s in slots:
        n = n + jnp.where(i >= s, 1, 0)
    return n


END_UNITS = (20, 20, 21, 22, 23, 24, 26, 28, 30, 31, 32, 33, 36, 37, 39, 40)
MID_UNITS = (35, 35, 36, 36, 37, 37, 38, 38)


def kernel(a, w, r, acc, ss_all, ax, ap, wl, wr, abuf, rbuf, ss_loc,
           recv_a, send_ya, send_yw, send_zi, send_zo, recv_wy, recv_wx, recv_wd, send_wx, send_wd,
           recv_da, recv_dw, send_da, send_dw, load_sem, load_w, load_a, recv_sub, send_first, credit_z, credit_y, send_ss, recv_ss):
    x = lax.axis_index("dp")
    z = lax.axis_index("tp2")
    t = lax.axis_index("tp")
    y = t // 2
    c = t % 2
    rows, cols = acc.shape
    kb = w.shape[0]
    ch = rows // NCH
    wch = cols // NWC
    unit = ch * GRP
    half = ch * HGRP
    sub = ch // NSUB
    side = z // 2
    end = (z == 0) | (z == 3)
    mid = (z == 1) | (z == 2)
    base = side * (NCH // 2)
    other = (1 - side) * (NCH // 2)
    z_in = jnp.where(side == 0, z + 1, z - 1)
    z_out = jnp.where(side == 0, z - 1, z + 1)

    partner = (x, z, y * 2 + 1 - c)
    x_peer = (1 - x, z, t)
    y_same = (x, z, (1 - y) * 2 + c)
    y_cross = (x, z, (1 - y) * 2 + 1 - c)

    def remote(src, dst, send, recv, dev):
        return pltpu.make_async_remote_copy(
            src_ref=src, dst_ref=dst, send_sem=send, recv_sem=recv, device_id=dev, device_id_type=MESH)

    def wait_bytes(ref, sem):
        pltpu.make_async_copy(ref, ref, sem).wait()

    barrier = pltpu.get_barrier_semaphore()
    for dev in (partner, x_peer, y_same, y_cross):
        pl.semaphore_signal(barrier, inc=1, device_id=dev, device_id_type=MESH)
    for k in range(1, 4):
        pl.semaphore_signal(barrier, inc=1, device_id=(x, lax.rem(z + k, 4), t), device_id_type=MESH)
    pl.semaphore_wait(barrier, 7)

    def mp(start, j):
        return start + FAR + lax.rem(j + NEAR, FAR)

    def chunk_rows(q):
        return pl.ds(pl.multiple_of(q * ch, ch), ch)

    def send_y_a(q, dst=None):
        dst = ax.at[q, c] if dst is None else dst
        for cc in range(2):
            row = ((1 - y) * 2 + cc) * rows + q * ch
            remote(a.at[pl.ds(pl.multiple_of(row, ch), ch)], dst, send_ya, recv_a.at[q],
                   (x, z, (1 - y) * 2 + cc)).start()

    def send_y_first(q):
        for k in range(NSUB):
            for cc in range(2):
                row = ((1 - y) * 2 + cc) * rows + q * ch + k * sub
                remote(a.at[pl.ds(pl.multiple_of(row, sub), sub)], ax.at[q, c, pl.ds(k * sub, sub)], send_ya,
                       recv_sub.at[k], (x, z, (1 - y) * 2 + cc)).start()

    def w_part(part, n):
        return (pl.ds(pl.multiple_of(part * (kb // 2), kb // 2), kb // 2), pl.ds(pl.multiple_of(n * wch, wch), wch))

    def send_y_w(n):
        rs, cs = w_part(x, n)
        remote(w.at[rs, cs], wr.at[c, rs, cs], send_yw, recv_wy.at[n], y_same).start()

    def y_sends(i):
        iw = jnp.where(end, i, i - FAR)
        ia = jnp.where(end, i - WS, i)

        @pl.when((iw >= 0) & (iw < WS) & (lax.rem(iw, 2) == 0))
        def _():
            send_y_w(iw // 2)

        @pl.when(end & (ia >= 0) & (ia < FAR))
        def _():
            send_y_a(base + ia)

        @pl.when(end & (ia == FAR))
        def _():
            pl.semaphore_wait(credit_y, 2)

        @pl.when(end & (ia >= FAR) & (ia < FAR + NEAR))
        def _():
            send_y_a(base + ia, wl.at[c, chunk_rows(base + ia)])

        @pl.when(mid & (ia == 0))
        def _():
            send_y_first(mp(base, 0))

        @pl.when(mid & (ia >= 1) & (ia < FAR))
        def _():
            send_y_a(mp(base, ia))

    lax.fori_loop(0, AHEAD, lambda i, _: (y_sends(i), None)[1], None)

    kpart = kb // NUNIT

    def partner_sends(i):
        @pl.when(i < NUNIT // 2)
        def _():
            for k in range(2):
                rs = pl.ds(pl.multiple_of((2 * i + k) * kpart, kpart), kpart)
                remote(w.at[rs], wl.at[1, rs], send_dw, recv_dw, partner).start()

        u = i - NUNIT // 2

        @pl.when((u >= 0) & (u < NUNIT))
        def _():
            src = pl.ds(pl.multiple_of((y * 2 + 1 - c) * rows + u * unit, unit), unit)
            remote(a.at[src], ap.at[pl.ds(pl.multiple_of(u * unit, unit), unit)], send_da, recv_da.at[u], partner).start()

    own_w = pltpu.make_async_copy(w, wl.at[0], load_w)
    own_w.start()

    def load(q):
        here = pl.ds(pl.multiple_of(q * ch, ch), ch)
        for b in range(2):
            pltpu.make_async_copy(ax.at[q, b], wl.at[b, here], load_a.at[q // HGRP]).start()

    def arrive(q, i):
        wait_bytes(ax.at[q], recv_a.at[q])

        @pl.when(i >= LOADS)
        def _():
            load(q)

    def arrive_late(q):
        wait_bytes(wl.at[:, chunk_rows(q)], recv_a.at[q])

    def pass_out_late(q):
        remote(ax.at[q], wl.at[:, chunk_rows(q)], send_zo, recv_a.at[q], (x, z_out, t)).start()

    def pass_in(q):
        remote(ax.at[q], ax.at[q], send_zi, recv_a.at[q], (x, z_in, t)).start()

    def pass_out(q):
        remote(ax.at[q], ax.at[q], send_zo, recv_a.at[q], (x, z_out, t)).start()

    def w_from_y(n):
        rs, cs = w_part(x, n)
        part = wr.at[c, rs, cs]
        wait_bytes(part, recv_wy.at[n])
        remote(part, part, send_wx, recv_wx.at[n], x_peer).start()
        remote(part, part, send_wd, recv_wd.at[n], partner).start()

    def w_from_x(n):
        rs, cs = w_part(1 - x, n)
        part = wr.at[c, rs, cs]
        wait_bytes(part, recv_wx.at[n])
        remote(part, part, send_wd, recv_wd.at[n], partner).start()

    def w_from_partner(n):
        cs = pl.ds(pl.multiple_of(n * wch, wch), wch)
        wait_bytes(wr.at[1 - c, :, cs], recv_wd.at[n])

    def z_chunk(j):
        own = (j == 0) | (lax.rem(j, 2) == 1)
        first = jnp.where(own, mp(base, (j + 1) // 2), mp(other, j // 2 - 1))
        return jnp.where(j < 2 * NEAR - 1, first, jnp.where(j < NEAR + FAR, mp(other, j - NEAR), other + j - NEAR - FAR))

    def comm(i):
        y_sends(i + AHEAD)
        iw = jnp.where(end, i, i - FAR)
        odd = lax.rem(i, 2) == 1

        @pl.when(odd & (iw >= 1) & (iw < WS))
        def _():
            w_from_y(iw // 2)

        @pl.when(odd & (iw >= 3) & (iw < WS + 2))
        def _():
            w_from_x((iw - 3) // 2)

        @pl.when(end)
        def _():
            @pl.when((i >= WS) & (i < WS + FAR))
            def _():
                q = base + i - WS
                arrive(q, i)
                pass_in(q)

            @pl.when((i >= WS + FAR) & (i < WS + FAR + NEAR))
            def _():
                arrive_late(base + i - WS)

            nlate = 1 + 2 * FAR + NEAR - LATE

            @pl.when((i >= 1 + LAG) & (i < nlate - 1))
            def _():
                arrive(z_chunk(i - 1 - LAG), i)

            @pl.when(i == nlate - 1)
            def _():
                lax.fori_loop(nlate - 2 - LAG, nlate - 1, lambda j, _: (arrive(z_chunk(j), i), None)[1], None)

            @pl.when((i >= nlate) & (i < nlate + LATE))
            def _():
                arrive_late(z_chunk(i - 1))

        @pl.when(mid)
        def _():
            @pl.when(i == 0)
            def _():
                q = mp(base, 0)
                for k in range(NSUB):
                    piece = ax.at[q, :, pl.ds(k * sub, sub)]
                    wait_bytes(piece, recv_sub.at[k])
                    remote(piece, piece, send_first, recv_a.at[q], (x, z_out, t)).start()
                pass_in(q)

            @pl.when((i >= 1) & (i < FAR))
            def _():
                q = mp(base, i)
                arrive(q, i)

                @pl.when(i < NEAR)
                def _():
                    pass_out(q)

                pass_in(q)

            @pl.when((i >= 1) & (i < 1 + FAR))
            def _():
                q = mp(other, i - 1)
                arrive(q, i)
                pass_out(q)

            @pl.when((i >= WS + 1) & (i < WS + 1 + FAR))
            def _():
                q = base + i - WS - 1
                arrive(q, i)
                pass_in(q)

            @pl.when((i >= WS + 2) & (i < WS + 2 + FAR))
            def _():
                q = other + i - WS - 2
                arrive(q, i)

                @pl.when(i < WS + 2 + FAR - LATE)
                def _():
                    pass_out(q)

                @pl.when(i == WS + 2 + FAR - LATE)
                def _():
                    pl.semaphore_wait(credit_z, 1)

                @pl.when(i >= WS + 2 + FAR - LATE)
                def _():
                    pass_out_late(q)

    def early_loads():
        def from_z(j, _):
            load(jnp.where(end, z_chunk(j), mp(other, j)))
            return None

        lax.fori_loop(0, jnp.where(end, LOADS - 1 - LAG, LOADS - 1), from_z, None)

        def from_y(j, _):
            load(mp(base, j))
            return None

        lax.fori_loop(0, jnp.where(end, 0, LOADS), from_y, None)

    tn = min(512, cols)
    ntile = cols // tn

    def local_loads(u):
        slot = lax.rem(u, 2)
        here = pl.ds(pl.multiple_of(u * unit, unit), unit)
        mine = pl.ds(pl.multiple_of(t * rows + u * unit, unit), unit)
        return (pltpu.make_async_copy(a.at[mine], abuf.at[slot, 0], load_sem.at[slot, 0]),
                pltpu.make_async_copy(ap.at[here], abuf.at[slot, 1], load_sem.at[slot, 1]),
                pltpu.make_async_copy(r.at[here], rbuf.at[slot], load_sem.at[slot, 2]))

    def local_unit(u):
        slot = lax.rem(u, 2)
        here = pl.ds(pl.multiple_of(u * unit, unit), unit)
        for cp in local_loads(u):
            cp.wait()

        @pl.when(u + 1 < NUNIT)
        def _():
            wait_bytes(ap.at[pl.ds(pl.multiple_of((u + 1) * unit, unit), unit)], recv_da.at[u + 1])
            for cp in local_loads(u + 1):
                cp.start()

        def tile(n, _):
            cs = pl.ds(pl.multiple_of(n * tn, tn), tn)
            p0 = jnp.dot(abuf[slot, 0], wl[0, :, cs], preferred_element_type=jnp.float32)
            p1 = jnp.dot(abuf[slot, 1], wl[1, :, cs], preferred_element_type=jnp.float32)
            acc[here, cs] = (rbuf[slot, :, cs].astype(jnp.float32) + p0.astype(jnp.bfloat16).astype(jnp.float32)
                             + p1.astype(jnp.bfloat16).astype(jnp.float32))
            return None

        lax.fori_loop(0, ntile, tile, None)

    gs = NUNIT // 2

    def unit_of(u):
        b = side * NUNIT
        o = (1 - side) * NUNIT
        end_order = (b + 6, b + 7, o + 6, o + 7, b, b + 1, o + 4, b + 2, o + 5, b + 3, o, o + 1, b + 4, o + 2, b + 5, o + 3)
        mid_order = (b, b + 1, o, o + 1, b + 2, b + 3, o + 2, o + 3) + (0,) * NUNIT
        q = jnp.int32(0)
        for k in range(NHALF):
            q = q + jnp.where(u == k, jnp.where(end, end_order[k], mid_order[k]), 0)
        return q

    def wait_load(q):
        here = pl.ds(pl.multiple_of(q * half, half), half)
        wait_bytes(wl.at[:, here], load_a.at[q])

    def far_product(here, cs):
        p0 = jnp.dot(wl[0, here, :], wr[0, :, cs], preferred_element_type=jnp.float32)
        p1 = jnp.dot(wl[1, here, :], wr[1, :, cs], preferred_element_type=jnp.float32)
        v = acc[here, cs] + (p0.astype(jnp.bfloat16).astype(jnp.float32) + p1.astype(jnp.bfloat16).astype(jnp.float32))
        acc[here, cs] = v
        return v

    def squares(v):
        sq = v * v
        part = sq[:, :128]
        for k in range(1, sq.shape[1] // 128):
            part = part + sq[:, k * 128:(k + 1) * 128]
        return part

    def keep_squares(q, part):
        ss_loc[q] = jnp.sum(part.T, axis=0, keepdims=True)

    def remote_unit(u, _):
        q = unit_of(u)
        here = pl.ds(pl.multiple_of(q * half, half), half)

        @pl.when(mid | (u < NHALF - 4))
        def _():
            wait_load(q)

        def tile(n, part):
            cs = pl.ds(pl.multiple_of(n * tn, tn), tn)
            return part + squares(far_product(here, cs))

        keep_squares(q, lax.fori_loop(0, ntile, tile, jnp.zeros((half, 128), jnp.float32)))
        return None

    def column_unit(k):
        return jnp.where(k < 2, side, 1 - side) * gs + 2 + lax.rem(k, 2)

    def column_step(n):
        w_from_partner(n)

        @pl.when(n == 0)
        def _():
            for k in range(4):
                for e in range(2):
                    wait_load(column_unit(jnp.int32(k)) * 2 + e)

        cs = pl.ds(pl.multiple_of(n * wch, wch), wch)

        def rows_of(k, _):
            here = pl.ds(pl.multiple_of(column_unit(k) * unit, unit), unit)
            far_product(here, cs)
            return None

        lax.fori_loop(0, 4, rows_of, None)

        @pl.when(n == NWC - 1)
        def _():
            def sums(k, _):
                q = column_unit(k // 2) * 2 + lax.rem(k, 2)
                here = pl.ds(pl.multiple_of(q * half, half), half)

                def tile(m, part):
                    return part + squares(acc[here, pl.ds(pl.multiple_of(m * tn, tn), tn)])

                keep_squares(q, lax.fori_loop(0, ntile, tile, jnp.zeros((half, 128), jnp.float32)))
                return None

            lax.fori_loop(0, 8, sums, None)

    def slot_body(i, _):
        partner_sends(i)

        @pl.when(i == LOADS)
        def _():
            early_loads()

        @pl.when(end & (i == LOADS))
        def _():
            pl.semaphore_signal(credit_z, inc=1, device_id=(x, z_in, t), device_id_type=MESH)
            for cc in range(2):
                pl.semaphore_signal(credit_y, inc=1, device_id=(x, z, (1 - y) * 2 + cc), device_id_type=MESH)

        comm(i)

        @pl.when(i == LOCAL0 - 1)
        def _():
            own_w.wait()
            wait_bytes(wl.at[1], recv_dw)
            wait_bytes(ap.at[pl.ds(0, unit)], recv_da.at[0])
            for cp in local_loads(0):
                cp.start()

        @pl.when((i >= LOCAL0) & (i < LOCAL0 + NUNIT))
        def _():
            local_unit(i - LOCAL0)

        @pl.when(end & (i == WREADY))
        def _():
            lax.fori_loop(0, NWC, lambda n, _: (w_from_partner(n), None)[1], None)

        jc = i - COLS0

        @pl.when(mid & (jc >= 0) & (jc < WS) & (lax.rem(jc, 2) == 0))
        def _():
            column_step(jc // 2)

        lo = jnp.where(end, step_count(i - 1, END_UNITS), step_count(i - 1, MID_UNITS))
        hi = jnp.where(end, step_count(i, END_UNITS), step_count(i, MID_UNITS))
        lax.fori_loop(lo, hi, remote_unit, None)
        return None

    lax.fori_loop(0, NSLOT, slot_body, None)

    ss_all[z] = ss_loc[...]
    for k in range(1, 4):
        remote(ss_loc, ss_all.at[z], send_ss.at[k - 1], recv_ss.at[z], (x, lax.rem(z + k, 4), t)).start()
    wait_bytes(wl.at[1], send_dw)
    wait_bytes(ap, send_da)
    wait_bytes(wr.at[0], send_wd)
    wait_bytes(wr.at[0, pl.ds(0, kb // 2)], send_wx)
    wait_bytes(wr.at[0, pl.ds(0, kb // 2)], send_yw)

    @pl.when(end)
    def _():
        wait_bytes(ax.at[pl.ds(0, FAR + NEAR)], send_ya)
        wait_bytes(ax.at[pl.ds(0, FAR)], send_zi)

    @pl.when(mid)
    def _():
        wait_bytes(ax.at[pl.ds(0, FAR)], send_ya)
        wait_bytes(ax.at[pl.ds(0, 2 * FAR)], send_zi)
        wait_bytes(ax.at[pl.ds(0, 2 * FAR + NEAR - 1)], send_zo)
        wait_bytes(ax.at[0], send_first)

    for k in range(1, 4):
        src = lax.rem(z + k, 4)
        remote(ss_loc, ss_all.at[src], send_ss.at[k - 1], recv_ss.at[src], (x, src, t)).wait_recv()
        remote(ss_loc, ss_all.at[src], send_ss.at[k - 1], recv_ss.at[src], (x, src, t)).wait_send()

def finish_kernel(h, ss, g, h_out, n_out, hbuf, nbuf, sem):
    rows, cols = h.shape
    step_rows = rows // NHALF

    def copies(q):
        slot = lax.rem(q, NBUF)
        here = pl.ds(pl.multiple_of(q * step_rows, step_rows), step_rows)
        return (pltpu.make_async_copy(hbuf.at[slot], h_out.at[here], sem.at[slot, 0]),
                pltpu.make_async_copy(nbuf.at[slot], n_out.at[here], sem.at[slot, 1]))

    def step(q, _):
        slot = lax.rem(q, NBUF)

        @pl.when(q >= NBUF)
        def _():
            for cp in copies(q - NBUF):
                cp.wait()

        total = ss[0, q] + ss[1, q] + ss[2, q] + ss[3, q]
        inv = lax.rsqrt(total / (cols * 4) + EPS_NORM)
        col = jnp.broadcast_to(inv, (128, 128)).T
        rs = pl.ds(pl.multiple_of(q * 128, 128), 128)
        for m in range(cols // 128):
            cs = slice(m * 128, (m + 1) * 128)
            v = h[rs, cs]
            hbuf[slot, :, cs] = v.astype(jnp.bfloat16)
            nbuf[slot, :, cs] = (v * col * g[:, cs]).astype(jnp.bfloat16)
        for cp in copies(q):
            cp.start()
        return None

    lax.fori_loop(0, NHALF, step, None)

    def drain(q, _):
        for cp in copies(q):
            cp.wait()
        return None

    lax.fori_loop(NHALF - NBUF, NHALF, drain, None)


def solution(mesh):
    def local_step(attn_blk, w_blk, res_blk, gain_blk):
        kb = attn_blk.shape[1]
        rows, cols = res_blk.shape
        unit = rows // NUNIT
        any_spec = pl.BlockSpec(memory_space=pl.ANY)
        vmem_spec = pl.BlockSpec(memory_space=pltpu.VMEM)
        bf16, f32 = jnp.bfloat16, jnp.float32
        dma = pltpu.SemaphoreType.DMA
        h, ss, _, _ = pl.pallas_call(
            kernel,
            out_shape=(
                pltpu.VMEM((rows, cols), f32),
                pltpu.VMEM((4, NHALF, 1, 128), f32),
                jax.ShapeDtypeStruct((NCH, 2, rows // NCH, kb), bf16),
                jax.ShapeDtypeStruct((rows, kb), bf16),
            ),
            in_specs=[any_spec, any_spec, any_spec],
            out_specs=(vmem_spec, vmem_spec, any_spec, any_spec),
            scratch_shapes=[
                pltpu.VMEM((2, kb, cols), bf16),
                pltpu.VMEM((2, kb, cols), bf16),
                pltpu.VMEM((2, 2, unit, kb), bf16),
                pltpu.VMEM((2, unit, cols), bf16),
                pltpu.VMEM((NHALF, 1, 128), f32),
                dma((NCH,)), dma, dma, dma, dma,
                dma((NWC,)), dma((NWC,)), dma((NWC,)), dma, dma,
                dma((NUNIT,)), dma, dma, dma,
                dma((2, 3)), dma, dma((NHALF,)), dma((NSUB,)), dma,
                pltpu.SemaphoreType.REGULAR, pltpu.SemaphoreType.REGULAR,
                dma((3,)), dma((4,)),
            ],
            compiler_params=pltpu.CompilerParams(
                collective_id=0, has_side_effects=True, vmem_limit_bytes=44 * 1024 * 1024),
            name="gather_project",
        )(attn_blk, w_blk, res_blk)
        return pl.pallas_call(
            finish_kernel,
            out_shape=(jax.ShapeDtypeStruct((rows, cols), bf16),) * 2,
            in_specs=[vmem_spec, vmem_spec, vmem_spec],
            out_specs=(any_spec, any_spec),
            scratch_shapes=[pltpu.VMEM((NBUF, rows // NHALF, cols), bf16)] * 2 + [dma((NBUF, 2))],
            compiler_params=pltpu.CompilerParams(vmem_limit_bytes=8 * 1024 * 1024),
            name="norm_store",
        )(h, ss, gain_blk.reshape(1, cols))

    row_spec = P(("dp", "tp"), "tp2")
    return jax.shard_map(local_step, mesh=mesh, in_specs=(P("dp", "tp"), P("tp", "tp2"), row_spec, P("tp2")), out_specs=(row_spec, row_spec), check_vma=False)
```
